32 devices in a mesh: dp: 2 (over x), tp: 4 (over z), cp: 4 (over y, core).
Axes of the slice: x: 2, y: 2, z: 4, core: 2. Of those that a mesh axis runs over, the one named last changes fastest.
Arguments:
- x: bfloat16 [8192, 4096], P(('dp', 'cp')), parts along dimension 0
- doc_id: int32 [8192], P(('dp', 'cp')), parts along dimension 0
- pos_in_doc: int32 [8192], P(('dp', 'cp')), parts along dimension 0
- norm_gain: float32 [4096], replicated
- w_q: bfloat16 [4096, 4096], P(None, 'tp')
- w_k: bfloat16 [4096, 1024], P(None, 'tp')
- w_v: bfloat16 [4096, 1024], P(None, 'tp')
- w_o: bfloat16 [4096, 4096], P('tp')
- inv_freq: float32 [64], replicated
Outputs:
- output 1: bfloat16 [8192, 4096], P(('dp', 'cp')), parts along dimension 0
- output 2: bfloat16 [8192, 8, 128], P(('dp', 'cp'), 'tp'), parts along dimension 0
- output 3: bfloat16 [8192, 8, 128], P(('dp', 'cp'), 'tp'), parts along dimension 0
There are 2 independent parts. The reference program is written for one: setup_inputs(seed, part) draws one part's arguments, and reference() takes and returns one part's arrays. A program takes and returns all parts, laid end to end along the dimension named above; an argument that names none is the same for every part.
All inputs are finite; a program needn't handle non-finite values.
Results may differ from the reference program's by a relative error of at most 0.00397746.
Values are sent between devices in bfloat16 or wider.
A program may use at most 1 GiB of HBM per device.

```python
import jax
import jax.numpy as jnp
from jax import lax

TOKENS = 4096
CP_SIZE = 4
D_MODEL = 4096
Q_HEADS = 32
KV_HEADS = 8
HEAD_DIM = 128
DOC_LEN = 128
ROPE_THETA = 10000
QUERY_ROWS = 128

PIECE_LEN = TOKENS // (2 * CP_SIZE)
GROUP_SIZE = Q_HEADS // KV_HEADS
MAX_DOCS = TOKENS // (DOC_LEN // 2) + 2


def to_stored(glob_arr):
    pieces = glob_arr.reshape((2 * CP_SIZE, PIECE_LEN) + glob_arr.shape[1:])
    paired = jnp.stack([pieces[:CP_SIZE], pieces[CP_SIZE:][::-1]], axis=1)
    return paired.reshape(glob_arr.shape)


def draw_documents(doc_key):
    key_long, key_before, key_after = jax.random.split(doc_key, 3)
    first_piece = (DOC_LEN - 2) // PIECE_LEN + 1
    long_piece = jax.random.randint(key_long, (), first_piece, 2 * CP_SIZE)
    long_start = long_piece * PIECE_LEN - DOC_LEN + 1
    long_end = long_start + DOC_LEN
    lens_before = jax.random.randint(key_before, (MAX_DOCS,), DOC_LEN // 2, DOC_LEN + 1)
    lens_after = jax.random.randint(key_after, (MAX_DOCS,), DOC_LEN // 2, DOC_LEN + 1)
    starts_before = jnp.cumsum(lens_before)
    starts_after = long_end + jnp.cumsum(lens_after) - lens_after
    start_marks = jnp.zeros((TOKENS,), jnp.int32).at[0].set(1).at[long_start].set(1)
    start_marks = start_marks.at[jnp.where(starts_before < long_start, starts_before, TOKENS)].set(1, mode='drop')
    start_marks = start_marks.at[starts_after].set(1, mode='drop')
    doc_glob = jnp.cumsum(start_marks) - 1
    tok_index = jnp.arange(TOKENS)
    pos_glob = tok_index - lax.cummax(tok_index * start_marks, axis=0)
    return doc_glob.astype(jnp.int32), pos_glob.astype(jnp.int32)


def normal_weight(weight_key, fan_in, fan_out):
    return (jax.random.normal(weight_key, (fan_in, fan_out), jnp.float32) * fan_in ** -0.5).astype(jnp.bfloat16)


def setup_inputs(seed: int = 0, part: int = 0) -> dict:
    part_key = jax.random.fold_in(jax.random.key(seed), part)
    key_doc, key_noise, key_drift = jax.random.split(part_key, 3)
    shared = jax.random.split(jax.random.key(seed + 1), 6)
    doc_glob, pos_glob = draw_documents(key_doc)
    pos_ratio = pos_glob.astype(jnp.float32) / DOC_LEN
    drift_dir = jax.random.normal(key_drift, (D_MODEL,), jnp.float32)
    x_noise = jax.random.normal(key_noise, (TOKENS, D_MODEL), jnp.float32)
    x_glob = x_noise + 3.0 * pos_ratio[:, None] * drift_dir[None, :]
    norm_gain = 1.0 + 0.25 * jax.random.normal(shared[0], (D_MODEL,), jnp.float32)
    w_q = normal_weight(shared[1], D_MODEL, Q_HEADS * HEAD_DIM)
    w_k = normal_weight(shared[2], D_MODEL, KV_HEADS * HEAD_DIM)
    w_v = normal_weight(shared[3], D_MODEL, KV_HEADS * HEAD_DIM)
    w_o = normal_weight(shared[4], Q_HEADS * HEAD_DIM, D_MODEL)
    base_freq = ROPE_THETA ** (-jnp.arange(0, HEAD_DIM, 2, dtype=jnp.float32) / HEAD_DIM)
    inv_freq = base_freq * jnp.exp(0.1 * jax.random.normal(shared[5], (HEAD_DIM // 2,), jnp.float32))
    return {'x': to_stored(x_glob).astype(jnp.bfloat16), 'doc_id': to_stored(doc_glob), 'pos_in_doc': to_stored(pos_glob), 'norm_gain': norm_gain, 'w_q': w_q, 'w_k': w_k, 'w_v': w_v, 'w_o': w_o, 'inv_freq': inv_freq}


def apply_rope(vectors, cos_t, sin_t):
    half_dim = vectors.shape[-1] // 2
    lower_half = vectors[..., :half_dim].astype(jnp.float32)
    upper_half = vectors[..., half_dim:].astype(jnp.float32)
    turned = jnp.concatenate([lower_half * cos_t - upper_half * sin_t, upper_half * cos_t + lower_half * sin_t], axis=-1)
    return turned.astype(jnp.bfloat16)


def reference(x, doc_id, pos_in_doc, norm_gain, w_q, w_k, w_v, w_o, inv_freq):
    x_f32 = x.astype(jnp.float32)
    inv_rms = lax.rsqrt(jnp.mean(x_f32 * x_f32, axis=-1, keepdims=True) + 1e-5)
    normed = (x_f32 * inv_rms * norm_gain).astype(jnp.bfloat16)
    q_new = jnp.dot(normed, w_q, preferred_element_type=jnp.float32).astype(jnp.bfloat16).reshape(TOKENS, KV_HEADS, GROUP_SIZE, HEAD_DIM)
    k_new = jnp.dot(normed, w_k, preferred_element_type=jnp.float32).astype(jnp.bfloat16).reshape(TOKENS, KV_HEADS, HEAD_DIM)
    v_new = jnp.dot(normed, w_v, preferred_element_type=jnp.float32).astype(jnp.bfloat16).reshape(TOKENS, KV_HEADS, HEAD_DIM)
    rope_angle = pos_in_doc.astype(jnp.float32)[:, None] * inv_freq[None, :]
    cos_t = jnp.cos(rope_angle)
    sin_t = jnp.sin(rope_angle)
    q_rot = apply_rope(q_new, cos_t[:, None, None, :], sin_t[:, None, None, :])
    k_rot = apply_rope(k_new, cos_t[:, None, :], sin_t[:, None, :])
    tok_index = to_stored(jnp.arange(TOKENS))
    k_f32 = k_rot.astype(jnp.float32)
    v_f32 = v_new.astype(jnp.float32)
    blocks = TOKENS // QUERY_ROWS

    def attend(block_args):
        q_blk, doc_blk, idx_blk = block_args
        scores = jnp.einsum('qngd,knd->ngqk', q_blk.astype(jnp.float32), k_f32) * (HEAD_DIM ** -0.5)
        visible = (doc_blk[:, None] == doc_id[None, :]) & (tok_index[None, :] <= idx_blk[:, None])
        scores = jnp.where(visible, scores, -1e30)
        attn_probs = jax.nn.softmax(scores, axis=-1).astype(jnp.bfloat16).astype(jnp.float32)
        return jnp.einsum('ngqk,knd->qngd', attn_probs, v_f32).astype(jnp.bfloat16)

    attn_out = lax.map(attend, (q_rot.reshape(blocks, QUERY_ROWS, KV_HEADS, GROUP_SIZE, HEAD_DIM), doc_id.reshape(blocks, QUERY_ROWS), tok_index.reshape(blocks, QUERY_ROWS)))
    mixed_out = jnp.dot(attn_out.reshape(TOKENS, Q_HEADS * HEAD_DIM), w_o, preferred_element_type=jnp.float32)
    y_out = (x_f32 + mixed_out).astype(jnp.bfloat16)
    return (y_out, k_rot, v_new)
```

```python
import functools

import jax
import jax.numpy as jnp
from jax import lax
from jax.experimental import pallas as pl
from jax.experimental.pallas import tpu as pltpu
from jax.sharding import PartitionSpec as P

MESH = pl.DeviceIdType.MESH
HBM = pltpu.HBM
VMEM = pltpu.VMEM
HEAD = 128
Q_TILE = 128
F32 = jnp.float32
BF16 = jnp.bfloat16


def rope(vec, cos_t, sin_t):
    vec = vec.astype(F32)
    return (vec * cos_t + pltpu.roll(vec, HEAD // 2, 1) * sin_t).astype(BF16)


def kv_kernel(x_ref, gain_ref, wk_ref, wv_ref, cos_ref, sin_ref, h_ref, kv_ref):
    rows, width = x_ref.shape
    step = 16

    def norm_rows(i, _):
        at = pl.ds(pl.multiple_of(i * step, step), step)
        xf = x_ref[at, :].astype(F32)
        inv = lax.rsqrt(jnp.sum(xf * xf, axis=-1, keepdims=True) * (1.0 / width) + 1e-5)
        h_ref[at, :] = (xf * inv * gain_ref[...]).astype(BF16)
        return 0

    lax.fori_loop(0, rows // step, norm_rows, 0)
    h = h_ref[...]
    k_new = jnp.dot(h, wk_ref[...], preferred_element_type=F32).astype(BF16)
    v_new = jnp.dot(h, wv_ref[...], preferred_element_type=F32).astype(BF16)
    cols = k_new.shape[1]
    for j in range(cols // HEAD):
        at = slice(j * HEAD, (j + 1) * HEAD)
        kv_ref[:, at] = rope(k_new[:, at], cos_ref[...], sin_ref[...])
    kv_ref[:, cols:] = v_new


def norm_kv(x, gain, w_k, w_v, cos_t, sin_t):
    rows, width = x.shape
    cols = w_k.shape[1]
    tile = 256
    const = lambda i: (0, 0)
    byrow = lambda i: (i, 0)
    return pl.pallas_call(
        kv_kernel,
        grid=(rows // tile,),
        in_specs=[
            pl.BlockSpec((tile, width), byrow),
            pl.BlockSpec((1, width), const),
            pl.BlockSpec((width, cols), const),
            pl.BlockSpec((width, cols), const),
            pl.BlockSpec((tile, HEAD), byrow),
            pl.BlockSpec((tile, HEAD), byrow),
        ],
        out_specs=[pl.BlockSpec((tile, width), byrow), pl.BlockSpec((tile, 2 * cols), byrow)],
        out_shape=[jax.ShapeDtypeStruct((rows, width), BF16), jax.ShapeDtypeStruct((rows, 2 * cols), BF16)],
        compiler_params=pltpu.CompilerParams(vmem_limit_bytes=32 << 20),
        cost_estimate=pl.CostEstimate(flops=4 * rows * width * cols, bytes_accessed=21 << 20, transcendentals=0),
        name="norm_kv",
    )(x, gain.reshape(1, width), w_k, w_v, cos_t, sin_t)


def q_kernel(h_ref, wq_ref, cos_ref, sin_ref, q_ref):
    q_new = jnp.dot(h_ref[...], wq_ref[...], preferred_element_type=F32).astype(BF16)
    for j in range(q_new.shape[1] // HEAD):
        at = slice(j * HEAD, (j + 1) * HEAD)
        q_ref[:, at] = rope(q_new[:, at], cos_ref[...], sin_ref[...])


def q_proj(h, w_q, cos_t, sin_t):
    rows, width = h.shape
    cols = w_q.shape[1]
    tile = 256
    const = lambda i: (0, 0)
    return pl.pallas_call(
        q_kernel,
        grid=(cols // tile,),
        in_specs=[
            pl.BlockSpec((rows, width), const),
            pl.BlockSpec((width, tile), lambda i: (0, i)),
            pl.BlockSpec((rows, HEAD), const),
            pl.BlockSpec((rows, HEAD), const),
        ],
        out_specs=pl.BlockSpec((rows, tile), lambda i: (0, i)),
        out_shape=jax.ShapeDtypeStruct((rows, cols), BF16),
        compiler_params=pltpu.CompilerParams(vmem_limit_bytes=40 << 20),
        cost_estimate=pl.CostEstimate(flops=2 * rows * width * cols, bytes_accessed=18 << 20, transcendentals=0),
        name="q_proj",
    )(h, w_q, cos_t, sin_t)


def attn_kernel(n_cp, group, gidx_ref, low_ref, place_ref, q_ref, tok_ref, pos_ref, kv0, kv1, kv2, kv3, o_ref, kv_ref, sems):
    head, blk = pl.program_id(0), pl.program_id(1)
    piece = kv0.shape[0] // 2
    kv_cols = kv0.shape[1] // 2

    @pl.when((head == 0) & (blk == 0))
    def _():
        copies = []
        for r, src in enumerate((kv0, kv1, kv2, kv3)):
            for half in range(2):
                at = pl.multiple_of(place_ref[2 * r + half], piece)
                copies.append(pltpu.make_async_copy(src.at[pl.ds(half * piece, piece)], kv_ref.at[pl.ds(at, piece)], sems.at[2 * r + half]))
        for c in copies:
            c.start()
        for c in copies:
            c.wait()

    q_rows = q_ref.shape[0]
    q = jnp.concatenate([q_ref[:, g * HEAD:(g + 1) * HEAD] for g in range(group)], axis=0)
    g0 = gidx_ref[blk]
    tok = jnp.concatenate([tok_ref[...]] * group, axis=0)
    first = tok - jnp.concatenate([pos_ref[...]] * group, axis=0)
    scale = HEAD ** -0.5
    k_at = pl.ds(pl.multiple_of(head * HEAD, HEAD), HEAD)
    v_at = pl.ds(pl.multiple_of(kv_cols + head * HEAD, HEAD), HEAD)

    def scores(start, width):
        keys = kv_ref[pl.ds(pl.multiple_of(start, Q_TILE), width), k_at]
        s = lax.dot_general(q, keys, (((1,), (1,)), ((), ())), preferred_element_type=F32) * scale
        u = start + lax.broadcasted_iota(jnp.int32, (1, width), 1)
        return jnp.where((u >= first) & (u <= tok), s, -1e30)

    def values(start, width):
        return kv_ref[pl.ds(pl.multiple_of(start, Q_TILE), width), v_at]

    near = jnp.maximum(g0 - Q_TILE, 0)
    s = scores(near, 2 * Q_TILE)
    m = jnp.max(s, axis=-1, keepdims=True)
    p = jnp.exp(s - m)
    total = jnp.sum(p, axis=-1, keepdims=True)
    acc = jnp.dot(p.astype(BF16), values(near, 2 * Q_TILE), preferred_element_type=F32)

    def far(i, carry):
        m, total, acc = carry
        start = i * Q_TILE
        s = scores(start, Q_TILE)
        m_new = jnp.maximum(m, jnp.max(s, axis=-1, keepdims=True))
        old = jnp.exp(m - m_new)
        p = jnp.exp(s - m_new)
        total = total * old + jnp.sum(p, axis=-1, keepdims=True)
        acc = acc * old + jnp.dot(p.astype(BF16), values(start, Q_TILE), preferred_element_type=F32)
        return m_new, total, acc

    m, total, acc = lax.fori_loop(low_ref[blk], near // Q_TILE, far, (m, total, acc))
    out = (acc / total).astype(BF16)
    for g in range(group):
        o_ref[:, g * HEAD:(g + 1) * HEAD] = out[g * q_rows:(g + 1) * q_rows]


def attention(q, kvs, tok, pos, cp):
    rows, q_cols = q.shape
    n_cp = len(kvs)
    kv_cols = kvs[0].shape[1] // 2
    heads = kv_cols // HEAD
    group = q_cols // kv_cols
    piece = rows // 2
    gidx = tok[::Q_TILE]
    low = (gidx - pos[::Q_TILE]) // Q_TILE
    owners = [cp ^ r for r in range(n_cp)]
    place = jnp.stack([w for o in owners for w in (o * piece, (2 * n_cp - 1 - o) * piece)]).astype(jnp.int32)
    q_map = lambda h, i, *_: (i, h)
    row_map = lambda h, i, *_: (i, 0)
    return pl.pallas_call(
        functools.partial(attn_kernel, n_cp, group),
        grid_spec=pltpu.PrefetchScalarGridSpec(
            num_scalar_prefetch=3,
            grid=(heads, rows // Q_TILE),
            in_specs=[
                pl.BlockSpec((Q_TILE, group * HEAD), q_map),
                pl.BlockSpec((Q_TILE, 1), row_map),
                pl.BlockSpec((Q_TILE, 1), row_map),
            ] + [pl.BlockSpec(memory_space=HBM)] * n_cp,
            out_specs=pl.BlockSpec((Q_TILE, group * HEAD), q_map),
            scratch_shapes=[VMEM((n_cp * rows, 2 * kv_cols), BF16), pltpu.SemaphoreType.DMA((2 * n_cp,))],
        ),
        out_shape=jax.ShapeDtypeStruct((rows, q_cols), BF16),
        compiler_params=pltpu.CompilerParams(vmem_limit_bytes=32 << 20),
        cost_estimate=pl.CostEstimate(flops=5 << 30, bytes_accessed=8 << 20, transcendentals=0),
        name="attn",
    )(gidx, low, place, q, tok[:, None], pos[:, None], *kvs)


def out_kernel(o_ref, fl_ref, fr_ref, fl2_ref, fr2_ref, wown_ref, x_ref, y_ref,
               wbuf, wtile, xtile, obuf, acc, ytile,
               load_sem, tile_sem, y_sem, wsend, wrecv, w3_send, w3_recv, own_send, fwd_send, o_recv):
    rows, kdim = o_ref.shape
    width = x_ref.shape[1]
    slice_rows = fl_ref.shape[0]
    half = slice_rows // 2
    chunks = 4
    c_rows = rows // chunks
    n_tile = 512
    y_cols = ytile.shape[2]
    dp, z, cp = lax.axis_index("dp"), lax.axis_index("tp"), lax.axis_index("cp")
    is_end = (z == 0) | (z == 3)
    is_mid = (z == 1) | (z == 2)
    core = {"cp": cp + 1 - 2 * lax.rem(cp, 2)}
    ynb = {"cp": lax.rem(cp + 2, 4)}
    xnb = {"dp": 1 - dp}
    left = {"tp": jnp.maximum(z - 1, 0)}
    right = {"tp": jnp.minimum(z + 1, 3)}
    p_own = dp * 4 + cp
    p_x = (1 - dp) * 4 + cp
    p_y = dp * 4 + lax.rem(cp + 2, 4)
    p_d = (1 - dp) * 4 + lax.rem(cp + 2, 4)
    p_core = dp * 4 + cp + 1 - 2 * lax.rem(cp, 2)
    low_side = z < 2
    s1 = jnp.where(low_side, 1 - z, 5 - z)
    s2 = jnp.where(low_side, 2, 1)
    s3 = jnp.where(low_side, 3, 0)

    def remote(src, dst, ssem, rsem, dev):
        return pltpu.make_async_remote_copy(src_ref=src, dst_ref=dst, send_sem=ssem, recv_sem=rsem, device_id=dev, device_id_type=MESH)

    barrier = pltpu.get_barrier_semaphore()
    for dev in (core, ynb, xnb):
        pl.semaphore_signal(barrier, inc=1, device_id=dev, device_id_type=MESH)

    @pl.when(z > 0)
    def _():
        pl.semaphore_signal(barrier, inc=1, device_id=left, device_id_type=MESH)

    @pl.when(z < 3)
    def _():
        pl.semaphore_signal(barrier, inc=1, device_id=right, device_id_type=MESH)

    def w_at(j, p, start=0, n=None):
        n = slice_rows if n is None else n
        return wbuf.at[j, pl.ds(pl.multiple_of(p * slice_rows + start, half), n)]

    def load_w(src, j):
        return pltpu.make_async_copy(src, w_at(j, p_own), load_sem.at[j])

    sources = ((fr_ref, fr2_ref, None), (fl_ref, fr_ref, fr2_ref), (fr_ref, fl_ref, fl2_ref), (fl_ref, fl2_ref, None))
    o_load = pltpu.make_async_copy(o_ref, obuf.at[z], load_sem.at[3])
    o_load.start()
    for zz in range(4):
        @pl.when(z == zz)
        def _(zz=zz):
            for j in range(3):
                if sources[zz][j] is not None:
                    load_w(sources[zz][j], j).start()

    @pl.when(is_end)
    def _():
        pl.semaphore_wait(barrier, 4)

    @pl.when(is_mid)
    def _():
        pl.semaphore_wait(barrier, 5)

    def w_copy(j, kind):
        dev = (xnb, ynb, core, ynb, xnb, core, core, core, core)[kind]
        src = (w_at(j, p_own), w_at(j, p_own), w_at(j, p_own), w_at(j, p_x, 0, half), w_at(j, p_y, half, half),
               w_at(j, p_x), w_at(j, p_y), w_at(j, p_d, 0, half), w_at(j, p_d, half, half))[kind]
        return remote(src, src, wsend.at[j, kind], wrecv.at[j, kind], dev)

    def core_p(p):
        return p + 1 - 2 * lax.rem(p, 2)

    def w_wait(j, kind):
        dst = (w_at(j, p_x), w_at(j, p_y), w_at(j, p_core), w_at(j, p_d, 0, half), w_at(j, p_d, half, half),
               w_at(j, core_p(p_x)), w_at(j, core_p(p_y)), w_at(j, core_p(p_d), 0, half), w_at(j, core_p(p_d), half, half))[kind]
        remote(dst, dst, wsend.at[j, kind], wrecv.at[j, kind], core).wait_recv()

    def spread_own(j):
        for kind in (0, 1, 2):
            w_copy(j, kind).start()

    def spread_relay(j):
        w_wait(j, 0)
        w_copy(j, 3).start()
        w_copy(j, 5).start()
        w_wait(j, 1)
        w_copy(j, 4).start()
        w_copy(j, 6).start()

    def spread_diag(j):
        w_wait(j, 3)
        w_copy(j, 7).start()
        w_wait(j, 4)
        w_copy(j, 8).start()

    def spread_done(j):
        for kind in (2, 5, 6, 7, 8):
            w_wait(j, kind)

    def o_at(s, c):
        return obuf.at[s, pl.ds(pl.multiple_of(c * c_rows, c_rows), c_rows)]

    def o_own(c, side):
        return remote(o_at(z, c), o_at(z, c), own_send.at[side, c], o_recv.at[z, c], (left, right)[side])

    def o_fwd(s, c, side):
        return remote(o_at(s, c), o_at(s, c), fwd_send.at[s, c], o_recv.at[s, c], (left, right)[side])

    def o_wait(s, c):
        remote(o_at(s, c), o_at(s, c), fwd_send.at[s, c], o_recv.at[s, c], left).wait_recv()

    def o_pass(s, c):
        o_wait(s, c)

        @pl.when(s < z)
        def _():
            o_fwd(s, c, 1).start()

        @pl.when(s > z)
        def _():
            o_fwd(s, c, 0).start()

    w3 = remote(w_at(2, p_own), w_at(2, p_own), w3_send, w3_recv, {"tp": jnp.where(z == 1, 0, 3)})

    @pl.when(is_mid)
    def _():
        load_w(fl_ref, 2).wait()
        w3.start()

    o_load.wait()
    for c in range(chunks):
        @pl.when(z > 0)
        def _(c=c):
            o_own(c, 0).start()

        @pl.when(z < 3)
        def _(c=c):
            o_own(c, 1).start()

    for j in range(2):
        load_w(fl_ref, j).wait()
        spread_own(j)

    def tile_loads(n, slot):
        at = pl.ds(pl.multiple_of(n * n_tile, n_tile), n_tile)
        return (pltpu.make_async_copy(wown_ref.at[:, at], wtile.at[slot], tile_sem.at[0, slot]),
                pltpu.make_async_copy(x_ref.at[:, at], xtile.at[slot], tile_sem.at[1, slot]))

    n_steps = width // n_tile
    for cpy in tile_loads(0, 0):
        cpy.start()

    def own_step(n, _):
        slot = lax.rem(n, 2)

        @pl.when(n + 1 < n_steps)
        def _():
            for cpy in tile_loads(n + 1, 1 - slot):
                cpy.start()

        for cpy in tile_loads(n, slot):
            cpy.wait()
        at = pl.ds(pl.multiple_of(n * n_tile, n_tile), n_tile)
        acc[:, at] = xtile[slot].astype(F32) + jnp.dot(obuf[z], wtile[slot], preferred_element_type=F32)
        return 0

    lax.fori_loop(0, n_steps, own_step, 0)

    def add_shard(j, s):
        def step(n, _):
            at = pl.ds(pl.multiple_of(n * n_tile, n_tile), n_tile)
            acc[:, at] += jnp.dot(obuf[s], wbuf[j, :, at], preferred_element_type=F32)
            return 0

        lax.fori_loop(0, n_steps, step, 0)

    spread_relay(0)
    spread_relay(1)

    @pl.when(is_end)
    def _():
        remote(w_at(2, p_own), w_at(2, p_own), w3_send, w3_recv, left).wait_recv()

    spread_own(2)

    @pl.when(is_mid)
    def _():
        for c in range(chunks):
            o_pass(s1, c)
            o_pass(s2, c)

    spread_diag(0)
    spread_done(0)

    @pl.when(is_end)
    def _():
        for c in range(chunks):
            o_wait(s1, c)

    add_shard(0, s1)
    spread_diag(1)
    spread_done(1)

    @pl.when(is_mid)
    def _():
        for c in range(chunks):
            o_pass(s3, c)

    spread_relay(2)

    @pl.when(is_end)
    def _():
        for c in range(chunks):
            o_wait(s2, c)

    add_shard(1, s2)
    spread_diag(2)
    spread_done(2)

    y_steps = width // y_cols

    def y_copy(i):
        slot = lax.rem(i, 2)
        r_at = pl.ds(pl.multiple_of((i // y_steps) * c_rows, c_rows), c_rows)
        n_at = pl.ds(pl.multiple_of(lax.rem(i, y_steps) * y_cols, y_cols), y_cols)
        return pltpu.make_async_copy(ytile.at[slot], y_ref.at[r_at, n_at], y_sem.at[slot])

    def last_step(i, _):
        c = i // y_steps

        @pl.when(is_end & (lax.rem(i, y_steps) == 0))
        def _():
            o_wait(s3, c)

        @pl.when(i >= 2)
        def _():
            y_copy(i - 2).wait()

        r_at = pl.ds(pl.multiple_of(c * c_rows, c_rows), c_rows)
        n_at = pl.ds(pl.multiple_of(lax.rem(i, y_steps) * y_cols, y_cols), y_cols)
        ytile[lax.rem(i, 2)] = (acc[r_at, n_at] + jnp.dot(obuf[s3, r_at, :], wbuf[2, :, n_at], preferred_element_type=F32)).astype(BF16)
        y_copy(i).start()
        return 0

    total = chunks * y_steps
    lax.fori_loop(0, total, last_step, 0)
    y_copy(total - 2).wait()
    y_copy(total - 1).wait()

    for j in range(3):
        for kind in range(9):
            w_copy(j, kind).wait_send()
    for c in range(chunks):
        @pl.when(z > 0)
        def _(c=c):
            o_own(c, 0).wait_send()

        @pl.when(z < 3)
        def _(c=c):
            o_own(c, 1).wait_send()

    @pl.when(is_mid)
    def _():
        w3.wait_send()
        for c in range(chunks):
            for s in (s1, s2, s3):
                o_fwd(s, c, 0).wait_send()


def out_proj(o, fl, fr, fl2, fr2, w_own, x):
    rows, kdim = o.shape
    width = x.shape[1]
    dma = pltpu.SemaphoreType.DMA
    return pl.pallas_call(
        out_kernel,
        in_specs=[pl.BlockSpec(memory_space=HBM)] * 7,
        out_specs=pl.BlockSpec(memory_space=HBM),
        out_shape=jax.ShapeDtypeStruct((rows, width), BF16),
        scratch_shapes=[
            VMEM((3, kdim, width), BF16),
            VMEM((2, kdim, 512), BF16),
            VMEM((2, rows, 512), BF16),
            VMEM((4, rows, kdim), BF16),
            VMEM((rows, width), F32),
            VMEM((2, rows // 4, 1024), BF16),
            dma((4,)), dma((2, 2)), dma((2,)), dma((3, 9)), dma((3, 9)), dma, dma,
            dma((2, 4)), dma((4, 4)), dma((4, 4)),
        ],
        compiler_params=pltpu.CompilerParams(collective_id=1, has_side_effects=True, vmem_limit_bytes=62 << 20),
        name="out_proj",
    )(o, fl, fr, fl2, fr2, w_own, x)


def solution(mesh):
    def local_step(x_in, doc_id, pos_in_doc, norm_gain, w_q, w_k, w_v, w_o, inv_freq):
        rows = x_in.shape[0]
        piece = rows // 2
        dp, cp = lax.axis_index("dp"), lax.axis_index("cp")
        n_cp = 4
        slice_rows = w_o.shape[0] // 8
        w_slice = lax.dynamic_slice(w_o, ((dp * 4 + cp) * slice_rows, 0), (slice_rows, w_o.shape[1]))
        fl = lax.ppermute(w_slice, "tp", [(0, 1), (1, 2), (2, 3)])
        fr = lax.ppermute(w_slice, "tp", [(1, 0), (2, 1), (3, 2)])

        angle = pos_in_doc.astype(F32)[:, None] * inv_freq[None, :]
        cos_h, sin_h = jnp.cos(angle), jnp.sin(angle)
        cos_t = jnp.concatenate([cos_h, cos_h], axis=-1)
        sin_t = jnp.concatenate([-sin_h, sin_h], axis=-1)
        h, kv = norm_kv(x_in, norm_gain, w_k, w_v, cos_t, sin_t)
        kv_y = lax.ppermute(kv, "cp", [(0, 2), (1, 3), (2, 0), (3, 1)])
        kv_c = lax.ppermute(kv, "cp", [(0, 1), (1, 0), (2, 3), (3, 2)])
        q = q_proj(h, w_q, cos_t, sin_t)
        fl2 = lax.ppermute(fl, "tp", [(1, 2), (2, 3)])
        fr2 = lax.ppermute(fr, "tp", [(1, 0), (2, 1)])
        kv_yc = lax.ppermute(kv_y, "cp", [(0, 1), (1, 0), (2, 3), (3, 2)])

        loc = jnp.arange(rows)
        tok = jnp.where(loc < piece, cp * piece + loc, (2 * n_cp - 1 - cp) * piece + loc - piece).astype(jnp.int32)
        o = attention(q, [kv, kv_c, kv_y, kv_yc], tok, pos_in_doc, cp)
        y = out_proj(o, fl, fr, fl2, fr2, w_o, x_in)
        cols = w_k.shape[1]
        k_out = kv[:, :cols].reshape(rows, cols // HEAD, HEAD)
        v_out = kv[:, cols:].reshape(rows, cols // HEAD, HEAD)
        return y, k_out, v_out

    row_spec = P(("dp", "cp"))
    in_specs = (P(("dp", "cp"), None), row_spec, row_spec, P(), P(None, "tp"), P(None, "tp"), P(None, "tp"), P("tp", None), P())
    out_specs = (P(("dp", "cp"), None), P(("dp", "cp"), "tp", None), P(("dp", "cp"), "tp", None))
    return jax.shard_map(local_step, mesh=mesh, in_specs=in_specs, out_specs=out_specs, check_vma=False)
```

```python
import functools

import jax
import jax.numpy as jnp
from jax import lax
from jax.experimental import pallas as pl
from jax.experimental.pallas import tpu as pltpu
from jax.sharding import PartitionSpec as P

MESH = pl.DeviceIdType.MESH
HBM = pltpu.HBM
VMEM = pltpu.VMEM
HEAD = 128
Q_TILE = 128
F32 = jnp.float32
BF16 = jnp.bfloat16


def rope(vec, cos_t, sin_t):
    vec = vec.astype(F32)
    return (vec * cos_t + pltpu.roll(vec, HEAD // 2, 1) * sin_t).astype(BF16)


def proj_kernel(x_ref, gain_ref, wk_ref, wv_ref, wq_ref, wo_ref, cos_ref, sin_ref,
                q_ref, kvg_ref, fla_ref, flb_ref, fra_ref, frb_ref, fl2_ref, fr2_ref,
                xbuf, hbuf, invbuf, wkbuf, wvbuf, wqbuf, kvbuf, qbuf,
                x_sem, w_sem, wq_sem, kvl_sem, q_sem, kv_send, kv_recv, r1_send, r1_recv, r2_send, r2_recv):
    chunks, q_tiles = 4, 4
    rows, width = hbuf.shape
    c_rows = rows // chunks
    piece = rows // 2
    cols = wkbuf.shape[1]
    q_cols = wqbuf.shape[2]
    half = fla_ref.shape[0]
    n_cp = 4
    dp, z, cp = lax.axis_index("dp"), lax.axis_index("tp"), lax.axis_index("cp")
    core_cp = cp + 1 - 2 * lax.rem(cp, 2)
    y_cp = lax.rem(cp + 2, 4)
    core, ynb = {"cp": core_cp}, {"cp": y_cp}
    left = {"tp": jnp.maximum(z - 1, 0)}
    right = {"tp": jnp.minimum(z + 1, 3)}
    is_mid = (z == 1) | (z == 2)

    def remote(src, dst, ssem, rsem, dev):
        return pltpu.make_async_remote_copy(src_ref=src, dst_ref=dst, send_sem=ssem, recv_sem=rsem, device_id=dev, device_id_type=MESH)

    barrier = pltpu.get_barrier_semaphore()
    for dev in (core, ynb):
        pl.semaphore_signal(barrier, inc=1, device_id=dev, device_id_type=MESH)

    @pl.when(z > 0)
    def _():
        pl.semaphore_signal(barrier, inc=1, device_id=left, device_id_type=MESH)

    @pl.when(z < 3)
    def _():
        pl.semaphore_signal(barrier, inc=1, device_id=right, device_id_type=MESH)

    def x_load(c):
        return pltpu.make_async_copy(x_ref.at[pl.ds(c * c_rows, c_rows)], xbuf.at[c], x_sem.at[c])

    def wq_load(t):
        return pltpu.make_async_copy(wq_ref.at[:, pl.ds(t * q_cols, q_cols)], wqbuf.at[t], wq_sem.at[t])

    wk_load = pltpu.make_async_copy(wk_ref, wkbuf, w_sem.at[0])
    wv_load = pltpu.make_async_copy(wv_ref, wvbuf, w_sem.at[1])
    x_load(0).start()
    wk_load.start()
    wv_load.start()
    for c in range(1, chunks):
        x_load(c).start()
    for t in range(q_tiles):
        wq_load(t).start()

    @pl.when(is_mid)
    def _():
        pl.semaphore_wait(barrier, 4)

    @pl.when(jnp.logical_not(is_mid))
    def _():
        pl.semaphore_wait(barrier, 3)

    p_own = dp * 4 + cp

    def r1(side, part):
        src = wo_ref.at[pl.ds(pl.multiple_of((p_own * 2 + part) * half, half), half)]
        dst = ((fra_ref, frb_ref), (fla_ref, flb_ref))[side][part]
        return remote(src, dst, r1_send.at[side, part], r1_recv.at[side, part], (left, right)[side])

    def r2(side):
        src = (fra_ref, fla_ref)[side]
        dst = (fr2_ref, fl2_ref)[side]
        return remote(src, dst, r2_send.at[side], r2_recv.at[side], (left, right)[side])

    for part in range(2):
        @pl.when(z > 0)
        def _(part=part):
            r1(0, part).start()

        @pl.when(z < 3)
        def _(part=part):
            r1(1, part).start()

    def kv_at(owner, c):
        start = jnp.where(c < chunks // 2, owner, 2 * n_cp - 1 - owner) * piece + (c % (chunks // 2)) * c_rows
        return kvg_ref.at[pl.ds(pl.multiple_of(start, c_rows), c_rows)]

    def kv_local(c):
        return pltpu.make_async_copy(kvbuf.at[pl.ds(c * c_rows, c_rows)], kv_at(cp, c), kvl_sem.at[c])

    def kv_copy(kind, c):
        at = kv_at((cp, cp, y_cp)[kind], c)
        return remote(at, at, kv_send.at[kind, c], kv_recv.at[kind, c], (ynb, core, core)[kind])

    def kv_wait(kind, c):
        at = kv_at((y_cp, core_cp, lax.rem(core_cp + 2, 4))[kind], c)
        remote(at, at, kv_send.at[kind, c], kv_recv.at[kind, c], core).wait_recv()

    def kv_out(c):
        kv_local(c).wait()
        kv_copy(0, c).start()
        kv_copy(1, c).start()

    step = 16

    def full(t):
        return jnp.concatenate([t, t], axis=-1)

    def turn(vec, r_at):
        cos_h, sin_h = cos_ref[r_at, :], sin_ref[r_at, :]
        return rope(vec, full(cos_h), jnp.concatenate([-sin_h, sin_h], axis=-1))

    for c in range(chunks):
        x_load(c).wait()

        def square_rows(i, _, c=c):
            at = pl.ds(pl.multiple_of(i * step, step), step)
            xf = xbuf[c, at, :].astype(F32)
            mean = jnp.sum(xf * xf, axis=-1, keepdims=True) * (1.0 / width)
            invbuf[at, :] = jnp.broadcast_to(lax.rsqrt(mean + 1e-5), (step, HEAD))
            return 0

        def norm_rows(i, _, c=c):
            at = pl.ds(pl.multiple_of(i * step, step), step)
            to = pl.ds(pl.multiple_of(c * c_rows + i * step, step), step)
            inv = invbuf[at, 0:1]
            hbuf[to, :] = (xbuf[c, at, :].astype(F32) * inv * gain_ref[...]).astype(BF16)
            return 0

        lax.fori_loop(0, c_rows // step, square_rows, 0, unroll=4)
        lax.fori_loop(0, c_rows // step, norm_rows, 0, unroll=2)
        if c == 0:
            wk_load.wait()
            wv_load.wait()
        r_at = pl.ds(c * c_rows, c_rows)
        h = hbuf[r_at, :]
        k_new = jnp.dot(h, wkbuf[...], preferred_element_type=F32).astype(BF16)
        v_new = jnp.dot(h, wvbuf[...], preferred_element_type=F32).astype(BF16)
        for j in range(cols // HEAD):
            kvbuf[r_at, j * HEAD:(j + 1) * HEAD] = turn(k_new[:, j * HEAD:(j + 1) * HEAD], r_at)
        kvbuf[r_at, cols:] = v_new
        kv_local(c).start()
        if c > 0:
            kv_out(c - 1)

    @pl.when(z > 0)
    def _():
        r1(1, 0).wait_recv()

    @pl.when(z < 3)
    def _():
        r1(0, 0).wait_recv()

    @pl.when(is_mid)
    def _():
        r2(0).start()
        r2(1).start()

    def q_out(t):
        return pltpu.make_async_copy(qbuf.at[t], q_ref.at[:, pl.ds(t * q_cols, q_cols)], q_sem.at[t])

    def q_tile(t):
        wq_load(t).wait()
        q_new = jnp.dot(hbuf[...], wqbuf[t], preferred_element_type=F32).astype(BF16)
        everything = pl.ds(0, rows)
        for j in range(q_cols // HEAD):
            qbuf[t, :, j * HEAD:(j + 1) * HEAD] = turn(q_new[:, j * HEAD:(j + 1) * HEAD], everything)
        q_out(t).start()

    q_tile(0)
    kv_out(chunks - 1)
    q_tile(1)
    for c in range(2):
        kv_wait(0, c)
        kv_copy(2, c).start()
    q_tile(2)
    q_tile(3)
    for c in range(2, chunks):
        kv_wait(0, c)
        kv_copy(2, c).start()
    for c in range(chunks):
        kv_wait(1, c)
        kv_wait(2, c)
    for t in range(q_tiles):
        q_out(t).wait()

    @pl.when(z > 0)
    def _():
        r1(1, 1).wait_recv()
        for part in range(2):
            r1(0, part).wait_send()

    @pl.when(z < 3)
    def _():
        r1(0, 1).wait_recv()
        for part in range(2):
            r1(1, part).wait_send()

    @pl.when(z > 1)
    def _():
        r2(1).wait_recv()

    @pl.when(z < 2)
    def _():
        r2(0).wait_recv()

    @pl.when(is_mid)
    def _():
        r2(0).wait_send()
        r2(1).wait_send()

    for c in range(chunks):
        for kind in range(3):
            kv_copy(kind, c).wait_send()


def project(x, gain, w_k, w_v, w_q, w_o, cos_h, sin_h):
    rows, width = x.shape
    cols = w_k.shape[1]
    q_cols = w_q.shape[1]
    half = w_o.shape[0] // 16
    dma = pltpu.SemaphoreType.DMA
    out = jax.ShapeDtypeStruct
    hbm = pl.BlockSpec(memory_space=HBM)
    vmem = pl.BlockSpec(memory_space=VMEM)
    return pl.pallas_call(
        proj_kernel,
        in_specs=[hbm, vmem, hbm, hbm, hbm, hbm, vmem, vmem],
        out_specs=[hbm] * 8,
        out_shape=[out((rows, q_cols), BF16), out((4 * rows, 2 * cols), BF16)] + [out((half, w_o.shape[1]), BF16)] * 6,
        scratch_shapes=[
            VMEM((4, rows // 4, width), BF16),
            VMEM((rows, width), BF16),
            VMEM((rows // 4, HEAD), F32),
            VMEM((width, cols), BF16),
            VMEM((width, cols), BF16),
            VMEM((4, width, q_cols // 4), BF16),
            VMEM((rows, 2 * cols), BF16),
            VMEM((4, rows, q_cols // 4), BF16),
            dma((4,)), dma((2,)), dma((4,)), dma((4,)), dma((4,)),
            dma((3, 4)), dma((3, 4)), dma((2, 2)), dma((2, 2)), dma((2,)), dma((2,)),
        ],
        compiler_params=pltpu.CompilerParams(collective_id=0, has_side_effects=True, vmem_limit_bytes=48 << 20),
        cost_estimate=pl.CostEstimate(flops=2 * rows * width * (2 * cols + q_cols), bytes_accessed=24 << 20, transcendentals=0),
        name="proj",
    )(x, gain.reshape(1, width), w_k, w_v, w_q, w_o, cos_h, sin_h)


def attn_kernel(group, pos_smem, q_ref, pos_ref, kv_ref, o_ref):
    head, blk = pl.program_id(0), pl.program_id(1)
    half_blks = pl.num_programs(1) // 2
    piece = half_blks * Q_TILE
    cp = lax.axis_index("cp")
    q_rows = q_ref.shape[0]
    kv_cols = kv_ref.shape[1] // 2
    q = jnp.concatenate([q_ref[:, g * HEAD:(g + 1) * HEAD] for g in range(group)], axis=0)
    pieces = kv_ref.shape[0] // piece
    g0 = jnp.where(blk < half_blks, cp * piece + blk * Q_TILE, (pieces - 1 - cp) * piece + (blk - half_blks) * Q_TILE)
    low = (g0 - pos_smem[blk * Q_TILE]) // Q_TILE
    tok_1 = g0 + lax.broadcasted_iota(jnp.int32, (q_rows, 1), 0)
    tok = jnp.concatenate([tok_1] * group, axis=0)
    first = jnp.concatenate([tok_1 - pos_ref[...]] * group, axis=0)
    scale = HEAD ** -0.5
    k_at = pl.ds(pl.multiple_of(head * HEAD, HEAD), HEAD)
    v_at = pl.ds(pl.multiple_of(kv_cols + head * HEAD, HEAD), HEAD)

    def scores(start, width):
        keys = kv_ref[pl.ds(pl.multiple_of(start, Q_TILE), width), k_at]
        s = lax.dot_general(q, keys, (((1,), (1,)), ((), ())), preferred_element_type=F32) * scale
        u = start + lax.broadcasted_iota(jnp.int32, (1, width), 1)
        return jnp.where((u >= first) & (u <= tok), s, -1e30)

    def values(start, width):
        return kv_ref[pl.ds(pl.multiple_of(start, Q_TILE), width), v_at]

    near = jnp.maximum(g0 - Q_TILE, 0)
    s = scores(near, 2 * Q_TILE)
    m = jnp.max(s, axis=-1, keepdims=True)
    p = jnp.exp(s - m)
    total = jnp.sum(p, axis=-1, keepdims=True)
    acc = jnp.dot(p.astype(BF16), values(near, 2 * Q_TILE), preferred_element_type=F32)

    def far(i, carry):
        m, total, acc = carry
        start = i * Q_TILE
        s = scores(start, Q_TILE)
        m_new = jnp.maximum(m, jnp.max(s, axis=-1, keepdims=True))
        old = jnp.exp(m - m_new)
        p = jnp.exp(s - m_new)
        total = total * old + jnp.sum(p, axis=-1, keepdims=True)
        acc = acc * old + jnp.dot(p.astype(BF16), values(start, Q_TILE), preferred_element_type=F32)
        return m_new, total, acc

    m, total, acc = lax.fori_loop(low, near // Q_TILE, far, (m, total, acc))
    out = (acc / total).astype(BF16)
    for g in range(group):
        o_ref[:, g * HEAD:(g + 1) * HEAD] = out[g * q_rows:(g + 1) * q_rows]


def attention(q, kvg, pos):
    rows, q_cols = q.shape
    kv_cols = kvg.shape[1] // 2
    heads = kv_cols // HEAD
    group = q_cols // kv_cols
    q_map = lambda h, i, *_: (i, h)
    return pl.pallas_call(
        functools.partial(attn_kernel, group),
        grid_spec=pltpu.PrefetchScalarGridSpec(
            num_scalar_prefetch=1,
            grid=(heads, rows // Q_TILE),
            in_specs=[
                pl.BlockSpec((Q_TILE, group * HEAD), q_map),
                pl.BlockSpec((Q_TILE, 1), lambda h, i, *_: (i, 0)),
                pl.BlockSpec(kvg.shape, lambda h, i, *_: (0, 0)),
            ],
            out_specs=pl.BlockSpec((Q_TILE, group * HEAD), q_map),
        ),
        out_shape=jax.ShapeDtypeStruct((rows, q_cols), BF16),
        compiler_params=pltpu.CompilerParams(vmem_limit_bytes=32 << 20),
        cost_estimate=pl.CostEstimate(flops=5 << 30, bytes_accessed=8 << 20, transcendentals=0),
        name="attn",
    )(pos, q, pos[:, None], kvg)


def out_kernel(o_ref, fla_ref, flb_ref, fra_ref, frb_ref, fl2a_ref, fl2b_ref, fr2a_ref, fr2b_ref, wown_ref, x_ref, y_ref,
               wbuf, wtile, xtile, obuf, acc, ytile,
               load_sem, tile_sem, y_sem, wsend, wrecv, w3_send, w3_recv, own_send, fwd_send, o_recv):
    rows, kdim = o_ref.shape
    width = x_ref.shape[1]
    half = fla_ref.shape[0]
    slice_rows = 2 * half
    chunks = 4
    c_rows = rows // chunks
    n_tile = 512
    y_cols = ytile.shape[2]
    dp, z, cp = lax.axis_index("dp"), lax.axis_index("tp"), lax.axis_index("cp")
    is_end = (z == 0) | (z == 3)
    is_mid = (z == 1) | (z == 2)
    core = {"cp": cp + 1 - 2 * lax.rem(cp, 2)}
    ynb = {"cp": lax.rem(cp + 2, 4)}
    xnb = {"dp": 1 - dp}
    left = {"tp": jnp.maximum(z - 1, 0)}
    right = {"tp": jnp.minimum(z + 1, 3)}
    p_own = dp * 4 + cp
    p_x = (1 - dp) * 4 + cp
    p_y = dp * 4 + lax.rem(cp + 2, 4)
    p_d = (1 - dp) * 4 + lax.rem(cp + 2, 4)
    p_core = dp * 4 + cp + 1 - 2 * lax.rem(cp, 2)
    low_side = z < 2
    s1 = jnp.where(low_side, 1 - z, 5 - z)
    s2 = jnp.where(low_side, 2, 1)
    s3 = jnp.where(low_side, 3, 0)

    def remote(src, dst, ssem, rsem, dev):
        return pltpu.make_async_remote_copy(src_ref=src, dst_ref=dst, send_sem=ssem, recv_sem=rsem, device_id=dev, device_id_type=MESH)

    barrier = pltpu.get_barrier_semaphore()
    for dev in (core, ynb, xnb):
        pl.semaphore_signal(barrier, inc=1, device_id=dev, device_id_type=MESH)

    @pl.when(z > 0)
    def _():
        pl.semaphore_signal(barrier, inc=1, device_id=left, device_id_type=MESH)

    @pl.when(z < 3)
    def _():
        pl.semaphore_signal(barrier, inc=1, device_id=right, device_id_type=MESH)

    def w_at(j, p, start=0, n=None):
        n = slice_rows if n is None else n
        return wbuf.at[j, pl.ds(pl.multiple_of(p * slice_rows + start, half), n)]

    def load_w(src, j, part):
        return pltpu.make_async_copy(src, w_at(j, p_own, part * half, half), load_sem.at[j, part])

    fl, fr, fl2, fr2 = (fla_ref, flb_ref), (fra_ref, frb_ref), (fl2a_ref, fl2b_ref), (fr2a_ref, fr2b_ref)
    sources = ((fr, fr2, None), (fl, fr, fr2), (fr, fl, fl2), (fl, fl2, None))
    for zz in range(4):
        @pl.when(z == zz)
        def _(zz=zz):
            for j in range(3):
                if sources[zz][j] is not None:
                    for part in range(2):
                        load_w(sources[zz][j][part], j, part).start()

    @pl.when(is_end)
    def _():
        pl.semaphore_wait(barrier, 4)

    @pl.when(is_mid)
    def _():
        pl.semaphore_wait(barrier, 5)

    def w_copy(j, kind):
        dev = (xnb, ynb, core, ynb, xnb, core, core, core, core)[kind]
        src = (w_at(j, p_own), w_at(j, p_own), w_at(j, p_own), w_at(j, p_x, 0, half), w_at(j, p_y, half, half),
               w_at(j, p_x), w_at(j, p_y), w_at(j, p_d, 0, half), w_at(j, p_d, half, half))[kind]
        return remote(src, src, wsend.at[j, kind], wrecv.at[j, kind], dev)

    def core_p(p):
        return p + 1 - 2 * lax.rem(p, 2)

    def w_wait(j, kind):
        dst = (w_at(j, p_x), w_at(j, p_y), w_at(j, p_core), w_at(j, p_d, 0, half), w_at(j, p_d, half, half),
               w_at(j, core_p(p_x)), w_at(j, core_p(p_y)), w_at(j, core_p(p_d), 0, half), w_at(j, core_p(p_d), half, half))[kind]
        remote(dst, dst, wsend.at[j, kind], wrecv.at[j, kind], core).wait_recv()

    def spread_own(j):
        for kind in (0, 1, 2):
            w_copy(j, kind).start()

    def spread_relay(j):
        w_wait(j, 0)
        w_copy(j, 3).start()
        w_copy(j, 5).start()
        w_wait(j, 1)
        w_copy(j, 4).start()
        w_copy(j, 6).start()

    def spread_diag(j):
        w_wait(j, 3)
        w_copy(j, 7).start()
        w_wait(j, 4)
        w_copy(j, 8).start()

    def spread_done(j):
        for kind in (2, 5, 6, 7, 8):
            w_wait(j, kind)

    def slot_of(s, dev_z):
        return s - (s > dev_z).astype(jnp.int32)

    def o_at(s, c, dev_z=None):
        return obuf.at[slot_of(s, z if dev_z is None else dev_z), pl.ds(pl.multiple_of(c * c_rows, c_rows), c_rows)]

    def o_own(c, side):
        src = o_ref.at[pl.ds(c * c_rows, c_rows)]
        return remote(src, o_at(z, c, z + (-1, 1)[side]), own_send.at[side, c], o_recv.at[z, c], (left, right)[side])

    def o_fwd(s, c, side):
        return remote(o_at(s, c), o_at(s, c, z + (-1, 1)[side]), fwd_send.at[s, c], o_recv.at[s, c], (left, right)[side])

    def o_wait(s, c):
        remote(o_at(s, c), o_at(s, c), fwd_send.at[s, c], o_recv.at[s, c], left).wait_recv()

    def o_pass(s, c):
        o_wait(s, c)

        @pl.when(s < z)
        def _():
            o_fwd(s, c, 1).start()

        @pl.when(s > z)
        def _():
            o_fwd(s, c, 0).start()

    w3 = remote(w_at(2, p_own), w_at(2, p_own), w3_send, w3_recv, {"tp": jnp.where(z == 1, 0, 3)})

    @pl.when(is_mid)
    def _():
        for part in range(2):
            load_w(fla_ref, 2, part).wait()
        w3.start()

    for c in range(chunks):
        @pl.when(z > 0)
        def _(c=c):
            o_own(c, 0).start()

        @pl.when(z < 3)
        def _(c=c):
            o_own(c, 1).start()

    for j in range(2):
        for part in range(2):
            load_w(fla_ref, j, part).wait()
        spread_own(j)

    def tile_loads(n, slot):
        at = pl.ds(pl.multiple_of(n * n_tile, n_tile), n_tile)
        return (pltpu.make_async_copy(wown_ref.at[:, at], wtile.at[slot], tile_sem.at[0, slot]),
                pltpu.make_async_copy(x_ref.at[:, at], xtile.at[slot], tile_sem.at[1, slot]))

    n_steps = width // n_tile
    for cpy in tile_loads(0, 0):
        cpy.start()

    def own_step(n, _):
        slot = lax.rem(n, 2)

        @pl.when(n + 1 < n_steps)
        def _():
            for cpy in tile_loads(n + 1, 1 - slot):
                cpy.start()

        for cpy in tile_loads(n, slot):
            cpy.wait()
        at = pl.ds(pl.multiple_of(n * n_tile, n_tile), n_tile)
        acc[:, at] = xtile[slot].astype(F32) + jnp.dot(o_ref[...], wtile[slot], preferred_element_type=F32)
        return 0

    lax.fori_loop(0, n_steps, own_step, 0)

    def add_shard(j, s):
        def step(n, _):
            at = pl.ds(pl.multiple_of(n * n_tile, n_tile), n_tile)
            acc[:, at] += jnp.dot(obuf[slot_of(s, z)], wbuf[j, :, at], preferred_element_type=F32)
            return 0

        lax.fori_loop(0, n_steps, step, 0)

    spread_relay(0)
    spread_relay(1)

    @pl.when(is_end)
    def _():
        remote(w_at(2, p_own), w_at(2, p_own), w3_send, w3_recv, left).wait_recv()

    spread_own(2)

    @pl.when(is_mid)
    def _():
        for c in range(chunks):
            o_pass(s1, c)
            o_pass(s2, c)

    spread_diag(0)
    spread_done(0)

    @pl.when(is_end)
    def _():
        for c in range(chunks):
            o_wait(s1, c)

    add_shard(0, s1)
    spread_diag(1)
    spread_done(1)

    @pl.when(is_mid)
    def _():
        for c in range(chunks):
            o_pass(s3, c)

    spread_relay(2)

    @pl.when(is_end)
    def _():
        for c in range(chunks):
            o_wait(s2, c)

    add_shard(1, s2)
    spread_diag(2)
    spread_done(2)

    y_steps = width // y_cols

    def y_copy(i):
        slot = lax.rem(i, 2)
        r_at = pl.ds(pl.multiple_of((i // y_steps) * c_rows, c_rows), c_rows)
        n_at = pl.ds(pl.multiple_of(lax.rem(i, y_steps) * y_cols, y_cols), y_cols)
        return pltpu.make_async_copy(ytile.at[slot], y_ref.at[r_at, n_at], y_sem.at[slot])

    def last_step(i, _):
        c = i // y_steps

        @pl.when(is_end & (lax.rem(i, y_steps) == 0))
        def _():
            o_wait(s3, c)

        @pl.when(i >= 2)
        def _():
            y_copy(i - 2).wait()

        r_at = pl.ds(pl.multiple_of(c * c_rows, c_rows), c_rows)
        n_at = pl.ds(pl.multiple_of(lax.rem(i, y_steps) * y_cols, y_cols), y_cols)
        ytile[lax.rem(i, 2)] = (acc[r_at, n_at] + jnp.dot(obuf[slot_of(s3, z), r_at, :], wbuf[2, :, n_at], preferred_element_type=F32)).astype(BF16)
        y_copy(i).start()
        return 0

    total = chunks * y_steps
    lax.fori_loop(0, total, last_step, 0)
    y_copy(total - 2).wait()
    y_copy(total - 1).wait()

    for j in range(3):
        for kind in range(9):
            w_copy(j, kind).wait_send()
    for c in range(chunks):
        @pl.when(z > 0)
        def _(c=c):
            o_own(c, 0).wait_send()

        @pl.when(z < 3)
        def _(c=c):
            o_own(c, 1).wait_send()

    @pl.when(is_mid)
    def _():
        w3.wait_send()
        for c in range(chunks):
            for s in (s1, s2, s3):
                o_fwd(s, c, 0).wait_send()


def out_proj(o, slices, w_own, x):
    rows, kdim = o.shape
    width = x.shape[1]
    dma = pltpu.SemaphoreType.DMA
    return pl.pallas_call(
        out_kernel,
        in_specs=[pl.BlockSpec(memory_space=VMEM)] + [pl.BlockSpec(memory_space=HBM)] * 10,
        out_specs=pl.BlockSpec(memory_space=pl.ANY),
        out_shape=jax.ShapeDtypeStruct((rows, width), BF16),
        scratch_shapes=[
            VMEM((3, kdim, width), BF16),
            VMEM((2, kdim, 512), BF16),
            VMEM((2, rows, 512), BF16),
            VMEM((3, rows, kdim), BF16),
            VMEM((rows, width), F32),
            VMEM((2, rows // 4, 1024), BF16),
            dma((3, 2)), dma((2, 2)), dma((2,)), dma((3, 9)), dma((3, 9)), dma, dma,
            dma((2, 4)), dma((4, 4)), dma((4, 4)),
        ],
        compiler_params=pltpu.CompilerParams(collective_id=1, has_side_effects=True, vmem_limit_bytes=58 << 20),
        name="out_proj",
    )(o, *slices, w_own, x)


def solution(mesh):
    def local_step(x_in, doc_id, pos_in_doc, norm_gain, w_q, w_k, w_v, w_o, inv_freq):
        rows = x_in.shape[0]
        angle = pos_in_doc.astype(F32)[:, None] * inv_freq[None, :]
        q, kvg, fla, flb, fra, frb, fl2a, fr2a = project(x_in, norm_gain, w_k, w_v, w_q, w_o, jnp.cos(angle), jnp.sin(angle))
        fl2b = lax.ppermute(flb, "tp", [(1, 2), (2, 3)])
        fr2b = lax.ppermute(frb, "tp", [(1, 0), (2, 1)])
        o = attention(q, kvg, pos_in_doc)
        y = out_proj(o, (fla, flb, fra, frb, fl2a, fl2b, fr2a, fr2b), w_o, x_in)
        piece = rows // 2
        cp = lax.axis_index("cp")
        at = (cp * piece, (7 - cp) * piece)
        kv = jnp.concatenate([lax.dynamic_slice(kvg, (a, 0), (piece, kvg.shape[1])) for a in at])
        cols = w_k.shape[1]
        k_out = kv[:, :cols].reshape(rows, cols // HEAD, HEAD)
        v_out = kv[:, cols:].reshape(rows, cols // HEAD, HEAD)
        return y, k_out, v_out

    row_spec = P(("dp", "cp"))
    in_specs = (P(("dp", "cp"), None), row_spec, row_spec, P(), P(None, "tp"), P(None, "tp"), P(None, "tp"), P("tp", None), P())
    out_specs = (P(("dp", "cp"), None), P(("dp", "cp"), "tp", None), P(("dp", "cp"), "tp", None))
    return jax.shard_map(local_step, mesh=mesh, in_specs=in_specs, out_specs=out_specs, check_vma=False)
```

```python
import functools

import jax
import jax.numpy as jnp
from jax import lax
from jax.experimental import pallas as pl
from jax.experimental.pallas import tpu as pltpu
from jax.sharding import PartitionSpec as P

MESH = pl.DeviceIdType.MESH
HBM = pltpu.HBM
VMEM = pltpu.VMEM
HEAD = 128
Q_TILE = 128
VMEM_MAX = 67043328
F32 = jnp.float32
BF16 = jnp.bfloat16


def rope(vec, cos_t, sin_t):
    vec = vec.astype(F32)
    return (vec * cos_t + pltpu.roll(vec, HEAD // 2, 1) * sin_t).astype(BF16)


def proj_kernel(x_ref, gain_ref, wk_ref, wv_ref, wq_ref, wo_ref, pos_ref, freq_ref,
                q_ref, kvg_ref, k_ref, v_ref, fla_ref, flb_ref, fra_ref, frb_ref, far_ref,
                xbuf, hbuf, invbuf, gainbuf, posbuf, freqbuf, cosbuf, sinbuf, wkbuf, wvbuf, wqbuf, kvbuf, k3buf, v3buf, qbuf,
                x_sem, w_sem, wq_sem, kvl_sem, kv3_sem, q_sem, kv_send, kv_recv, r1_send, r1_recv, r2_send, r2_recv):
    chunks, q_tiles = 4, 4
    rows, width = hbuf.shape
    c_rows = rows // chunks
    piece = rows // 2
    cols = wkbuf.shape[1]
    q_cols = wqbuf.shape[2]
    half = fla_ref.shape[0]
    n_cp = 4
    dp, z, cp = lax.axis_index("dp"), lax.axis_index("tp"), lax.axis_index("cp")
    core_cp = cp + 1 - 2 * lax.rem(cp, 2)
    y_cp = lax.rem(cp + 2, 4)
    core, ynb = {"cp": core_cp}, {"cp": y_cp}
    left = {"tp": jnp.maximum(z - 1, 0)}
    right = {"tp": jnp.minimum(z + 1, 3)}
    is_mid = (z == 1) | (z == 2)

    def remote(src, dst, ssem, rsem, dev):
        return pltpu.make_async_remote_copy(src_ref=src, dst_ref=dst, send_sem=ssem, recv_sem=rsem, device_id=dev, device_id_type=MESH)

    barrier = pltpu.get_barrier_semaphore()
    for dev in (core, ynb):
        pl.semaphore_signal(barrier, inc=1, device_id=dev, device_id_type=MESH)

    @pl.when(z > 0)
    def _():
        pl.semaphore_signal(barrier, inc=1, device_id=left, device_id_type=MESH)

    @pl.when(z < 3)
    def _():
        pl.semaphore_signal(barrier, inc=1, device_id=right, device_id_type=MESH)

    def x_load(c):
        return pltpu.make_async_copy(x_ref.at[pl.ds(c * c_rows, c_rows)], xbuf.at[c], x_sem.at[c])

    def wq_load(t):
        return pltpu.make_async_copy(wq_ref.at[:, pl.ds(t * q_cols, q_cols)], wqbuf.at[t], wq_sem.at[t])

    wk_load = pltpu.make_async_copy(wk_ref, wkbuf, w_sem.at[0])
    wv_load = pltpu.make_async_copy(wv_ref, wvbuf, w_sem.at[1])
    small = [pltpu.make_async_copy(src, dst, w_sem.at[2 + i]) for i, (src, dst) in enumerate(((gain_ref, gainbuf), (pos_ref, posbuf), (freq_ref, freqbuf)))]
    for cpy in small:
        cpy.start()
    x_load(0).start()
    wk_load.start()
    wv_load.start()
    for c in range(1, chunks):
        x_load(c).start()
    for t in range(q_tiles):
        wq_load(t).start()

    @pl.when(is_mid)
    def _():
        pl.semaphore_wait(barrier, 4)

    @pl.when(jnp.logical_not(is_mid))
    def _():
        pl.semaphore_wait(barrier, 3)

    p_own = dp * 4 + cp

    def r1(side, part):
        src = wo_ref.at[pl.ds(pl.multiple_of((p_own * 2 + part) * half, half), half)]
        dst = ((fra_ref, frb_ref), (fla_ref, flb_ref))[side][part]
        return remote(src, dst, r1_send.at[side, part], r1_recv.at[side, part], (left, right)[side])

    def r2(side):
        src = (fra_ref, fla_ref)[side]
        return remote(src, far_ref, r2_send.at[side], r2_recv, (left, right)[side])

    for part in range(2):
        @pl.when(z > 0)
        def _(part=part):
            r1(0, part).start()

        @pl.when(z < 3)
        def _(part=part):
            r1(1, part).start()

    def kv_at(owner, c):
        start = jnp.where(c < chunks // 2, owner, 2 * n_cp - 1 - owner) * piece + (c % (chunks // 2)) * c_rows
        return kvg_ref.at[pl.ds(pl.multiple_of(start, c_rows), c_rows)]

    def kv_local(c):
        return pltpu.make_async_copy(kvbuf.at[pl.ds(c * c_rows, c_rows)], kv_at(cp, c), kvl_sem.at[c])

    def kv_copy(kind, c):
        at = kv_at((cp, cp, y_cp)[kind], c)
        return remote(at, at, kv_send.at[kind, c], kv_recv.at[kind, c], (ynb, core, core)[kind])

    def kv_wait(kind, c):
        at = kv_at((y_cp, core_cp, lax.rem(core_cp + 2, 4))[kind], c)
        remote(at, at, kv_send.at[kind, c], kv_recv.at[kind, c], core).wait_recv()

    def kv_out(c):
        kv_local(c).wait()
        kv_copy(0, c).start()
        kv_copy(1, c).start()

    def cache_out(c):
        at = pl.ds(c * c_rows, c_rows)
        return (pltpu.make_async_copy(k3buf.at[at], k_ref.at[at], kv3_sem.at[0, c]),
                pltpu.make_async_copy(v3buf.at[at], v_ref.at[at], kv3_sem.at[1, c]))

    step = 16

    for cpy in small:
        cpy.wait()

    def angles(i, _):
        at = pl.ds(pl.multiple_of(i * HEAD, HEAD), HEAD)
        angle = posbuf[at, :].astype(F32) * freqbuf[...]
        cos_h, sin_h = jnp.cos(angle), jnp.sin(angle)
        cosbuf[at, :] = jnp.concatenate([cos_h, cos_h], axis=-1)
        sinbuf[at, :] = jnp.concatenate([-sin_h, sin_h], axis=-1)
        return 0

    lax.fori_loop(0, rows // HEAD, angles, 0)

    def turn(vec, r_at):
        return rope(vec, cosbuf[r_at, :], sinbuf[r_at, :])

    for c in range(chunks):
        x_load(c).wait()

        def square_rows(i, _, c=c):
            at = pl.ds(pl.multiple_of(i * step, step), step)
            xf = xbuf[c, at, :].astype(F32)
            mean = jnp.sum(xf * xf, axis=-1, keepdims=True) * (1.0 / width)
            invbuf[at, :] = jnp.broadcast_to(lax.rsqrt(mean + 1e-5), (step, HEAD))
            return 0

        def norm_rows(i, _, c=c):
            at = pl.ds(pl.multiple_of(i * step, step), step)
            to = pl.ds(pl.multiple_of(c * c_rows + i * step, step), step)
            inv = invbuf[at, 0:1]
            hbuf[to, :] = (xbuf[c, at, :].astype(F32) * inv * gainbuf[...]).astype(BF16)
            return 0

        lax.fori_loop(0, c_rows // step, square_rows, 0, unroll=4)
        lax.fori_loop(0, c_rows // step, norm_rows, 0, unroll=2)
        if c == 0:
            wk_load.wait()
            wv_load.wait()
        r_at = pl.ds(c * c_rows, c_rows)
        h = hbuf[r_at, :]
        k_new = jnp.dot(h, wkbuf[...], preferred_element_type=F32).astype(BF16)
        v_new = jnp.dot(h, wvbuf[...], preferred_element_type=F32).astype(BF16)
        for j in range(cols // HEAD):
            at = slice(j * HEAD, (j + 1) * HEAD)
            k_head = turn(k_new[:, at], r_at)
            kvbuf[r_at, at] = k_head
            k3buf[r_at, j, :] = k_head
            v3buf[r_at, j, :] = v_new[:, at]
        kvbuf[r_at, cols:] = v_new
        kv_local(c).start()
        for cpy in cache_out(c):
            cpy.start()
        if c > 0:
            kv_out(c - 1)

    @pl.when(z > 0)
    def _():
        r1(1, 0).wait_recv()

    @pl.when(z < 3)
    def _():
        r1(0, 0).wait_recv()

    @pl.when(is_mid)
    def _():
        r2(0).start()
        r2(1).start()

    def q_out(t):
        return pltpu.make_async_copy(qbuf.at[t], q_ref.at[:, pl.ds(t * q_cols, q_cols)], q_sem.at[t])

    def q_tile(t):
        wq_load(t).wait()
        q_new = jnp.dot(hbuf[...], wqbuf[t], preferred_element_type=F32).astype(BF16)
        everything = pl.ds(0, rows)
        for j in range(q_cols // HEAD):
            qbuf[t, :, j * HEAD:(j + 1) * HEAD] = turn(q_new[:, j * HEAD:(j + 1) * HEAD], everything)
        q_out(t).start()

    q_tile(0)
    kv_out(chunks - 1)
    q_tile(1)
    for c in range(2):
        kv_wait(0, c)
        kv_copy(2, c).start()
    q_tile(2)
    q_tile(3)
    for c in range(2, chunks):
        kv_wait(0, c)
        kv_copy(2, c).start()
    for c in range(chunks):
        kv_wait(1, c)
        kv_wait(2, c)
    for t in range(q_tiles):
        q_out(t).wait()
    for c in range(chunks):
        for cpy in cache_out(c):
            cpy.wait()

    @pl.when(z > 0)
    def _():
        r1(1, 1).wait_recv()
        for part in range(2):
            r1(0, part).wait_send()

    @pl.when(z < 3)
    def _():
        r1(0, 1).wait_recv()
        for part in range(2):
            r1(1, part).wait_send()

    r2(0).wait_recv()

    @pl.when(is_mid)
    def _():
        r2(0).wait_send()
        r2(1).wait_send()

    for c in range(chunks):
        for kind in range(3):
            kv_copy(kind, c).wait_send()


def project(x, gain, w_k, w_v, w_q, w_o, pos, inv_freq):
    rows, width = x.shape
    cols = w_k.shape[1]
    q_cols = w_q.shape[1]
    half = w_o.shape[0] // 16
    dma = pltpu.SemaphoreType.DMA
    out = jax.ShapeDtypeStruct
    hbm = pl.BlockSpec(memory_space=HBM)
    return pl.pallas_call(
        proj_kernel,
        in_specs=[hbm] * 8,
        out_specs=[hbm] * 9,
        out_shape=[out((rows, q_cols), BF16), out((4 * rows, 2 * cols), BF16)] + [out((rows, cols // HEAD, HEAD), BF16)] * 2
        + [out((half, w_o.shape[1]), BF16)] * 5,
        scratch_shapes=[
            VMEM((4, rows // 4, width), BF16),
            VMEM((rows, width), BF16),
            VMEM((rows // 4, HEAD), F32),
            VMEM((1, width), F32),
            VMEM((rows, 1), jnp.int32),
            VMEM((1, HEAD // 2), F32),
            VMEM((rows, HEAD), F32),
            VMEM((rows, HEAD), F32),
            VMEM((width, cols), BF16),
            VMEM((width, cols), BF16),
            VMEM((4, width, q_cols // 4), BF16),
            VMEM((rows, 2 * cols), BF16),
            VMEM((rows, cols // HEAD, HEAD), BF16),
            VMEM((rows, cols // HEAD, HEAD), BF16),
            VMEM((4, rows, q_cols // 4), BF16),
            dma((4,)), dma((5,)), dma((4,)), dma((4,)), dma((2, 4)), dma((4,)),
            dma((3, 4)), dma((3, 4)), dma((2, 2)), dma((2, 2)), dma((2,)), dma,
        ],
        compiler_params=pltpu.CompilerParams(collective_id=0, has_side_effects=True, vmem_limit_bytes=VMEM_MAX),
        cost_estimate=pl.CostEstimate(flops=2 * rows * width * (2 * cols + q_cols), bytes_accessed=24 << 20, transcendentals=0),
        name="proj",
    )(x, gain.reshape(1, width), w_k, w_v, w_q, w_o, pos[:, None], inv_freq.reshape(1, HEAD // 2))


def attn_kernel(pos_smem, q_ref, pos_ref, kv_ref, k_ref, v_ref, o_ref, k_out_ref, v_out_ref, kbuf, vbuf, in_sem, out_sem):
    blk = pl.program_id(0)

    cache = ((k_ref, kbuf, k_out_ref), (v_ref, vbuf, v_out_ref))
    loads = [pltpu.make_async_copy(src, buf, in_sem.at[i]) for i, (src, buf, _) in enumerate(cache)]
    stores = [pltpu.make_async_copy(buf, dst, out_sem.at[i]) for i, (_, buf, dst) in enumerate(cache)]

    @pl.when(blk == 0)
    def _():
        for c in loads:
            c.start()

    @pl.when(blk == 2)
    def _():
        for c, d in zip(loads, stores):
            c.wait()
            d.start()

    half_blks = pl.num_programs(0) // 2
    piece = half_blks * Q_TILE
    cp = lax.axis_index("cp")
    q_rows = q_ref.shape[0]
    kv_cols = kv_ref.shape[1] // 2
    heads = kv_cols // HEAD
    group = q_ref.shape[1] // kv_cols
    pieces = kv_ref.shape[0] // piece
    g0 = jnp.where(blk < half_blks, cp * piece + blk * Q_TILE, (pieces - 1 - cp) * piece + (blk - half_blks) * Q_TILE)
    low = (g0 - pos_smem[blk * Q_TILE]) // Q_TILE
    tok_1 = g0 + lax.broadcasted_iota(jnp.int32, (q_rows, 1), 0)
    tok = jnp.concatenate([tok_1] * group, axis=0)
    first = jnp.concatenate([tok_1 - pos_ref[...]] * group, axis=0)
    factor = HEAD ** -0.5 * 1.4426950408889634

    def head_q(n):
        return jnp.concatenate([q_ref[:, (n * group + g) * HEAD:(n * group + g + 1) * HEAD] for g in range(group)], axis=0)

    def scores(n, q, start, width):
        keys = kv_ref[pl.ds(pl.multiple_of(start, Q_TILE), width), n * HEAD:(n + 1) * HEAD]
        s = lax.dot_general(q, keys, (((1,), (1,)), ((), ())), preferred_element_type=F32)
        u = start + lax.broadcasted_iota(jnp.int32, (1, width), 1)
        return jnp.where((u >= first) & (u <= tok), s, -1e30)

    def values(n, start, width):
        return kv_ref[pl.ds(pl.multiple_of(start, Q_TILE), width), kv_cols + n * HEAD:kv_cols + (n + 1) * HEAD]

    near = jnp.maximum(g0 - Q_TILE, 0)
    states = []
    for n in range(heads):
        s = scores(n, head_q(n), near, 2 * Q_TILE)
        m = jnp.max(s, axis=-1, keepdims=True)
        p = jnp.exp2((s - m) * factor)
        total = jnp.sum(p, axis=-1, keepdims=True)
        acc = jnp.dot(p.astype(BF16), values(n, near, 2 * Q_TILE), preferred_element_type=F32)
        states.append((m, total, acc))

    def far(n, i, carry):
        m, total, acc = carry
        start = i * Q_TILE
        s = scores(n, head_q(n), start, Q_TILE)
        m_new = jnp.maximum(m, jnp.max(s, axis=-1, keepdims=True))
        old = jnp.exp2((m - m_new) * factor)
        p = jnp.exp2((s - m_new) * factor)
        total = total * old + jnp.sum(p, axis=-1, keepdims=True)
        acc = acc * old + jnp.dot(p.astype(BF16), values(n, start, Q_TILE), preferred_element_type=F32)
        return m_new, total, acc

    def put(n, state):
        out = (state[2] / state[1]).astype(BF16)
        for g in range(group):
            o_ref[:, (n * group + g) * HEAD:(n * group + g + 1) * HEAD] = out[g * q_rows:(g + 1) * q_rows]

    for n in range(heads):
        put(n, states[n])

    @pl.when(low < near // Q_TILE)
    def _():
        for n in range(heads):
            put(n, lax.fori_loop(low, near // Q_TILE, functools.partial(far, n), states[n]))

    @pl.when(blk == pl.num_programs(0) - 1)
    def _():
        for d in stores:
            d.wait()


def attention(q, kvg, pos, k, v):
    rows, q_cols = q.shape
    hbm = pl.BlockSpec(memory_space=HBM)
    shape = jax.ShapeDtypeStruct
    return pl.pallas_call(
        attn_kernel,
        grid_spec=pltpu.PrefetchScalarGridSpec(
            num_scalar_prefetch=1,
            grid=(rows // Q_TILE,),
            in_specs=[
                pl.BlockSpec((Q_TILE, q_cols), lambda i, *_: (i, 0)),
                pl.BlockSpec((Q_TILE, 1), lambda i, *_: (i, 0)),
                pl.BlockSpec(kvg.shape, lambda i, *_: (0, 0)),
                hbm,
                hbm,
            ],
            out_specs=[pl.BlockSpec((Q_TILE, q_cols), lambda i, *_: (i, 0)), hbm, hbm],
            scratch_shapes=[VMEM(k.shape, BF16), VMEM(v.shape, BF16), pltpu.SemaphoreType.DMA((2,)), pltpu.SemaphoreType.DMA((2,))],
        ),
        out_shape=[shape((rows, q_cols), BF16), shape(k.shape, BF16), shape(v.shape, BF16)],
        compiler_params=pltpu.CompilerParams(vmem_limit_bytes=VMEM_MAX),
        cost_estimate=pl.CostEstimate(flops=5 << 30, bytes_accessed=8 << 20, transcendentals=0),
        name="attn",
    )(pos, q, pos[:, None], kvg, k, v)


def out_kernel(o_ref, fla_ref, flb_ref, fra_ref, frb_ref, far_ref, fl2b_ref, fr2b_ref, third_ref, wown_ref, x_ref, y_ref,
               wbuf, wtile, xtile, obuf, acc, ytile,
               load_sem, tile_sem, y_sem, wsend, wrecv, w3_send, w3_recv, own_send, fwd_send, o_recv):
    rows, kdim = o_ref.shape
    width = x_ref.shape[1]
    half = fla_ref.shape[0]
    slice_rows = 2 * half
    chunks = 4
    c_rows = rows // chunks
    n_tile = xtile.shape[2]
    y_cols = ytile.shape[2]
    dp, z, cp = lax.axis_index("dp"), lax.axis_index("tp"), lax.axis_index("cp")
    is_end = (z == 0) | (z == 3)
    is_mid = (z == 1) | (z == 2)
    core = {"cp": cp + 1 - 2 * lax.rem(cp, 2)}
    ynb = {"cp": lax.rem(cp + 2, 4)}
    xnb = {"dp": 1 - dp}
    left = {"tp": jnp.maximum(z - 1, 0)}
    right = {"tp": jnp.minimum(z + 1, 3)}
    p_own = dp * 4 + cp
    p_x = (1 - dp) * 4 + cp
    p_y = dp * 4 + lax.rem(cp + 2, 4)
    p_d = (1 - dp) * 4 + lax.rem(cp + 2, 4)
    p_core = dp * 4 + cp + 1 - 2 * lax.rem(cp, 2)
    low_side = z < 2
    s1 = jnp.where(low_side, 1 - z, 5 - z)
    s2 = jnp.where(low_side, 2, 1)
    s3 = jnp.where(low_side, 3, 0)

    def remote(src, dst, ssem, rsem, dev):
        return pltpu.make_async_remote_copy(src_ref=src, dst_ref=dst, send_sem=ssem, recv_sem=rsem, device_id=dev, device_id_type=MESH)

    barrier = pltpu.get_barrier_semaphore()
    for dev in (core, ynb, xnb):
        pl.semaphore_signal(barrier, inc=1, device_id=dev, device_id_type=MESH)

    @pl.when(z > 0)
    def _():
        pl.semaphore_signal(barrier, inc=1, device_id=left, device_id_type=MESH)

    @pl.when(z < 3)
    def _():
        pl.semaphore_signal(barrier, inc=1, device_id=right, device_id_type=MESH)

    def w_at(j, p, start=0, n=None):
        n = slice_rows if n is None else n
        return wbuf.at[j, pl.ds(pl.multiple_of(p * slice_rows + start, half), n)]

    def load_w(src, j, part):
        return pltpu.make_async_copy(src, w_at(j, p_own, part * half, half), load_sem.at[j, part])

    fl, fr, fl2, fr2 = (fla_ref, flb_ref), (fra_ref, frb_ref), (far_ref, fl2b_ref), (far_ref, fr2b_ref)
    sources = ((fr, fr2, (third_ref,)), (fl, fr, fr2), (fr, fl, fl2), (fl, fl2, (third_ref,)))
    for zz in range(4):
        @pl.when(z == zz)
        def _(zz=zz):
            for j in range(3):
                for part, src in enumerate(sources[zz][j]):
                    load_w(src, j, part).start()

    @pl.when(is_end)
    def _():
        pl.semaphore_wait(barrier, 4)

    @pl.when(is_mid)
    def _():
        pl.semaphore_wait(barrier, 5)

    def w_copy(j, kind):
        dev = (xnb, ynb, core, ynb, xnb, core, core, core, core)[kind]
        src = (w_at(j, p_own), w_at(j, p_own), w_at(j, p_own), w_at(j, p_x, 0, half), w_at(j, p_y, half, half),
               w_at(j, p_x), w_at(j, p_y), w_at(j, p_d, 0, half), w_at(j, p_d, half, half))[kind]
        return remote(src, src, wsend.at[j, kind], wrecv.at[j, kind], dev)

    def core_p(p):
        return p + 1 - 2 * lax.rem(p, 2)

    def w_wait(j, kind):
        dst = (w_at(j, p_x), w_at(j, p_y), w_at(j, p_core), w_at(j, p_d, 0, half), w_at(j, p_d, half, half),
               w_at(j, core_p(p_x)), w_at(j, core_p(p_y)), w_at(j, core_p(p_d), 0, half), w_at(j, core_p(p_d), half, half))[kind]
        remote(dst, dst, wsend.at[j, kind], wrecv.at[j, kind], core).wait_recv()

    def spread_own(j):
        for kind in (0, 1, 2):
            w_copy(j, kind).start()

    def spread_relay(j):
        w_wait(j, 0)
        w_copy(j, 3).start()
        w_copy(j, 5).start()
        w_wait(j, 1)
        w_copy(j, 4).start()
        w_copy(j, 6).start()

    def spread_diag(j):
        w_wait(j, 3)
        w_copy(j, 7).start()
        w_wait(j, 4)
        w_copy(j, 8).start()

    def spread_done(j):
        for kind in (2, 5, 6, 7, 8):
            w_wait(j, kind)

    def slot_of(s, dev_z):
        return s - (s > dev_z).astype(jnp.int32)

    def o_at(s, c, dev_z=None):
        return obuf.at[slot_of(s, z if dev_z is None else dev_z), pl.ds(pl.multiple_of(c * c_rows, c_rows), c_rows)]

    def o_own(c, side):
        src = o_ref.at[pl.ds(c * c_rows, c_rows)]
        return remote(src, o_at(z, c, z + (-1, 1)[side]), own_send.at[side, c], o_recv.at[z, c], (left, right)[side])

    def o_fwd(s, c, side):
        return remote(o_at(s, c), o_at(s, c, z + (-1, 1)[side]), fwd_send.at[s, c], o_recv.at[s, c], (left, right)[side])

    def o_wait(s, c):
        remote(o_at(s, c), o_at(s, c), fwd_send.at[s, c], o_recv.at[s, c], left).wait_recv()

    def o_pass(s, c):
        o_wait(s, c)

        @pl.when(s < z)
        def _():
            o_fwd(s, c, 1).start()

        @pl.when(s > z)
        def _():
            o_fwd(s, c, 0).start()

    w3_at = w_at(2, p_own, half, half)
    w3 = remote(w3_at, w3_at, w3_send, w3_recv, {"tp": jnp.where(z == 1, 0, 3)})

    @pl.when(is_mid)
    def _():
        load_w(fla_ref, 2, 1).wait()
        w3.start()

    for c in range(chunks):
        @pl.when(z > 0)
        def _(c=c):
            o_own(c, 0).start()

        @pl.when(z < 3)
        def _(c=c):
            o_own(c, 1).start()

    for j in range(2):
        for part in range(2):
            load_w(fla_ref, j, part).wait()
        spread_own(j)

    def tile_loads(n, slot):
        at = pl.ds(pl.multiple_of(n * n_tile, n_tile), n_tile)
        return (pltpu.make_async_copy(wown_ref.at[:, at], wtile.at[slot], tile_sem.at[0, slot]),
                pltpu.make_async_copy(x_ref.at[:, at], xtile.at[slot], tile_sem.at[1, slot]))

    n_steps = width // n_tile
    for cpy in tile_loads(0, 0):
        cpy.start()

    def own_step(n, _):
        slot = lax.rem(n, 2)

        @pl.when(n + 1 < n_steps)
        def _():
            for cpy in tile_loads(n + 1, 1 - slot):
                cpy.start()

        for cpy in tile_loads(n, slot):
            cpy.wait()
        at = pl.ds(pl.multiple_of(n * n_tile, n_tile), n_tile)
        acc[:, at] = xtile[slot].astype(F32) + jnp.dot(o_ref[...], wtile[slot], preferred_element_type=F32)
        return 0

    lax.fori_loop(0, n_steps, own_step, 0)

    def add_shard(j, s):
        wide = 512

        def step(n, _):
            at = pl.ds(pl.multiple_of(n * wide, wide), wide)
            acc[:, at] += jnp.dot(obuf[slot_of(s, z)], wbuf[j, :, at], preferred_element_type=F32)
            return 0

        lax.fori_loop(0, width // wide, step, 0)

    spread_relay(0)
    spread_relay(1)

    @pl.when(is_end)
    def _():
        remote(w3_at, w3_at, w3_send, w3_recv, left).wait_recv()

    load_w(fla_ref, 2, 0).wait()
    spread_own(2)

    @pl.when(is_mid)
    def _():
        for c in range(chunks):
            o_pass(s1, c)
            o_pass(s2, c)

    spread_diag(0)
    spread_done(0)

    @pl.when(is_end)
    def _():
        for c in range(chunks):
            o_wait(s1, c)

    add_shard(0, s1)
    spread_diag(1)
    spread_done(1)

    @pl.when(is_mid)
    def _():
        for c in range(chunks):
            o_pass(s3, c)

    spread_relay(2)

    @pl.when(is_end)
    def _():
        for c in range(chunks):
            o_wait(s2, c)

    add_shard(1, s2)
    spread_diag(2)
    spread_done(2)

    y_steps = width // y_cols

    def y_copy(i):
        slot = lax.rem(i, 2)
        r_at = pl.ds(pl.multiple_of((i // y_steps) * c_rows, c_rows), c_rows)
        n_at = pl.ds(pl.multiple_of(lax.rem(i, y_steps) * y_cols, y_cols), y_cols)
        return pltpu.make_async_copy(ytile.at[slot], y_ref.at[r_at, n_at], y_sem.at[slot])

    def last_step(i, _):
        c = i // y_steps

        @pl.when(is_end & (lax.rem(i, y_steps) == 0))
        def _():
            o_wait(s3, c)

        @pl.when(i >= 2)
        def _():
            y_copy(i - 2).wait()

        r_at = pl.ds(pl.multiple_of(c * c_rows, c_rows), c_rows)
        n_at = pl.ds(pl.multiple_of(lax.rem(i, y_steps) * y_cols, y_cols), y_cols)
        ytile[lax.rem(i, 2)] = (acc[r_at, n_at] + jnp.dot(obuf[slot_of(s3, z), r_at, :], wbuf[2, :, n_at], preferred_element_type=F32)).astype(BF16)
        y_copy(i).start()
        return 0

    total = chunks * y_steps
    lax.fori_loop(0, total, last_step, 0)
    y_copy(total - 2).wait()
    y_copy(total - 1).wait()

    for j in range(3):
        for kind in range(9):
            w_copy(j, kind).wait_send()
    for c in range(chunks):
        @pl.when(z > 0)
        def _(c=c):
            o_own(c, 0).wait_send()

        @pl.when(z < 3)
        def _(c=c):
            o_own(c, 1).wait_send()

    @pl.when(is_mid)
    def _():
        w3.wait_send()
        for c in range(chunks):
            for s in (s1, s2, s3):
                o_fwd(s, c, 0).wait_send()


def out_proj(o, slices, w_own, x):
    rows, kdim = o.shape
    width = x.shape[1]
    dma = pltpu.SemaphoreType.DMA
    return pl.pallas_call(
        out_kernel,
        in_specs=[pl.BlockSpec(memory_space=VMEM)] + [pl.BlockSpec(memory_space=HBM)] * 5 + [pl.BlockSpec(memory_space=pl.ANY)] * 3 + [pl.BlockSpec(memory_space=HBM)] * 2,
        out_specs=pl.BlockSpec(memory_space=pl.ANY),
        out_shape=jax.ShapeDtypeStruct((rows, width), BF16),
        scratch_shapes=[
            VMEM((3, kdim, width), BF16),
            VMEM((2, kdim, 256), BF16),
            VMEM((2, rows, 256), BF16),
            VMEM((3, rows, kdim), BF16),
            VMEM((rows, width), F32),
            VMEM((2, rows // 4, 1024), BF16),
            dma((3, 2)), dma((2, 2)), dma((2,)), dma((3, 9)), dma((3, 9)), dma, dma,
            dma((2, 4)), dma((4, 4)), dma((4, 4)),
        ],
        compiler_params=pltpu.CompilerParams(collective_id=1, has_side_effects=True, vmem_limit_bytes=VMEM_MAX),
        name="out_proj",
    )(o, *slices, w_own, x)


def settle_kernel(src_ref, dst_ref, buf, in_sem, out_sem):
    parts, rows = buf.shape[0], buf.shape[1]

    def load(i):
        return pltpu.make_async_copy(src_ref.at[pl.ds(i * rows, rows)], buf.at[i], in_sem.at[i])

    def store(i):
        return pltpu.make_async_copy(buf.at[i], dst_ref.at[pl.ds(i * rows, rows)], out_sem.at[i])

    for i in range(parts):
        load(i).start()
    for i in range(parts):
        load(i).wait()
        store(i).start()
    for i in range(parts):
        store(i).wait()


def settle(y):
    parts = 16
    rows, width = y.shape
    dma = pltpu.SemaphoreType.DMA
    return pl.pallas_call(
        settle_kernel,
        in_specs=[pl.BlockSpec(memory_space=HBM)],
        out_specs=pl.BlockSpec(memory_space=HBM),
        out_shape=jax.ShapeDtypeStruct(y.shape, y.dtype),
        scratch_shapes=[VMEM((parts, rows // parts, width), y.dtype), dma((parts,)), dma((parts,))],
        name="settle",
    )(y)


def solution(mesh):
    def local_step(x_in, doc_id, pos_in_doc, norm_gain, w_q, w_k, w_v, w_o, inv_freq):
        rows = x_in.shape[0]
        q, kvg, k_new, v_new, fla, flb, fra, frb, far = project(x_in, norm_gain, w_k, w_v, w_q, w_o, pos_in_doc, inv_freq)
        fl2b = lax.ppermute(flb, "tp", [(1, 2), (2, 3)])
        fr2b = lax.ppermute(frb, "tp", [(1, 0), (2, 1)])
        third = lax.ppermute(far, "tp", [(1, 0), (2, 3)])
        o, k_out, v_out = attention(q, kvg, pos_in_doc, k_new, v_new)
        y = settle(out_proj(o, (fla, flb, fra, frb, far, fl2b, fr2b, third), w_o, x_in))
        return y, k_out, v_out

    row_spec = P(("dp", "cp"))
    in_specs = (P(("dp", "cp"), None), row_spec, row_spec, P(), P(None, "tp"), P(None, "tp"), P(None, "tp"), P("tp", None), P())
    out_specs = (P(("dp", "cp"), None), P(("dp", "cp"), "tp", None), P(("dp", "cp"), "tp", None))
    return jax.shard_map(local_step, mesh=mesh, in_specs=in_specs, out_specs=out_specs, check_vma=False)
```

```python
import functools

import jax
import jax.numpy as jnp
from jax import lax
from jax.experimental import pallas as pl
from jax.experimental.pallas import tpu as pltpu
from jax.sharding import PartitionSpec as P

MESH = pl.DeviceIdType.MESH
HBM = pltpu.HBM
VMEM = pltpu.VMEM
HEAD = 128
Q_TILE = 128
VMEM_MAX = 67043328
F32 = jnp.float32
BF16 = jnp.bfloat16


def in_vmem(arr):
    return pltpu.with_memory_space_constraint(arr, VMEM)


def rope(vec, cos_t, sin_t):
    vec = vec.astype(F32)
    return (vec * cos_t + pltpu.roll(vec, HEAD // 2, 1) * sin_t).astype(BF16)


def proj_kernel(x_ref, gain_ref, wk_ref, wv_ref, wq_ref, wo_ref, pos_ref, freq_ref,
                q_ref, kvg_ref, k_ref, v_ref, fl_ref, fr_ref, fara_ref, farb_ref,
                xbuf, hbuf, invbuf, gainbuf, posbuf, freqbuf, cosbuf, sinbuf, wkbuf, wvbuf, wqbuf, kvbuf, k3buf, v3buf, qbuf,
                x_sem, w_sem, wq_sem, kvl_sem, kv3_sem, q_sem, kv_send, kv_recv, r1_send, r1_recv, r2_send, r2_recv):
    chunks, q_tiles = 4, 4
    rows, width = hbuf.shape
    c_rows = rows // chunks
    piece = rows // 2
    cols = wkbuf.shape[1]
    q_cols = wqbuf.shape[2]
    half = fl_ref.shape[0] // 2
    n_cp = 4
    dp, z, cp = lax.axis_index("dp"), lax.axis_index("tp"), lax.axis_index("cp")
    core_cp = cp + 1 - 2 * lax.rem(cp, 2)
    y_cp = lax.rem(cp + 2, 4)
    core, ynb = {"cp": core_cp}, {"cp": y_cp}
    left = {"tp": jnp.maximum(z - 1, 0)}
    right = {"tp": jnp.minimum(z + 1, 3)}
    is_mid = (z == 1) | (z == 2)

    def remote(src, dst, ssem, rsem, dev):
        return pltpu.make_async_remote_copy(src_ref=src, dst_ref=dst, send_sem=ssem, recv_sem=rsem, device_id=dev, device_id_type=MESH)

    barrier = pltpu.get_barrier_semaphore()
    for dev in (core, ynb):
        pl.semaphore_signal(barrier, inc=1, device_id=dev, device_id_type=MESH)

    @pl.when(z > 0)
    def _():
        pl.semaphore_signal(barrier, inc=1, device_id=left, device_id_type=MESH)

    @pl.when(z < 3)
    def _():
        pl.semaphore_signal(barrier, inc=1, device_id=right, device_id_type=MESH)

    def x_load(c):
        return pltpu.make_async_copy(x_ref.at[pl.ds(c * c_rows, c_rows)], xbuf.at[c], x_sem.at[c])

    def wq_load(t):
        return pltpu.make_async_copy(wq_ref.at[:, pl.ds(t * q_cols, q_cols)], wqbuf.at[t], wq_sem.at[t])

    wk_load = pltpu.make_async_copy(wk_ref, wkbuf, w_sem.at[0])
    wv_load = pltpu.make_async_copy(wv_ref, wvbuf, w_sem.at[1])
    small = [pltpu.make_async_copy(src, dst, w_sem.at[2 + i]) for i, (src, dst) in enumerate(((gain_ref, gainbuf), (pos_ref, posbuf), (freq_ref, freqbuf)))]
    for cpy in small:
        cpy.start()
    x_load(0).start()
    wk_load.start()
    wv_load.start()
    for c in range(1, chunks):
        x_load(c).start()
    for t in range(q_tiles):
        wq_load(t).start()

    @pl.when(is_mid)
    def _():
        pl.semaphore_wait(barrier, 4)

    @pl.when(jnp.logical_not(is_mid))
    def _():
        pl.semaphore_wait(barrier, 3)

    p_own = dp * 4 + cp

    def part_of(ref, part):
        return ref.at[pl.ds(part * half, half)]

    def r1(side, part):
        src = wo_ref.at[pl.ds(pl.multiple_of((p_own * 2 + part) * half, half), half)]
        dst = part_of((fr_ref, fl_ref)[side], part)
        return remote(src, dst, r1_send.at[side, part], r1_recv.at[side, part], (left, right)[side])

    def r2(side, part):
        src = part_of((fr_ref, fl_ref)[side], part)
        return remote(src, (fara_ref, farb_ref)[part], r2_send.at[side, part], r2_recv.at[part], (left, right)[side])

    def second_hop(part):
        @pl.when(z > 0)
        def _():
            r1(1, part).wait_recv()

        @pl.when(z < 3)
        def _():
            r1(0, part).wait_recv()

        @pl.when(is_mid)
        def _():
            r2(0, part).start()
            r2(1, part).start()

    for part in range(2):
        @pl.when(z > 0)
        def _(part=part):
            r1(0, part).start()

        @pl.when(z < 3)
        def _(part=part):
            r1(1, part).start()

    def kv_at(owner, c):
        start = jnp.where(c < chunks // 2, owner, 2 * n_cp - 1 - owner) * piece + (c % (chunks // 2)) * c_rows
        return kvg_ref.at[pl.ds(pl.multiple_of(start, c_rows), c_rows)]

    def kv_local(c):
        return pltpu.make_async_copy(kvbuf.at[pl.ds(c * c_rows, c_rows)], kv_at(cp, c), kvl_sem.at[c])

    def kv_copy(kind, c):
        at = kv_at((cp, cp, y_cp)[kind], c)
        return remote(at, at, kv_send.at[kind, c], kv_recv.at[kind, c], (ynb, core, core)[kind])

    def kv_wait(kind, c):
        at = kv_at((y_cp, core_cp, lax.rem(core_cp + 2, 4))[kind], c)
        remote(at, at, kv_send.at[kind, c], kv_recv.at[kind, c], core).wait_recv()

    def kv_out(c):
        kv_local(c).wait()
        kv_copy(0, c).start()
        kv_copy(1, c).start()

    def cache_out(c):
        at = pl.ds(c * c_rows, c_rows)
        return (pltpu.make_async_copy(k3buf.at[at], k_ref.at[at], kv3_sem.at[0, c]),
                pltpu.make_async_copy(v3buf.at[at], v_ref.at[at], kv3_sem.at[1, c]))

    step = 16

    for cpy in small:
        cpy.wait()

    pos_cols = jnp.transpose(posbuf[...].astype(F32))
    for i in range(rows // HEAD):
        angle = pos_cols[:, i:i + 1] * freqbuf[...]
        cos_h, sin_h = jnp.cos(angle), jnp.sin(angle)
        cosbuf[i * HEAD:(i + 1) * HEAD, :] = jnp.concatenate([cos_h, cos_h], axis=-1)
        sinbuf[i * HEAD:(i + 1) * HEAD, :] = jnp.concatenate([-sin_h, sin_h], axis=-1)

    def turn(vec, r_at):
        return rope(vec, cosbuf[r_at, :], sinbuf[r_at, :])

    for c in range(chunks):
        x_load(c).wait()

        def square_rows(i, _, c=c):
            at = pl.ds(pl.multiple_of(i * step, step), step)
            xf = xbuf[c, at, :].astype(F32)
            mean = jnp.sum(xf * xf, axis=-1, keepdims=True) * (1.0 / width)
            invbuf[at, :] = jnp.broadcast_to(lax.rsqrt(mean + 1e-5), (step, HEAD))
            return 0

        def norm_rows(i, _, c=c):
            at = pl.ds(pl.multiple_of(i * step, step), step)
            to = pl.ds(pl.multiple_of(c * c_rows + i * step, step), step)
            inv = invbuf[at, 0:1]
            hbuf[to, :] = (xbuf[c, at, :].astype(F32) * inv * gainbuf[...]).astype(BF16)
            return 0

        lax.fori_loop(0, c_rows // step, square_rows, 0, unroll=4)
        lax.fori_loop(0, c_rows // step, norm_rows, 0, unroll=2)
        if c == 0:
            wk_load.wait()
            wv_load.wait()
        r_at = pl.ds(c * c_rows, c_rows)
        h = hbuf[r_at, :]
        k_new = jnp.dot(h, wkbuf[...], preferred_element_type=F32).astype(BF16)
        v_new = jnp.dot(h, wvbuf[...], preferred_element_type=F32).astype(BF16)
        for j in range(cols // HEAD):
            at = slice(j * HEAD, (j + 1) * HEAD)
            k_head = turn(k_new[:, at], r_at)
            kvbuf[r_at, at] = k_head
            k3buf[r_at, j, :] = k_head
            v3buf[r_at, j, :] = v_new[:, at]
        kvbuf[r_at, cols:] = v_new
        kv_local(c).start()
        for cpy in cache_out(c):
            cpy.start()
        if c > 0:
            kv_out(c - 1)

    second_hop(0)

    def q_out(t):
        return pltpu.make_async_copy(qbuf.at[t], q_ref.at[:, pl.ds(t * q_cols, q_cols)], q_sem.at[t])

    def q_tile(t):
        wq_load(t).wait()
        q_new = jnp.dot(hbuf[...], wqbuf[t], preferred_element_type=F32).astype(BF16)
        everything = pl.ds(0, rows)
        for j in range(q_cols // HEAD):
            qbuf[t, :, j * HEAD:(j + 1) * HEAD] = turn(q_new[:, j * HEAD:(j + 1) * HEAD], everything)
        q_out(t).start()

    q_tile(0)
    kv_out(chunks - 1)
    q_tile(1)
    for c in range(2):
        kv_wait(0, c)
        kv_copy(2, c).start()
    q_tile(2)
    second_hop(1)
    q_tile(3)
    for c in range(2, chunks):
        kv_wait(0, c)
        kv_copy(2, c).start()
    for c in range(chunks):
        kv_wait(1, c)
        kv_wait(2, c)
    for t in range(q_tiles):
        q_out(t).wait()
    for c in range(chunks):
        for cpy in cache_out(c):
            cpy.wait()

    for part in range(2):
        @pl.when(z > 0)
        def _(part=part):
            r1(0, part).wait_send()

        @pl.when(z < 3)
        def _(part=part):
            r1(1, part).wait_send()

        r2(0, part).wait_recv()

        @pl.when(is_mid)
        def _(part=part):
            r2(0, part).wait_send()
            r2(1, part).wait_send()

    for c in range(chunks):
        for kind in range(3):
            kv_copy(kind, c).wait_send()


def project(x, gain, w_k, w_v, w_q, w_o, pos, inv_freq):
    rows, width = x.shape
    cols = w_k.shape[1]
    q_cols = w_q.shape[1]
    w_rows = w_o.shape[0] // 8
    dma = pltpu.SemaphoreType.DMA
    hbm = pl.BlockSpec(memory_space=HBM)
    return pl.pallas_call(
        proj_kernel,
        in_specs=[hbm] * 8,
        out_specs=[hbm] * 8,
        out_shape=[HBM((rows, q_cols), BF16), HBM((4 * rows, 2 * cols), BF16)] + [HBM((rows, cols // HEAD, HEAD), BF16)] * 2
        + [HBM((w_rows, w_o.shape[1]), BF16)] * 2 + [HBM((w_rows // 2, w_o.shape[1]), BF16)] * 2,
        scratch_shapes=[
            VMEM((4, rows // 4, width), BF16),
            VMEM((rows, width), BF16),
            VMEM((rows // 4, HEAD), F32),
            VMEM((1, width), F32),
            VMEM((rows // HEAD, HEAD), jnp.int32),
            VMEM((1, HEAD // 2), F32),
            VMEM((rows, HEAD), F32),
            VMEM((rows, HEAD), F32),
            VMEM((width, cols), BF16),
            VMEM((width, cols), BF16),
            VMEM((4, width, q_cols // 4), BF16),
            VMEM((rows, 2 * cols), BF16),
            VMEM((rows, cols // HEAD, HEAD), BF16),
            VMEM((rows, cols // HEAD, HEAD), BF16),
            VMEM((4, rows, q_cols // 4), BF16),
            dma((4,)), dma((5,)), dma((4,)), dma((4,)), dma((2, 4)), dma((4,)),
            dma((3, 4)), dma((3, 4)), dma((2, 2)), dma((2, 2)), dma((2, 2)), dma((2,)),
        ],
        compiler_params=pltpu.CompilerParams(collective_id=0, has_side_effects=True, vmem_limit_bytes=VMEM_MAX),
        cost_estimate=pl.CostEstimate(flops=2 * rows * width * (2 * cols + q_cols), bytes_accessed=24 << 20, transcendentals=0),
        name="proj",
    )(x, gain.reshape(1, width), w_k, w_v, w_q, w_o, pos.reshape(rows // HEAD, HEAD), inv_freq.reshape(1, HEAD // 2))


def attn_kernel(pos_smem, q_ref, pos_ref, kv_ref, k_ref, v_ref, o_ref, k_out_ref, v_out_ref, kbuf, vbuf, in_sem, out_sem):
    blk = pl.program_id(0)

    cache = ((k_ref, kbuf, k_out_ref), (v_ref, vbuf, v_out_ref))
    loads = [pltpu.make_async_copy(src, buf, in_sem.at[i]) for i, (src, buf, _) in enumerate(cache)]
    stores = [pltpu.make_async_copy(buf, dst, out_sem.at[i]) for i, (_, buf, dst) in enumerate(cache)]

    @pl.when(blk == 0)
    def _():
        for c in loads:
            c.start()

    @pl.when(blk == 2)
    def _():
        for c, d in zip(loads, stores):
            c.wait()
            d.start()

    half_blks = pl.num_programs(0) // 2
    piece = half_blks * Q_TILE
    cp = lax.axis_index("cp")
    q_rows = Q_TILE
    kv_cols = kv_ref.shape[1] // 2
    heads = kv_cols // HEAD
    group = q_ref.shape[1] // kv_cols
    pieces = kv_ref.shape[0] // piece
    g0 = jnp.where(blk < half_blks, cp * piece + blk * Q_TILE, (pieces - 1 - cp) * piece + (blk - half_blks) * Q_TILE)
    low = (g0 - pos_smem[blk * Q_TILE]) // Q_TILE
    tok_1 = g0 + lax.broadcasted_iota(jnp.int32, (q_rows, 1), 0)
    tok = jnp.concatenate([tok_1] * group, axis=0)
    pos_cols = jnp.transpose(pos_ref[...].astype(F32))
    mine = lax.broadcasted_iota(jnp.int32, pos_cols.shape, 1) == blk
    pos_1 = jnp.sum(jnp.where(mine, pos_cols, 0.0), axis=1, keepdims=True).astype(jnp.int32)
    first = jnp.concatenate([tok_1 - pos_1] * group, axis=0)
    factor = HEAD ** -0.5 * 1.4426950408889634

    def head_q(n):
        return jnp.concatenate([q_ref[:, (n * group + g) * HEAD:(n * group + g + 1) * HEAD] for g in range(group)], axis=0)

    def scores(n, q, start, width):
        keys = kv_ref[pl.ds(pl.multiple_of(start, Q_TILE), width), n * HEAD:(n + 1) * HEAD]
        s = lax.dot_general(q, keys, (((1,), (1,)), ((), ())), preferred_element_type=F32)
        u = start + lax.broadcasted_iota(jnp.int32, (1, width), 1)
        return jnp.where((u >= first) & (u <= tok), s, -1e30)

    def values(n, start, width):
        return kv_ref[pl.ds(pl.multiple_of(start, Q_TILE), width), kv_cols + n * HEAD:kv_cols + (n + 1) * HEAD]

    near = jnp.maximum(g0 - Q_TILE, 0)
    states = []
    for n in range(heads):
        s = scores(n, head_q(n), near, 2 * Q_TILE)
        m = jnp.max(s, axis=-1, keepdims=True)
        p = jnp.exp2((s - m) * factor)
        total = jnp.sum(p, axis=-1, keepdims=True)
        acc = jnp.dot(p.astype(BF16), values(n, near, 2 * Q_TILE), preferred_element_type=F32)
        states.append((m, total, acc))

    def far(n, i, carry):
        m, total, acc = carry
        start = i * Q_TILE
        s = scores(n, head_q(n), start, Q_TILE)
        m_new = jnp.maximum(m, jnp.max(s, axis=-1, keepdims=True))
        old = jnp.exp2((m - m_new) * factor)
        p = jnp.exp2((s - m_new) * factor)
        total = total * old + jnp.sum(p, axis=-1, keepdims=True)
        acc = acc * old + jnp.dot(p.astype(BF16), values(n, start, Q_TILE), preferred_element_type=F32)
        return m_new, total, acc

    def put(n, state):
        out = (state[2] / state[1]).astype(BF16)
        for g in range(group):
            o_ref[:, (n * group + g) * HEAD:(n * group + g + 1) * HEAD] = out[g * q_rows:(g + 1) * q_rows]

    for n in range(heads):
        put(n, states[n])

    @pl.when(low < near // Q_TILE)
    def _():
        for n in range(heads):
            put(n, lax.fori_loop(low, near // Q_TILE, functools.partial(far, n), states[n]))

    @pl.when(blk == pl.num_programs(0) - 1)
    def _():
        for d in stores:
            d.wait()


def attention(q, kvg, pos, k, v):
    rows, q_cols = q.shape
    hbm, vmem = pl.BlockSpec(memory_space=HBM), pl.BlockSpec(memory_space=VMEM)
    return pl.pallas_call(
        attn_kernel,
        grid_spec=pltpu.PrefetchScalarGridSpec(
            num_scalar_prefetch=1,
            grid=(rows // Q_TILE,),
            in_specs=[pl.BlockSpec((Q_TILE, q_cols), lambda i, *_: (i, 0)), vmem, vmem, hbm, hbm],
            out_specs=[pl.BlockSpec((Q_TILE, q_cols), lambda i, *_: (i, 0)), hbm, hbm],
            scratch_shapes=[VMEM(k.shape, BF16), VMEM(v.shape, BF16), pltpu.SemaphoreType.DMA((2,)), pltpu.SemaphoreType.DMA((2,))],
        ),
        out_shape=[HBM((rows, q_cols), BF16), HBM(k.shape, BF16), HBM(v.shape, BF16)],
        compiler_params=pltpu.CompilerParams(vmem_limit_bytes=VMEM_MAX),
        cost_estimate=pl.CostEstimate(flops=5 << 30, bytes_accessed=8 << 20, transcendentals=0),
        name="attn",
    )(pos, q, pos.reshape(rows // HEAD, HEAD), kvg, k, v)


def out_kernel(o_ref, fl_ref, fr_ref, fara_ref, farb_ref, third_ref, wown_ref, x_ref, y_ref,
               wbuf, wtile, xtile, obuf, own, acc,
               load_sem, tile_sem, own_sem, wsend, wrecv, w3_send, w3_recv, own_send, fwd_send, o_recv):
    rows, kdim = o_ref.shape
    width = x_ref.shape[1]
    slice_rows = fl_ref.shape[0]
    half = slice_rows // 2
    chunks = 4
    c_rows = rows // chunks
    n_tile = xtile.shape[2]
    y_cols = 1024
    dp, z, cp = lax.axis_index("dp"), lax.axis_index("tp"), lax.axis_index("cp")
    is_end = (z == 0) | (z == 3)
    is_mid = (z == 1) | (z == 2)
    core = {"cp": cp + 1 - 2 * lax.rem(cp, 2)}
    ynb = {"cp": lax.rem(cp + 2, 4)}
    xnb = {"dp": 1 - dp}
    left = {"tp": jnp.maximum(z - 1, 0)}
    right = {"tp": jnp.minimum(z + 1, 3)}
    p_own = dp * 4 + cp
    p_x = (1 - dp) * 4 + cp
    p_y = dp * 4 + lax.rem(cp + 2, 4)
    p_d = (1 - dp) * 4 + lax.rem(cp + 2, 4)
    p_core = dp * 4 + cp + 1 - 2 * lax.rem(cp, 2)
    low_side = z < 2
    s1 = jnp.where(low_side, 1 - z, 5 - z)
    s2 = jnp.where(low_side, 2, 1)
    s3 = jnp.where(low_side, 3, 0)

    def remote(src, dst, ssem, rsem, dev):
        return pltpu.make_async_remote_copy(src_ref=src, dst_ref=dst, send_sem=ssem, recv_sem=rsem, device_id=dev, device_id_type=MESH)

    barrier = pltpu.get_barrier_semaphore()
    for dev in (core, ynb, xnb):
        pl.semaphore_signal(barrier, inc=1, device_id=dev, device_id_type=MESH)

    @pl.when(z > 0)
    def _():
        pl.semaphore_signal(barrier, inc=1, device_id=left, device_id_type=MESH)

    @pl.when(z < 3)
    def _():
        pl.semaphore_signal(barrier, inc=1, device_id=right, device_id_type=MESH)

    own_load = pltpu.make_async_copy(o_ref, own, own_sem)
    own_load.start()

    def w_at(j, p, start=0, n=None):
        n = slice_rows if n is None else n
        return wbuf.at[j, pl.ds(pl.multiple_of(p * slice_rows + start, half), n)]

    def load_w(src, j, part):
        return pltpu.make_async_copy(src, w_at(j, p_own, part * half, half), load_sem.at[j, part])

    def parts_of(ref):
        return ref.at[pl.ds(0, half)], ref.at[pl.ds(half, half)]

    fl, fr, far, third = parts_of(fl_ref), parts_of(fr_ref), (fara_ref, farb_ref), (third_ref,)
    sources = ((fr, far, third), (fl, fr, far), (fr, fl, far), (fl, far, third))
    for zz in range(4):
        @pl.when(z == zz)
        def _(zz=zz):
            for j in range(3):
                for part, src in enumerate(sources[zz][j]):
                    load_w(src, j, part).start()

    @pl.when(is_end)
    def _():
        pl.semaphore_wait(barrier, 4)

    @pl.when(is_mid)
    def _():
        pl.semaphore_wait(barrier, 5)

    def w_copy(j, kind):
        dev = (xnb, ynb, core, ynb, xnb, core, core, core, core)[kind]
        src = (w_at(j, p_own), w_at(j, p_own), w_at(j, p_own), w_at(j, p_x, 0, half), w_at(j, p_y, half, half),
               w_at(j, p_x), w_at(j, p_y), w_at(j, p_d, 0, half), w_at(j, p_d, half, half))[kind]
        return remote(src, src, wsend.at[j, kind], wrecv.at[j, kind], dev)

    def core_p(p):
        return p + 1 - 2 * lax.rem(p, 2)

    def w_wait(j, kind):
        dst = (w_at(j, p_x), w_at(j, p_y), w_at(j, p_core), w_at(j, p_d, 0, half), w_at(j, p_d, half, half),
               w_at(j, core_p(p_x)), w_at(j, core_p(p_y)), w_at(j, core_p(p_d), 0, half), w_at(j, core_p(p_d), half, half))[kind]
        remote(dst, dst, wsend.at[j, kind], wrecv.at[j, kind], core).wait_recv()

    def spread_own(j):
        for kind in (0, 1, 2):
            w_copy(j, kind).start()

    def spread_relay(j):
        w_wait(j, 0)
        w_copy(j, 3).start()
        w_copy(j, 5).start()
        w_wait(j, 1)
        w_copy(j, 4).start()
        w_copy(j, 6).start()

    def spread_diag(j):
        w_wait(j, 3)
        w_copy(j, 7).start()
        w_wait(j, 4)
        w_copy(j, 8).start()

    def spread_done(j):
        for kind in (2, 5, 6, 7, 8):
            w_wait(j, kind)

    def slot_of(s, dev_z):
        return s - (s > dev_z).astype(jnp.int32)

    def o_at(s, c, dev_z=None):
        return obuf.at[slot_of(s, z if dev_z is None else dev_z), pl.ds(pl.multiple_of(c * c_rows, c_rows), c_rows)]

    def o_own(c, side):
        src = o_ref.at[pl.ds(c * c_rows, c_rows)]
        return remote(src, o_at(z, c, z + (-1, 1)[side]), own_send.at[side, c], o_recv.at[z, c], (left, right)[side])

    def o_fwd(s, c, side):
        return remote(o_at(s, c), o_at(s, c, z + (-1, 1)[side]), fwd_send.at[s, c], o_recv.at[s, c], (left, right)[side])

    def o_wait(s, c):
        remote(o_at(s, c), o_at(s, c), fwd_send.at[s, c], o_recv.at[s, c], left).wait_recv()

    def o_pass(s, c):
        o_wait(s, c)

        @pl.when(s < z)
        def _():
            o_fwd(s, c, 1).start()

        @pl.when(s > z)
        def _():
            o_fwd(s, c, 0).start()

    w3_at = w_at(2, p_own, half, half)
    w3 = remote(w3_at, w3_at, w3_send, w3_recv, {"tp": jnp.where(z == 1, 0, 3)})

    def send_own(c):
        @pl.when(z > 0)
        def _():
            o_own(c, 0).start()

        @pl.when(z < 3)
        def _():
            o_own(c, 1).start()

    send_own(0)

    @pl.when(is_mid)
    def _():
        load_w(third_ref, 2, 1).wait()
        w3.start()

    for c in range(1, chunks):
        send_own(c)

    for j in range(2):
        for part in range(2):
            load_w(third_ref, j, part).wait()
        spread_own(j)

    def tile_loads(n, slot):
        at = pl.ds(pl.multiple_of(n * n_tile, n_tile), n_tile)
        return (pltpu.make_async_copy(wown_ref.at[:, at], wtile.at[slot], tile_sem.at[0, slot]),
                pltpu.make_async_copy(x_ref.at[:, at], xtile.at[slot], tile_sem.at[1, slot]))

    n_steps = width // n_tile
    for cpy in tile_loads(0, 0):
        cpy.start()
    own_load.wait()

    def own_step(n, _):
        slot = lax.rem(n, 2)

        @pl.when(n + 1 < n_steps)
        def _():
            for cpy in tile_loads(n + 1, 1 - slot):
                cpy.start()

        for cpy in tile_loads(n, slot):
            cpy.wait()
        at = pl.ds(pl.multiple_of(n * n_tile, n_tile), n_tile)
        acc[:, at] = xtile[slot].astype(F32) + jnp.dot(own[...], wtile[slot], preferred_element_type=F32)
        return 0

    lax.fori_loop(0, n_steps, own_step, 0)

    def add_shard(j, s):
        wide = 512

        def step(n, _):
            at = pl.ds(pl.multiple_of(n * wide, wide), wide)
            acc[:, at] += jnp.dot(obuf[slot_of(s, z)], wbuf[j, :, at], preferred_element_type=F32)
            return 0

        lax.fori_loop(0, width // wide, step, 0)

    spread_relay(0)
    spread_relay(1)

    @pl.when(is_end)
    def _():
        remote(w3_at, w3_at, w3_send, w3_recv, left).wait_recv()

    load_w(third_ref, 2, 0).wait()
    spread_own(2)

    @pl.when(is_mid)
    def _():
        for c in range(chunks):
            o_pass(s1, c)
            o_pass(s2, c)

    spread_diag(0)
    spread_done(0)

    @pl.when(is_end)
    def _():
        for c in range(chunks):
            o_wait(s1, c)

    add_shard(0, s1)
    spread_diag(1)
    spread_done(1)

    @pl.when(is_mid)
    def _():
        for c in range(chunks):
            o_pass(s3, c)

    spread_relay(2)

    @pl.when(is_end)
    def _():
        for c in range(chunks):
            o_wait(s2, c)

    add_shard(1, s2)
    spread_diag(2)
    spread_done(2)

    y_steps = width // y_cols

    def last_step(i, _):
        c = i // y_steps

        @pl.when(is_end & (lax.rem(i, y_steps) == 0))
        def _():
            o_wait(s3, c)

        r_at = pl.ds(pl.multiple_of(c * c_rows, c_rows), c_rows)
        n_at = pl.ds(pl.multiple_of(lax.rem(i, y_steps) * y_cols, y_cols), y_cols)
        y_ref[r_at, n_at] = (acc[r_at, n_at] + jnp.dot(obuf[slot_of(s3, z), r_at, :], wbuf[2, :, n_at], preferred_element_type=F32)).astype(BF16)
        return 0

    lax.fori_loop(0, chunks * y_steps, last_step, 0)

    for j in range(3):
        for kind in range(9):
            w_copy(j, kind).wait_send()
    for c in range(chunks):
        @pl.when(z > 0)
        def _(c=c):
            o_own(c, 0).wait_send()

        @pl.when(z < 3)
        def _(c=c):
            o_own(c, 1).wait_send()

    @pl.when(is_mid)
    def _():
        w3.wait_send()
        for c in range(chunks):
            for s in (s1, s2, s3):
                o_fwd(s, c, 0).wait_send()


def out_proj(o, slices, w_own, x):
    rows, kdim = o.shape
    width = x.shape[1]
    dma = pltpu.SemaphoreType.DMA
    return pl.pallas_call(
        out_kernel,
        in_specs=[pl.BlockSpec(memory_space=HBM)] * 8,
        out_specs=pl.BlockSpec(memory_space=VMEM),
        out_shape=VMEM((rows, width), BF16),
        scratch_shapes=[
            VMEM((3, kdim, width), BF16),
            VMEM((2, kdim, 256), BF16),
            VMEM((2, rows, 256), BF16),
            VMEM((3, rows, kdim), BF16),
            VMEM((rows, kdim), BF16),
            VMEM((rows, width), F32),
            dma((3, 2)), dma((2, 2)), dma, dma((3, 9)), dma((3, 9)), dma, dma,
            dma((2, 4)), dma((4, 4)), dma((4, 4)),
        ],
        compiler_params=pltpu.CompilerParams(collective_id=1, has_side_effects=True, vmem_limit_bytes=54 << 20),
        name="out_proj",
    )(o, *slices, w_own, x)


def settle_kernel(src_ref, dst_ref, sem):
    parts = sem.shape[0]
    rows = src_ref.shape[0] // parts
    copies = [pltpu.make_async_copy(src_ref.at[pl.ds(i * rows, rows)], dst_ref.at[pl.ds(i * rows, rows)], sem.at[i]) for i in range(parts)]
    for c in copies:
        c.start()
    for c in copies:
        c.wait()


def settle(y):
    return pl.pallas_call(
        settle_kernel,
        in_specs=[pl.BlockSpec(memory_space=VMEM)],
        out_specs=pl.BlockSpec(memory_space=HBM),
        out_shape=HBM(y.shape, y.dtype),
        scratch_shapes=[pltpu.SemaphoreType.DMA((8,))],
        compiler_params=pltpu.CompilerParams(vmem_limit_bytes=16 << 20),
        name="settle",
    )(y)


def solution(mesh):
    def local_step(x_in, doc_id, pos_in_doc, norm_gain, w_q, w_k, w_v, w_o, inv_freq):
        rows = x_in.shape[0]
        q, kvg, k_new, v_new, fl, fr, fara, farb = project(x_in, norm_gain, w_k, w_v, w_q, w_o, pos_in_doc, inv_freq)
        third = lax.ppermute(fara, "tp", [(1, 0), (2, 3)])
        o, k_out, v_out = attention(q, kvg, pos_in_doc, k_new, v_new)
        y = settle(in_vmem(out_proj(o, (fl, fr, fara, farb, third), w_o, x_in)))
        return y, k_out, v_out

    row_spec = P(("dp", "cp"))
    in_specs = (P(("dp", "cp"), None), row_spec, row_spec, P(), P(None, "tp"), P(None, "tp"), P(None, "tp"), P("tp", None), P())
    out_specs = (P(("dp", "cp"), None), P(("dp", "cp"), "tp", None), P(("dp", "cp"), "tp", None))
    return jax.shard_map(local_step, mesh=mesh, in_specs=in_specs, out_specs=out_specs, check_vma=False)
```

```python
import functools

import jax
import jax.numpy as jnp
from jax import lax
from jax.experimental import pallas as pl
from jax.experimental.pallas import tpu as pltpu
from jax.sharding import PartitionSpec as P

MESH = pl.DeviceIdType.MESH
HBM = pltpu.HBM
VMEM = pltpu.VMEM
HEAD = 128
Q_TILE = 128
VMEM_MAX = 67043328
F32 = jnp.float32
BF16 = jnp.bfloat16


def in_vmem(arr):
    return pltpu.with_memory_space_constraint(arr, VMEM)


def rope(vec, cos_t, sin_t):
    vec = vec.astype(F32)
    return (vec * cos_t + pltpu.roll(vec, HEAD // 2, 1) * sin_t).astype(BF16)


def proj_kernel(x_ref, gain_ref, wk_ref, wv_ref, wq_ref, wo_ref, pos_ref, freq_ref,
                q_ref, kvg_ref, k_ref, v_ref, fl_ref, fr_ref, fara_ref, farb_ref,
                xbuf, hbuf, invbuf, gainbuf, posbuf, freqbuf, cosbuf, sinbuf, wkbuf, wvbuf, wqbuf, kvbuf, k3buf, v3buf, qbuf,
                x_sem, w_sem, wq_sem, kvl_sem, kv3_sem, q_sem, kv_send, kv_recv, r1_send, r1_recv, r2_send, r2_recv):
    chunks, q_tiles = 4, 4
    rows, width = hbuf.shape
    c_rows = rows // chunks
    piece = rows // 2
    cols = wkbuf.shape[1]
    q_cols = wqbuf.shape[2]
    half = fl_ref.shape[0] // 2
    n_cp = 4
    dp, z, cp = lax.axis_index("dp"), lax.axis_index("tp"), lax.axis_index("cp")
    core_cp = cp + 1 - 2 * lax.rem(cp, 2)
    y_cp = lax.rem(cp + 2, 4)
    core, ynb = {"cp": core_cp}, {"cp": y_cp}
    left = {"tp": jnp.maximum(z - 1, 0)}
    right = {"tp": jnp.minimum(z + 1, 3)}
    is_mid = (z == 1) | (z == 2)

    def remote(src, dst, ssem, rsem, dev):
        return pltpu.make_async_remote_copy(src_ref=src, dst_ref=dst, send_sem=ssem, recv_sem=rsem, device_id=dev, device_id_type=MESH)

    barrier = pltpu.get_barrier_semaphore()
    for dev in (core, ynb):
        pl.semaphore_signal(barrier, inc=1, device_id=dev, device_id_type=MESH)

    @pl.when(z > 0)
    def _():
        pl.semaphore_signal(barrier, inc=1, device_id=left, device_id_type=MESH)

    @pl.when(z < 3)
    def _():
        pl.semaphore_signal(barrier, inc=1, device_id=right, device_id_type=MESH)

    def x_load(c):
        return pltpu.make_async_copy(x_ref.at[pl.ds(c * c_rows, c_rows)], xbuf.at[c], x_sem.at[c])

    def wq_load(t):
        return pltpu.make_async_copy(wq_ref.at[:, pl.ds(t * q_cols, q_cols)], wqbuf.at[t], wq_sem.at[t])

    wk_load = pltpu.make_async_copy(wk_ref, wkbuf, w_sem.at[0])
    wv_load = pltpu.make_async_copy(wv_ref, wvbuf, w_sem.at[1])
    small = [pltpu.make_async_copy(src, dst, w_sem.at[2 + i]) for i, (src, dst) in enumerate(((gain_ref, gainbuf), (pos_ref, posbuf), (freq_ref, freqbuf)))]
    for cpy in small:
        cpy.start()
    x_load(0).start()
    wk_load.start()
    wv_load.start()
    for c in range(1, chunks):
        x_load(c).start()
    for t in range(q_tiles):
        wq_load(t).start()

    @pl.when(is_mid)
    def _():
        pl.semaphore_wait(barrier, 4)

    @pl.when(jnp.logical_not(is_mid))
    def _():
        pl.semaphore_wait(barrier, 3)

    p_own = dp * 4 + cp

    def part_of(ref, part):
        return ref.at[pl.ds(part * half, half)]

    def r1(side, part):
        src = wo_ref.at[pl.ds(pl.multiple_of((p_own * 2 + part) * half, half), half)]
        dst = part_of((fr_ref, fl_ref)[side], part)
        return remote(src, dst, r1_send.at[side, part], r1_recv.at[side, part], (left, right)[side])

    def r2(side, part):
        src = part_of((fr_ref, fl_ref)[side], part)
        return remote(src, (fara_ref, farb_ref)[part], r2_send.at[side, part], r2_recv.at[part], (left, right)[side])

    def second_hop(part):
        @pl.when(z > 0)
        def _():
            r1(1, part).wait_recv()

        @pl.when(z < 3)
        def _():
            r1(0, part).wait_recv()

        @pl.when(is_mid)
        def _():
            r2(0, part).start()
            r2(1, part).start()

    for part in range(2):
        @pl.when(z > 0)
        def _(part=part):
            r1(0, part).start()

        @pl.when(z < 3)
        def _(part=part):
            r1(1, part).start()

    def kv_at(owner, c):
        start = jnp.where(c < chunks // 2, owner, 2 * n_cp - 1 - owner) * piece + (c % (chunks // 2)) * c_rows
        return kvg_ref.at[pl.ds(pl.multiple_of(start, c_rows), c_rows)]

    def kv_local(c):
        return pltpu.make_async_copy(kvbuf.at[pl.ds(c * c_rows, c_rows)], kv_at(cp, c), kvl_sem.at[c])

    def kv_copy(kind, c):
        at = kv_at((cp, cp, y_cp)[kind], c)
        return remote(at, at, kv_send.at[kind, c], kv_recv.at[kind, c], (ynb, core, core)[kind])

    def kv_wait(kind, c):
        at = kv_at((y_cp, core_cp, lax.rem(core_cp + 2, 4))[kind], c)
        remote(at, at, kv_send.at[kind, c], kv_recv.at[kind, c], core).wait_recv()

    def kv_out(c):
        kv_local(c).wait()
        kv_copy(0, c).start()
        kv_copy(1, c).start()

    def cache_out(c):
        at = pl.ds(c * c_rows, c_rows)
        return (pltpu.make_async_copy(k3buf.at[at], k_ref.at[at], kv3_sem.at[0, c]),
                pltpu.make_async_copy(v3buf.at[at], v_ref.at[at], kv3_sem.at[1, c]))

    step = 16

    for cpy in small:
        cpy.wait()

    pos_cols = jnp.transpose(posbuf[...].astype(F32))
    for i in range(rows // HEAD):
        angle = pos_cols[:, i:i + 1] * freqbuf[...]
        cos_h, sin_h = jnp.cos(angle), jnp.sin(angle)
        cosbuf[i * HEAD:(i + 1) * HEAD, :] = jnp.concatenate([cos_h, cos_h], axis=-1)
        sinbuf[i * HEAD:(i + 1) * HEAD, :] = jnp.concatenate([-sin_h, sin_h], axis=-1)

    def turn(vec, r_at):
        return rope(vec, cosbuf[r_at, :], sinbuf[r_at, :])

    for c in range(chunks):
        x_load(c).wait()

        def square_rows(i, _, c=c):
            at = pl.ds(pl.multiple_of(i * step, step), step)
            xf = xbuf[c, at, :].astype(F32)
            mean = jnp.sum(xf * xf, axis=-1, keepdims=True) * (1.0 / width)
            invbuf[at, :] = jnp.broadcast_to(lax.rsqrt(mean + 1e-5), (step, HEAD))
            return 0

        def norm_rows(i, _, c=c):
            at = pl.ds(pl.multiple_of(i * step, step), step)
            to = pl.ds(pl.multiple_of(c * c_rows + i * step, step), step)
            inv = invbuf[at, 0:1]
            hbuf[to, :] = (xbuf[c, at, :].astype(F32) * inv * gainbuf[...]).astype(BF16)
            return 0

        lax.fori_loop(0, c_rows // step, square_rows, 0, unroll=4)
        lax.fori_loop(0, c_rows // step, norm_rows, 0, unroll=2)
        if c == 0:
            wk_load.wait()
            wv_load.wait()
        r_at = pl.ds(c * c_rows, c_rows)
        h = hbuf[r_at, :]
        k_new = jnp.dot(h, wkbuf[...], preferred_element_type=F32).astype(BF16)
        v_new = jnp.dot(h, wvbuf[...], preferred_element_type=F32).astype(BF16)
        for j in range(cols // HEAD):
            at = slice(j * HEAD, (j + 1) * HEAD)
            k_head = turn(k_new[:, at], r_at)
            kvbuf[r_at, at] = k_head
            k3buf[r_at, j, :] = k_head
            v3buf[r_at, j, :] = v_new[:, at]
        kvbuf[r_at, cols:] = v_new
        kv_local(c).start()
        for cpy in cache_out(c):
            cpy.start()
        if c > 0:
            kv_out(c - 1)

    second_hop(0)

    def q_out(t):
        return pltpu.make_async_copy(qbuf.at[t], q_ref.at[:, pl.ds(t * q_cols, q_cols)], q_sem.at[t])

    def q_tile(t):
        wq_load(t).wait()
        q_new = jnp.dot(hbuf[...], wqbuf[t], preferred_element_type=F32).astype(BF16)
        everything = pl.ds(0, rows)
        for j in range(q_cols // HEAD):
            qbuf[t, :, j * HEAD:(j + 1) * HEAD] = turn(q_new[:, j * HEAD:(j + 1) * HEAD], everything)
        q_out(t).start()

    q_tile(0)
    kv_out(chunks - 1)
    q_tile(1)
    for c in range(2):
        kv_wait(0, c)
        kv_copy(2, c).start()
    q_tile(2)
    second_hop(1)
    q_tile(3)
    for c in range(2, chunks):
        kv_wait(0, c)
        kv_copy(2, c).start()
    for c in range(chunks):
        kv_wait(1, c)
        kv_wait(2, c)
    for t in range(q_tiles):
        q_out(t).wait()
    for c in range(chunks):
        for cpy in cache_out(c):
            cpy.wait()

    for part in range(2):
        @pl.when(z > 0)
        def _(part=part):
            r1(0, part).wait_send()

        @pl.when(z < 3)
        def _(part=part):
            r1(1, part).wait_send()

        r2(0, part).wait_recv()

        @pl.when(is_mid)
        def _(part=part):
            r2(0, part).wait_send()
            r2(1, part).wait_send()

    for c in range(chunks):
        for kind in range(3):
            kv_copy(kind, c).wait_send()


def project(x, gain, w_k, w_v, w_q, w_o, pos, inv_freq):
    rows, width = x.shape
    cols = w_k.shape[1]
    q_cols = w_q.shape[1]
    w_rows = w_o.shape[0] // 8
    dma = pltpu.SemaphoreType.DMA
    hbm = pl.BlockSpec(memory_space=HBM)
    return pl.pallas_call(
        proj_kernel,
        in_specs=[hbm] * 8,
        out_specs=[hbm] * 8,
        out_shape=[HBM((rows, q_cols), BF16), HBM((4 * rows, 2 * cols), BF16)] + [HBM((rows, cols // HEAD, HEAD), BF16)] * 2
        + [HBM((w_rows, w_o.shape[1]), BF16)] * 2 + [HBM((w_rows // 2, w_o.shape[1]), BF16)] * 2,
        scratch_shapes=[
            VMEM((4, rows // 4, width), BF16),
            VMEM((rows, width), BF16),
            VMEM((rows // 4, HEAD), F32),
            VMEM((1, width), F32),
            VMEM((rows // HEAD, HEAD), jnp.int32),
            VMEM((1, HEAD // 2), F32),
            VMEM((rows, HEAD), F32),
            VMEM((rows, HEAD), F32),
            VMEM((width, cols), BF16),
            VMEM((width, cols), BF16),
            VMEM((4, width, q_cols // 4), BF16),
            VMEM((rows, 2 * cols), BF16),
            VMEM((rows, cols // HEAD, HEAD), BF16),
            VMEM((rows, cols // HEAD, HEAD), BF16),
            VMEM((4, rows, q_cols // 4), BF16),
            dma((4,)), dma((5,)), dma((4,)), dma((4,)), dma((2, 4)), dma((4,)),
            dma((3, 4)), dma((3, 4)), dma((2, 2)), dma((2, 2)), dma((2, 2)), dma((2,)),
        ],
        compiler_params=pltpu.CompilerParams(collective_id=0, has_side_effects=True, vmem_limit_bytes=VMEM_MAX),
        cost_estimate=pl.CostEstimate(flops=2 * rows * width * (2 * cols + q_cols), bytes_accessed=24 << 20, transcendentals=0),
        name="proj",
    )(x, gain.reshape(1, width), w_k, w_v, w_q, w_o, pos.reshape(rows // HEAD, HEAD), inv_freq.reshape(1, HEAD // 2))


def attn_kernel(pos_smem, q_ref, pos_ref, kv_ref, k_ref, v_ref, o_ref, k_out_ref, v_out_ref, kbuf, vbuf, in_sem, out_sem):
    blk = pl.program_id(0)

    cache = ((k_ref, kbuf, k_out_ref), (v_ref, vbuf, v_out_ref))
    loads = [pltpu.make_async_copy(src, buf, in_sem.at[i]) for i, (src, buf, _) in enumerate(cache)]
    stores = [pltpu.make_async_copy(buf, dst, out_sem.at[i]) for i, (_, buf, dst) in enumerate(cache)]

    @pl.when(blk == 0)
    def _():
        for c in loads:
            c.start()

    @pl.when(blk == 2)
    def _():
        for c, d in zip(loads, stores):
            c.wait()
            d.start()

    half_blks = pl.num_programs(0) // 2
    piece = half_blks * Q_TILE
    cp = lax.axis_index("cp")
    q_rows = Q_TILE
    kv_cols = kv_ref.shape[1] // 2
    heads = kv_cols // HEAD
    group = q_ref.shape[1] // kv_cols
    pieces = kv_ref.shape[0] // piece
    g0 = jnp.where(blk < half_blks, cp * piece + blk * Q_TILE, (pieces - 1 - cp) * piece + (blk - half_blks) * Q_TILE)
    low = (g0 - pos_smem[blk * Q_TILE]) // Q_TILE
    tok_1 = g0 + lax.broadcasted_iota(jnp.int32, (q_rows, 1), 0)
    tok = jnp.concatenate([tok_1] * group, axis=0)
    pos_cols = jnp.transpose(pos_ref[...].astype(F32))
    mine = lax.broadcasted_iota(jnp.int32, pos_cols.shape, 1) == blk
    pos_1 = jnp.sum(jnp.where(mine, pos_cols, 0.0), axis=1, keepdims=True).astype(jnp.int32)
    first = jnp.concatenate([tok_1 - pos_1] * group, axis=0)
    factor = HEAD ** -0.5 * 1.4426950408889634

    def head_q(n):
        return jnp.concatenate([q_ref[:, (n * group + g) * HEAD:(n * group + g + 1) * HEAD] for g in range(group)], axis=0)

    def scores(n, q, start, width):
        keys = kv_ref[pl.ds(pl.multiple_of(start, Q_TILE), width), n * HEAD:(n + 1) * HEAD]
        s = lax.dot_general(q, keys, (((1,), (1,)), ((), ())), preferred_element_type=F32)
        u = start + lax.broadcasted_iota(jnp.int32, (1, width), 1)
        return jnp.where((u >= first) & (u <= tok), s, -1e30)

    def values(n, start, width):
        return kv_ref[pl.ds(pl.multiple_of(start, Q_TILE), width), kv_cols + n * HEAD:kv_cols + (n + 1) * HEAD]

    near = jnp.maximum(g0 - Q_TILE, 0)
    states = []
    for n in range(heads):
        s = scores(n, head_q(n), near, 2 * Q_TILE)
        m = jnp.max(s, axis=-1, keepdims=True)
        p = jnp.exp2((s - m) * factor)
        total = jnp.sum(p, axis=-1, keepdims=True)
        acc = jnp.dot(p.astype(BF16), values(n, near, 2 * Q_TILE), preferred_element_type=F32)
        states.append((m, total, acc))

    def far(n, i, carry):
        m, total, acc = carry
        start = i * Q_TILE
        s = scores(n, head_q(n), start, Q_TILE)
        m_new = jnp.maximum(m, jnp.max(s, axis=-1, keepdims=True))
        old = jnp.exp2((m - m_new) * factor)
        p = jnp.exp2((s - m_new) * factor)
        total = total * old + jnp.sum(p, axis=-1, keepdims=True)
        acc = acc * old + jnp.dot(p.astype(BF16), values(n, start, Q_TILE), preferred_element_type=F32)
        return m_new, total, acc

    def put(n, state):
        out = (state[2] / state[1]).astype(BF16)
        for g in range(group):
            o_ref[:, (n * group + g) * HEAD:(n * group + g + 1) * HEAD] = out[g * q_rows:(g + 1) * q_rows]

    for n in range(heads):
        put(n, states[n])

    @pl.when(low < near // Q_TILE)
    def _():
        for n in range(heads):
            put(n, lax.fori_loop(low, near // Q_TILE, functools.partial(far, n), states[n]))

    @pl.when(blk == pl.num_programs(0) - 1)
    def _():
        for d in stores:
            d.wait()


def attention(q, kvg, pos, k, v):
    rows, q_cols = q.shape
    hbm, vmem = pl.BlockSpec(memory_space=HBM), pl.BlockSpec(memory_space=VMEM)
    return pl.pallas_call(
        attn_kernel,
        grid_spec=pltpu.PrefetchScalarGridSpec(
            num_scalar_prefetch=1,
            grid=(rows // Q_TILE,),
            in_specs=[pl.BlockSpec((Q_TILE, q_cols), lambda i, *_: (i, 0)), vmem, vmem, hbm, hbm],
            out_specs=[pl.BlockSpec((Q_TILE, q_cols), lambda i, *_: (i, 0)), hbm, hbm],
            scratch_shapes=[VMEM(k.shape, BF16), VMEM(v.shape, BF16), pltpu.SemaphoreType.DMA((2,)), pltpu.SemaphoreType.DMA((2,))],
        ),
        out_shape=[HBM((rows, q_cols), BF16), HBM(k.shape, BF16), HBM(v.shape, BF16)],
        compiler_params=pltpu.CompilerParams(vmem_limit_bytes=VMEM_MAX),
        cost_estimate=pl.CostEstimate(flops=5 << 30, bytes_accessed=8 << 20, transcendentals=0),
        name="attn",
    )(pos, q, pos.reshape(rows // HEAD, HEAD), kvg, k, v)


def out_kernel(o_ref, fl_ref, fr_ref, fara_ref, farb_ref, third_ref, wown_ref, x_ref, y_ref, wlast, olast_ref, alast_ref,
               wbuf, wtile, xtile, obuf, own, acc,
               load_sem, tile_sem, own_sem, wsend, wrecv, w3_send, w3_recv, own_send, fwd_send, o_recv):
    rows, kdim = o_ref.shape
    width = x_ref.shape[1]
    slice_rows = fl_ref.shape[0]
    half = slice_rows // 2
    chunks = own_send.shape[1]
    c_rows = rows // chunks
    n_tile = xtile.shape[2]
    y_cols = 1024
    dp, z, cp = lax.axis_index("dp"), lax.axis_index("tp"), lax.axis_index("cp")
    is_end = (z == 0) | (z == 3)
    is_mid = (z == 1) | (z == 2)
    core = {"cp": cp + 1 - 2 * lax.rem(cp, 2)}
    ynb = {"cp": lax.rem(cp + 2, 4)}
    xnb = {"dp": 1 - dp}
    left = {"tp": jnp.maximum(z - 1, 0)}
    right = {"tp": jnp.minimum(z + 1, 3)}
    p_own = dp * 4 + cp
    p_x = (1 - dp) * 4 + cp
    p_y = dp * 4 + lax.rem(cp + 2, 4)
    p_d = (1 - dp) * 4 + lax.rem(cp + 2, 4)
    p_core = dp * 4 + cp + 1 - 2 * lax.rem(cp, 2)
    low_side = z < 2
    s1 = jnp.where(low_side, 1 - z, 5 - z)
    s2 = jnp.where(low_side, 2, 1)
    s3 = jnp.where(low_side, 3, 0)

    def remote(src, dst, ssem, rsem, dev):
        return pltpu.make_async_remote_copy(src_ref=src, dst_ref=dst, send_sem=ssem, recv_sem=rsem, device_id=dev, device_id_type=MESH)

    barrier = pltpu.get_barrier_semaphore()
    for dev in (core, ynb, xnb):
        pl.semaphore_signal(barrier, inc=1, device_id=dev, device_id_type=MESH)

    @pl.when(z > 0)
    def _():
        pl.semaphore_signal(barrier, inc=1, device_id=left, device_id_type=MESH)

    @pl.when(z < 3)
    def _():
        pl.semaphore_signal(barrier, inc=1, device_id=right, device_id_type=MESH)

    own_load = pltpu.make_async_copy(o_ref, own, own_sem)
    own_load.start()

    def w_at(j, p, start=0, n=None):
        n = slice_rows if n is None else n
        at = pl.ds(pl.multiple_of(p * slice_rows + start, half), n)
        return wlast.at[at] if j == 2 else wbuf.at[j, at]

    def load_w(src, j, part):
        return pltpu.make_async_copy(src, w_at(j, p_own, part * half, half), load_sem.at[j, part])

    def parts_of(ref):
        return ref.at[pl.ds(0, half)], ref.at[pl.ds(half, half)]

    fl, fr, far, third = parts_of(fl_ref), parts_of(fr_ref), (fara_ref, farb_ref), (third_ref,)
    sources = ((fr, far, third), (fl, fr, far), (fr, fl, far), (fl, far, third))
    for zz in range(4):
        @pl.when(z == zz)
        def _(zz=zz):
            for j in range(3):
                for part, src in enumerate(sources[zz][j]):
                    load_w(src, j, part).start()

    @pl.when(is_end)
    def _():
        pl.semaphore_wait(barrier, 4)

    @pl.when(is_mid)
    def _():
        pl.semaphore_wait(barrier, 5)

    def w_copy(j, kind):
        dev = (xnb, ynb, core, ynb, xnb, core, core, core, core)[kind]
        src = (w_at(j, p_own), w_at(j, p_own), w_at(j, p_own), w_at(j, p_x, 0, half), w_at(j, p_y, half, half),
               w_at(j, p_x), w_at(j, p_y), w_at(j, p_d, 0, half), w_at(j, p_d, half, half))[kind]
        return remote(src, src, wsend.at[j, kind], wrecv.at[j, kind], dev)

    def core_p(p):
        return p + 1 - 2 * lax.rem(p, 2)

    def w_wait(j, kind):
        dst = (w_at(j, p_x), w_at(j, p_y), w_at(j, p_core), w_at(j, p_d, 0, half), w_at(j, p_d, half, half),
               w_at(j, core_p(p_x)), w_at(j, core_p(p_y)), w_at(j, core_p(p_d), 0, half), w_at(j, core_p(p_d), half, half))[kind]
        remote(dst, dst, wsend.at[j, kind], wrecv.at[j, kind], core).wait_recv()

    def spread_own(j):
        for kind in (0, 1, 2):
            w_copy(j, kind).start()

    def spread_relay(j):
        w_wait(j, 0)
        w_copy(j, 3).start()
        w_copy(j, 5).start()
        w_wait(j, 1)
        w_copy(j, 4).start()
        w_copy(j, 6).start()

    def spread_diag(j):
        w_wait(j, 3)
        w_copy(j, 7).start()
        w_wait(j, 4)
        w_copy(j, 8).start()

    def spread_done(j):
        for kind in (2, 5, 6, 7, 8):
            w_wait(j, kind)

    def slot_of(s, dev_z):
        return s - (s > dev_z).astype(jnp.int32)

    def o_at(s, c, dev_z=None):
        return obuf.at[slot_of(s, z if dev_z is None else dev_z), pl.ds(pl.multiple_of(c * c_rows, c_rows), c_rows)]

    def o_own(c, side):
        src = o_ref.at[pl.ds(c * c_rows, c_rows)]
        return remote(src, o_at(z, c, z + (-1, 1)[side]), own_send.at[side, c], o_recv.at[z, c], (left, right)[side])

    def o_fwd(s, c, side):
        return remote(o_at(s, c), o_at(s, c, z + (-1, 1)[side]), fwd_send.at[s, c], o_recv.at[s, c], (left, right)[side])

    def o_wait(s, c):
        remote(o_at(s, c), o_at(s, c), fwd_send.at[s, c], o_recv.at[s, c], left).wait_recv()

    def o_pass(s, c):
        o_wait(s, c)

        @pl.when(s < z)
        def _():
            o_fwd(s, c, 1).start()

        @pl.when(s > z)
        def _():
            o_fwd(s, c, 0).start()

    w3_at = w_at(2, p_own, half, half)
    w3 = remote(w3_at, w3_at, w3_send, w3_recv, {"tp": jnp.where(z == 1, 0, 3)})

    def send_own(c):
        @pl.when(z > 0)
        def _():
            o_own(c, 0).start()

        @pl.when(z < 3)
        def _():
            o_own(c, 1).start()

    send_own(0)

    @pl.when(is_mid)
    def _():
        load_w(third_ref, 2, 1).wait()
        w3.start()

    for c in range(1, chunks):
        send_own(c)

    for j in range(2):
        for part in range(2):
            load_w(third_ref, j, part).wait()
        spread_own(j)

    def tile_loads(n, slot):
        at = pl.ds(pl.multiple_of(n * n_tile, n_tile), n_tile)
        return (pltpu.make_async_copy(wown_ref.at[:, at], wtile.at[slot], tile_sem.at[0, slot]),
                pltpu.make_async_copy(x_ref.at[:, at], xtile.at[slot], tile_sem.at[1, slot]))

    n_steps = width // n_tile
    for cpy in tile_loads(0, 0):
        cpy.start()
    own_load.wait()

    def own_step(n, _):
        slot = lax.rem(n, 2)

        @pl.when(n + 1 < n_steps)
        def _():
            for cpy in tile_loads(n + 1, 1 - slot):
                cpy.start()

        for cpy in tile_loads(n, slot):
            cpy.wait()
        at = pl.ds(pl.multiple_of(n * n_tile, n_tile), n_tile)
        acc[:, at] = xtile[slot].astype(F32) + jnp.dot(own[...], wtile[slot], preferred_element_type=F32)
        return 0

    lax.fori_loop(0, n_steps, own_step, 0)

    def add_shard(j, s):
        wide = 512

        def step(n, _):
            at = pl.ds(pl.multiple_of(n * wide, wide), wide)
            acc[:, at] += jnp.dot(obuf[slot_of(s, z)], wbuf[j, :, at], preferred_element_type=F32)
            return 0

        lax.fori_loop(0, width // wide, step, 0)

    spread_relay(0)
    spread_relay(1)

    @pl.when(is_end)
    def _():
        remote(w3_at, w3_at, w3_send, w3_recv, left).wait_recv()

    load_w(third_ref, 2, 0).wait()
    spread_own(2)

    @pl.when(is_mid)
    def _():
        for c in range(chunks):
            o_pass(s1, c)
            o_pass(s2, c)

    spread_diag(0)
    spread_done(0)

    @pl.when(is_end)
    def _():
        for c in range(chunks):
            o_wait(s1, c)

    add_shard(0, s1)
    spread_diag(1)
    spread_done(1)

    @pl.when(is_mid)
    def _():
        for c in range(chunks):
            o_pass(s3, c)

    spread_relay(2)

    @pl.when(is_end)
    def _():
        for c in range(chunks):
            o_wait(s2, c)

    add_shard(1, s2)
    spread_diag(2)
    spread_done(2)

    y_steps = width // y_cols

    def last_step(i, _):
        c = i // y_steps

        @pl.when(is_end & (lax.rem(i, y_steps) == 0))
        def _():
            o_wait(s3, c)

        r_at = pl.ds(pl.multiple_of(c * c_rows, c_rows), c_rows)
        n_at = pl.ds(pl.multiple_of(lax.rem(i, y_steps) * y_cols, y_cols), y_cols)
        y_ref[r_at, n_at] = (acc[r_at, n_at] + jnp.dot(obuf[slot_of(s3, z), r_at, :], wlast[:, n_at], preferred_element_type=F32)).astype(BF16)
        return 0

    rest = pl.ds((chunks - 1) * c_rows, c_rows)
    alast_ref[...] = acc[rest, :]
    lax.fori_loop(0, (chunks - 1) * y_steps, last_step, 0)

    @pl.when(is_end)
    def _():
        o_wait(s3, chunks - 1)

    olast_ref[...] = obuf[slot_of(s3, z), rest, :]

    for j in range(3):
        for kind in range(9):
            w_copy(j, kind).wait_send()
    for c in range(chunks):
        @pl.when(z > 0)
        def _(c=c):
            o_own(c, 0).wait_send()

        @pl.when(z < 3)
        def _(c=c):
            o_own(c, 1).wait_send()

    @pl.when(is_mid)
    def _():
        w3.wait_send()
        for c in range(chunks):
            for s in (s1, s2, s3):
                o_fwd(s, c, 0).wait_send()


def out_proj(o, slices, w_own, x):
    rows, kdim = o.shape
    chunks = 8
    last = rows // chunks
    width = x.shape[1]
    dma = pltpu.SemaphoreType.DMA
    return pl.pallas_call(
        out_kernel,
        in_specs=[pl.BlockSpec(memory_space=HBM)] * 8,
        out_specs=[pl.BlockSpec(memory_space=VMEM)] * 4,
        out_shape=[
            VMEM((rows - last, width), BF16),
            VMEM((kdim, width), BF16),
            VMEM((last, kdim), BF16),
            VMEM((last, width), F32),
        ],
        scratch_shapes=[
            VMEM((2, kdim, width), BF16),
            VMEM((2, kdim, 256), BF16),
            VMEM((2, rows, 256), BF16),
            VMEM((3, rows, kdim), BF16),
            VMEM((rows, kdim), BF16),
            VMEM((rows, width), F32),
            dma((3, 2)), dma((2, 2)), dma, dma((3, 9)), dma((3, 9)), dma, dma,
            dma((2, chunks)), dma((4, chunks)), dma((4, chunks)),
        ],
        compiler_params=pltpu.CompilerParams(collective_id=1, has_side_effects=True, vmem_limit_bytes=45 << 20),
        name="out_proj",
    )(o, *slices, w_own, x)


def settle_kernel(src_ref, w_ref, o_ref, acc_ref, y_ref, ytile, sem, last_sem):
    parts, tiles = sem.shape[0], last_sem.shape[0]
    rows = src_ref.shape[0] // parts
    copies = [pltpu.make_async_copy(src_ref.at[pl.ds(i * rows, rows)], y_ref.at[pl.ds(i * rows, rows)], sem.at[i]) for i in range(parts)]
    for c in copies:
        c.start()
    cols = w_ref.shape[1] // tiles
    for t in range(tiles):
        at = pl.ds(t * cols, cols)
        ytile[:, at] = (acc_ref[:, at] + jnp.dot(o_ref[...], w_ref[:, at], preferred_element_type=F32)).astype(BF16)
        copies.append(pltpu.make_async_copy(ytile.at[:, at], y_ref.at[pl.ds(src_ref.shape[0], ytile.shape[0]), at], last_sem.at[t]))
        copies[-1].start()
    for c in copies:
        c.wait()


def settle(y, w_last, o_last, acc_last):
    rows, width = y.shape
    last = o_last.shape[0]
    dma = pltpu.SemaphoreType.DMA
    return pl.pallas_call(
        settle_kernel,
        in_specs=[pl.BlockSpec(memory_space=VMEM)] * 4,
        out_specs=pl.BlockSpec(memory_space=HBM),
        out_shape=HBM((rows + last, width), y.dtype),
        scratch_shapes=[VMEM((last, width), BF16), dma((7,)), dma((4,))],
        compiler_params=pltpu.CompilerParams(vmem_limit_bytes=16 << 20),
        name="settle",
    )(in_vmem(y), in_vmem(w_last), in_vmem(o_last), in_vmem(acc_last))


def solution(mesh):
    def local_step(x_in, doc_id, pos_in_doc, norm_gain, w_q, w_k, w_v, w_o, inv_freq):
        rows = x_in.shape[0]
        q, kvg, k_new, v_new, fl, fr, fara, farb = project(x_in, norm_gain, w_k, w_v, w_q, w_o, pos_in_doc, inv_freq)
        third = lax.ppermute(fara, "tp", [(1, 0), (2, 3)])
        o, k_out, v_out = attention(q, kvg, pos_in_doc, k_new, v_new)
        y = settle(*out_proj(o, (fl, fr, fara, farb, third), w_o, x_in))
        return y, k_out, v_out

    row_spec = P(("dp", "cp"))
    in_specs = (P(("dp", "cp"), None), row_spec, row_spec, P(), P(None, "tp"), P(None, "tp"), P(None, "tp"), P("tp", None), P())
    out_specs = (P(("dp", "cp"), None), P(("dp", "cp"), "tp", None), P(("dp", "cp"), "tp", None))
    return jax.shard_map(local_step, mesh=mesh, in_specs=in_specs, out_specs=out_specs, check_vma=False)
```

```python
import functools

import jax
import jax.numpy as jnp
from jax import lax
from jax.experimental import pallas as pl
from jax.experimental.pallas import tpu as pltpu
from jax.sharding import PartitionSpec as P

MESH = pl.DeviceIdType.MESH
HBM = pltpu.HBM
VMEM = pltpu.VMEM
HEAD = 128
Q_TILE = 128
VMEM_MAX = 67043328
F32 = jnp.float32
BF16 = jnp.bfloat16


def in_vmem(arr):
    return pltpu.with_memory_space_constraint(arr, VMEM)


def rope(vec, cos_t, sin_t):
    vec = vec.astype(F32)
    return (vec * cos_t + pltpu.roll(vec, HEAD // 2, 1) * sin_t).astype(BF16)


def proj_kernel(x_ref, gain_ref, wk_ref, wv_ref, wq_ref, wo_ref, pos_ref, freq_ref,
                q_ref, kvg_ref, k_ref, v_ref, fl_ref, fr_ref, fara_ref, farb_ref,
                xbuf, hbuf, invbuf, gainbuf, posbuf, freqbuf, cosbuf, sinbuf, wkbuf, wvbuf, wqbuf, kvbuf, k3buf, v3buf, qbuf,
                x_sem, w_sem, wq_sem, kvl_sem, kv3_sem, q_sem, kv_send, kv_recv, r1_send, r1_recv, r2_send, r2_recv):
    chunks, q_tiles = 4, 4
    rows, width = hbuf.shape
    c_rows = rows // chunks
    piece = rows // 2
    cols = wkbuf.shape[1]
    q_cols = wqbuf.shape[2]
    half = fl_ref.shape[0] // 2
    n_cp = 4
    dp, z, cp = lax.axis_index("dp"), lax.axis_index("tp"), lax.axis_index("cp")
    core_cp = cp + 1 - 2 * lax.rem(cp, 2)
    y_cp = lax.rem(cp + 2, 4)
    core, ynb = {"cp": core_cp}, {"cp": y_cp}
    left = {"tp": jnp.maximum(z - 1, 0)}
    right = {"tp": jnp.minimum(z + 1, 3)}
    is_mid = (z == 1) | (z == 2)

    def remote(src, dst, ssem, rsem, dev):
        return pltpu.make_async_remote_copy(src_ref=src, dst_ref=dst, send_sem=ssem, recv_sem=rsem, device_id=dev, device_id_type=MESH)

    barrier = pltpu.get_barrier_semaphore()
    for dev in (core, ynb):
        pl.semaphore_signal(barrier, inc=1, device_id=dev, device_id_type=MESH)

    @pl.when(z > 0)
    def _():
        pl.semaphore_signal(barrier, inc=1, device_id=left, device_id_type=MESH)

    @pl.when(z < 3)
    def _():
        pl.semaphore_signal(barrier, inc=1, device_id=right, device_id_type=MESH)

    def x_load(c):
        return pltpu.make_async_copy(x_ref.at[pl.ds(c * c_rows, c_rows)], xbuf.at[c], x_sem.at[c])

    def wq_load(t):
        return pltpu.make_async_copy(wq_ref.at[:, pl.ds(t * q_cols, q_cols)], wqbuf.at[t], wq_sem.at[t])

    wk_load = pltpu.make_async_copy(wk_ref, wkbuf, w_sem.at[0])
    wv_load = pltpu.make_async_copy(wv_ref, wvbuf, w_sem.at[1])
    small = [pltpu.make_async_copy(src, dst, w_sem.at[2 + i]) for i, (src, dst) in enumerate(((gain_ref, gainbuf), (pos_ref, posbuf), (freq_ref, freqbuf)))]
    for cpy in small:
        cpy.start()
    x_load(0).start()
    wk_load.start()
    wv_load.start()
    for c in range(1, chunks):
        x_load(c).start()
    for t in range(q_tiles):
        wq_load(t).start()

    @pl.when(is_mid)
    def _():
        pl.semaphore_wait(barrier, 4)

    @pl.when(jnp.logical_not(is_mid))
    def _():
        pl.semaphore_wait(barrier, 3)

    p_own = dp * 4 + cp

    def part_of(ref, part):
        return ref.at[pl.ds(part * half, half)]

    def r1(side, part):
        src = wo_ref.at[pl.ds(pl.multiple_of((p_own * 2 + part) * half, half), half)]
        dst = part_of((fr_ref, fl_ref)[side], part)
        return remote(src, dst, r1_send.at[side, part], r1_recv.at[side, part], (left, right)[side])

    def r2(side, part):
        src = part_of((fr_ref, fl_ref)[side], part)
        return remote(src, (fara_ref, farb_ref)[part], r2_send.at[side, part], r2_recv.at[part], (left, right)[side])

    def second_hop(part):
        @pl.when(z > 0)
        def _():
            r1(1, part).wait_recv()

        @pl.when(z < 3)
        def _():
            r1(0, part).wait_recv()

        @pl.when(is_mid)
        def _():
            r2(0, part).start()
            r2(1, part).start()

    for part in range(2):
        @pl.when(z > 0)
        def _(part=part):
            r1(0, part).start()

        @pl.when(z < 3)
        def _(part=part):
            r1(1, part).start()

    def kv_at(owner, c):
        start = jnp.where(c < chunks // 2, owner, 2 * n_cp - 1 - owner) * piece + (c % (chunks // 2)) * c_rows
        return kvg_ref.at[pl.ds(pl.multiple_of(start, c_rows), c_rows)]

    def kv_local(c):
        return pltpu.make_async_copy(kvbuf.at[pl.ds(c * c_rows, c_rows)], kv_at(cp, c), kvl_sem.at[c])

    def kv_copy(kind, c):
        at = kv_at((cp, cp, y_cp)[kind], c)
        return remote(at, at, kv_send.at[kind, c], kv_recv.at[kind, c], (ynb, core, core)[kind])

    def kv_wait(kind, c):
        at = kv_at((y_cp, core_cp, lax.rem(core_cp + 2, 4))[kind], c)
        remote(at, at, kv_send.at[kind, c], kv_recv.at[kind, c], core).wait_recv()

    def kv_out(c):
        kv_local(c).wait()
        kv_copy(0, c).start()
        kv_copy(1, c).start()

    def cache_out(c):
        at = pl.ds(c * c_rows, c_rows)
        return (pltpu.make_async_copy(k3buf.at[at], k_ref.at[at], kv3_sem.at[0, c]),
                pltpu.make_async_copy(v3buf.at[at], v_ref.at[at], kv3_sem.at[1, c]))

    step = 16

    for cpy in small:
        cpy.wait()

    pos_cols = jnp.transpose(posbuf[...].astype(F32))
    for i in range(rows // HEAD):
        angle = pos_cols[:, i:i + 1] * freqbuf[...]
        cos_h, sin_h = jnp.cos(angle), jnp.sin(angle)
        cosbuf[i * HEAD:(i + 1) * HEAD, :] = jnp.concatenate([cos_h, cos_h], axis=-1)
        sinbuf[i * HEAD:(i + 1) * HEAD, :] = jnp.concatenate([-sin_h, sin_h], axis=-1)

    def turn(vec, r_at):
        return rope(vec, cosbuf[r_at, :], sinbuf[r_at, :])

    for c in range(chunks):
        x_load(c).wait()

        def square_rows(i, _, c=c):
            at = pl.ds(pl.multiple_of(i * step, step), step)
            xf = xbuf[c, at, :].astype(F32)
            mean = jnp.sum(xf * xf, axis=-1, keepdims=True) * (1.0 / width)
            invbuf[at, :] = jnp.broadcast_to(lax.rsqrt(mean + 1e-5), (step, HEAD))
            return 0

        def norm_rows(i, _, c=c):
            at = pl.ds(pl.multiple_of(i * step, step), step)
            to = pl.ds(pl.multiple_of(c * c_rows + i * step, step), step)
            inv = invbuf[at, 0:1]
            hbuf[to, :] = (xbuf[c, at, :].astype(F32) * inv * gainbuf[...]).astype(BF16)
            return 0

        lax.fori_loop(0, c_rows // step, square_rows, 0, unroll=4)
        lax.fori_loop(0, c_rows // step, norm_rows, 0, unroll=2)
        if c == 0:
            wk_load.wait()
            wv_load.wait()
        r_at = pl.ds(c * c_rows, c_rows)
        h = hbuf[r_at, :]
        k_new = jnp.dot(h, wkbuf[...], preferred_element_type=F32).astype(BF16)
        v_new = jnp.dot(h, wvbuf[...], preferred_element_type=F32).astype(BF16)
        for j in range(cols // HEAD):
            at = slice(j * HEAD, (j + 1) * HEAD)
            k_head = turn(k_new[:, at], r_at)
            kvbuf[r_at, at] = k_head
            k3buf[r_at, j, :] = k_head
            v3buf[r_at, j, :] = v_new[:, at]
        kvbuf[r_at, cols:] = v_new
        kv_local(c).start()
        for cpy in cache_out(c):
            cpy.start()
        if c > 0:
            kv_out(c - 1)

    second_hop(0)

    def q_out(t):
        return pltpu.make_async_copy(qbuf.at[t], q_ref.at[:, pl.ds(t * q_cols, q_cols)], q_sem.at[t])

    def q_tile(t):
        wq_load(t).wait()
        q_new = jnp.dot(hbuf[...], wqbuf[t], preferred_element_type=F32).astype(BF16)
        everything = pl.ds(0, rows)
        for j in range(q_cols // HEAD):
            qbuf[t, :, j * HEAD:(j + 1) * HEAD] = turn(q_new[:, j * HEAD:(j + 1) * HEAD], everything)
        q_out(t).start()

    q_tile(0)
    kv_out(chunks - 1)
    q_tile(1)
    for c in range(2):
        kv_wait(0, c)
        kv_copy(2, c).start()
    q_tile(2)
    second_hop(1)
    q_tile(3)
    for c in range(2, chunks):
        kv_wait(0, c)
        kv_copy(2, c).start()
    for c in range(chunks):
        kv_wait(1, c)
        kv_wait(2, c)
    for t in range(q_tiles):
        q_out(t).wait()
    for c in range(chunks):
        for cpy in cache_out(c):
            cpy.wait()

    for part in range(2):
        @pl.when(z > 0)
        def _(part=part):
            r1(0, part).wait_send()

        @pl.when(z < 3)
        def _(part=part):
            r1(1, part).wait_send()

        r2(0, part).wait_recv()

        @pl.when(is_mid)
        def _(part=part):
            r2(0, part).wait_send()
            r2(1, part).wait_send()

    for c in range(chunks):
        for kind in range(3):
            kv_copy(kind, c).wait_send()


def project(x, gain, w_k, w_v, w_q, w_o, pos, inv_freq):
    rows, width = x.shape
    cols = w_k.shape[1]
    q_cols = w_q.shape[1]
    w_rows = w_o.shape[0] // 8
    dma = pltpu.SemaphoreType.DMA
    hbm = pl.BlockSpec(memory_space=HBM)
    return pl.pallas_call(
        proj_kernel,
        in_specs=[hbm] * 8,
        out_specs=[hbm] * 8,
        out_shape=[HBM((rows, q_cols), BF16), HBM((4 * rows, 2 * cols), BF16)] + [HBM((rows, cols // HEAD, HEAD), BF16)] * 2
        + [HBM((w_rows, w_o.shape[1]), BF16)] * 2 + [HBM((w_rows // 2, w_o.shape[1]), BF16)] * 2,
        scratch_shapes=[
            VMEM((4, rows // 4, width), BF16),
            VMEM((rows, width), BF16),
            VMEM((rows // 4, HEAD), F32),
            VMEM((1, width), F32),
            VMEM((rows // HEAD, HEAD), jnp.int32),
            VMEM((1, HEAD // 2), F32),
            VMEM((rows, HEAD), F32),
            VMEM((rows, HEAD), F32),
            VMEM((width, cols), BF16),
            VMEM((width, cols), BF16),
            VMEM((4, width, q_cols // 4), BF16),
            VMEM((rows, 2 * cols), BF16),
            VMEM((rows, cols // HEAD, HEAD), BF16),
            VMEM((rows, cols // HEAD, HEAD), BF16),
            VMEM((4, rows, q_cols // 4), BF16),
            dma((4,)), dma((5,)), dma((4,)), dma((4,)), dma((2, 4)), dma((4,)),
            dma((3, 4)), dma((3, 4)), dma((2, 2)), dma((2, 2)), dma((2, 2)), dma((2,)),
        ],
        compiler_params=pltpu.CompilerParams(collective_id=0, has_side_effects=True, vmem_limit_bytes=VMEM_MAX),
        cost_estimate=pl.CostEstimate(flops=2 * rows * width * (2 * cols + q_cols), bytes_accessed=24 << 20, transcendentals=0),
        name="proj",
    )(x, gain.reshape(1, width), w_k, w_v, w_q, w_o, pos.reshape(rows // HEAD, HEAD), inv_freq.reshape(1, HEAD // 2))


def attn_kernel(pos_smem, q_ref, pos_ref, kv_ref, k_ref, v_ref, o_ref, k_out_ref, v_out_ref, kbuf, vbuf, in_sem, out_sem):
    blk = pl.program_id(0)

    cache = ((k_ref, kbuf, k_out_ref), (v_ref, vbuf, v_out_ref))
    loads = [pltpu.make_async_copy(src, buf, in_sem.at[i]) for i, (src, buf, _) in enumerate(cache)]
    stores = [pltpu.make_async_copy(buf, dst, out_sem.at[i]) for i, (_, buf, dst) in enumerate(cache)]

    @pl.when(blk == 0)
    def _():
        for c in loads:
            c.start()

    @pl.when(blk == 2)
    def _():
        for c, d in zip(loads, stores):
            c.wait()
            d.start()

    half_blks = pl.num_programs(0) // 2
    piece = half_blks * Q_TILE
    cp = lax.axis_index("cp")
    q_rows = Q_TILE
    kv_cols = kv_ref.shape[1] // 2
    heads = kv_cols // HEAD
    group = q_ref.shape[1] // kv_cols
    pieces = kv_ref.shape[0] // piece
    g0 = jnp.where(blk < half_blks, cp * piece + blk * Q_TILE, (pieces - 1 - cp) * piece + (blk - half_blks) * Q_TILE)
    low = (g0 - pos_smem[blk * Q_TILE]) // Q_TILE
    tok_1 = g0 + lax.broadcasted_iota(jnp.int32, (q_rows, 1), 0)
    tok = jnp.concatenate([tok_1] * group, axis=0)
    pos_cols = jnp.transpose(pos_ref[...].astype(F32))
    mine = lax.broadcasted_iota(jnp.int32, pos_cols.shape, 1) == blk
    pos_1 = jnp.sum(jnp.where(mine, pos_cols, 0.0), axis=1, keepdims=True).astype(jnp.int32)
    first = jnp.concatenate([tok_1 - pos_1] * group, axis=0)
    factor = HEAD ** -0.5 * 1.4426950408889634

    def head_q(n):
        return jnp.concatenate([q_ref[:, (n * group + g) * HEAD:(n * group + g + 1) * HEAD] for g in range(group)], axis=0)

    def scores(n, q, start, width):
        keys = kv_ref[pl.ds(pl.multiple_of(start, Q_TILE), width), n * HEAD:(n + 1) * HEAD]
        s = lax.dot_general(q, keys, (((1,), (1,)), ((), ())), preferred_element_type=F32)
        u = start + lax.broadcasted_iota(jnp.int32, (1, width), 1)
        return jnp.where((u >= first) & (u <= tok), s, -1e30)

    def values(n, start, width):
        return kv_ref[pl.ds(pl.multiple_of(start, Q_TILE), width), kv_cols + n * HEAD:kv_cols + (n + 1) * HEAD]

    near = jnp.maximum(g0 - Q_TILE, 0)
    wide = 2 * Q_TILE

    def probs(s, m, inv):
        return (jnp.exp2((s - m) * factor) * inv).astype(BF16)

    def put(n, acc):
        out = acc.astype(BF16)
        for g in range(group):
            o_ref[:, (n * group + g) * HEAD:(n * group + g + 1) * HEAD] = out[g * q_rows:(g + 1) * q_rows]

    states = []
    for n in range(heads):
        s = scores(n, head_q(n), near, wide)
        m = jnp.max(s, axis=-1, keepdims=True)
        e = jnp.exp2((s - m) * factor)
        total = jnp.sum(e, axis=-1, keepdims=True)
        p = (e * (1.0 / total)).astype(BF16)
        put(n, jnp.dot(p, values(n, near, wide), preferred_element_type=F32))
        states.append((m, total))

    @pl.when(low < near // Q_TILE)
    def _():
        for n in range(heads):
            def far_sum(i, carry, n=n):
                m, total = carry
                s = scores(n, head_q(n), i * Q_TILE, Q_TILE)
                m_new = jnp.maximum(m, jnp.max(s, axis=-1, keepdims=True))
                part = jnp.sum(jnp.exp2((s - m_new) * factor), axis=-1, keepdims=True)
                return m_new, total * jnp.exp2((m - m_new) * factor) + part

            m, total = lax.fori_loop(low, near // Q_TILE, far_sum, states[n])
            inv = 1.0 / total

            def far_pv(i, acc, n=n, m=m, inv=inv):
                p = probs(scores(n, head_q(n), i * Q_TILE, Q_TILE), m, inv)
                return acc + jnp.dot(p, values(n, i * Q_TILE, Q_TILE), preferred_element_type=F32)

            p = probs(scores(n, head_q(n), near, wide), m, inv)
            acc = jnp.dot(p, values(n, near, wide), preferred_element_type=F32)
            put(n, lax.fori_loop(low, near // Q_TILE, far_pv, acc))

    @pl.when(blk == pl.num_programs(0) - 1)
    def _():
        for d in stores:
            d.wait()


def attention(q, kvg, pos, k, v):
    rows, q_cols = q.shape
    hbm, vmem = pl.BlockSpec(memory_space=HBM), pl.BlockSpec(memory_space=VMEM)
    return pl.pallas_call(
        attn_kernel,
        grid_spec=pltpu.PrefetchScalarGridSpec(
            num_scalar_prefetch=1,
            grid=(rows // Q_TILE,),
            in_specs=[pl.BlockSpec((Q_TILE, q_cols), lambda i, *_: (i, 0)), vmem, vmem, hbm, hbm],
            out_specs=[pl.BlockSpec((Q_TILE, q_cols), lambda i, *_: (i, 0)), hbm, hbm],
            scratch_shapes=[VMEM(k.shape, BF16), VMEM(v.shape, BF16), pltpu.SemaphoreType.DMA((2,)), pltpu.SemaphoreType.DMA((2,))],
        ),
        out_shape=[HBM((rows, q_cols), BF16), HBM(k.shape, BF16), HBM(v.shape, BF16)],
        compiler_params=pltpu.CompilerParams(vmem_limit_bytes=VMEM_MAX),
        cost_estimate=pl.CostEstimate(flops=5 << 30, bytes_accessed=8 << 20, transcendentals=0),
        name="attn",
    )(pos, q, pos.reshape(rows // HEAD, HEAD), kvg, k, v)


def out_kernel(o_ref, fl_ref, fr_ref, fara_ref, farb_ref, third_ref, wown_ref, x_ref, y_ref, wlast, olast_ref, alast_ref,
               wbuf, wtile, xtile, obuf, own, acc,
               load_sem, tile_sem, own_sem, wsend, wrecv, w3_send, w3_recv, own_send, fwd_send, o_recv):
    rows, kdim = o_ref.shape
    width = x_ref.shape[1]
    slice_rows = fl_ref.shape[0]
    half = slice_rows // 2
    chunks = own_send.shape[1]
    c_rows = rows // chunks
    n_tile = xtile.shape[2]
    y_cols = 1024
    dp, z, cp = lax.axis_index("dp"), lax.axis_index("tp"), lax.axis_index("cp")
    is_end = (z == 0) | (z == 3)
    is_mid = (z == 1) | (z == 2)
    core = {"cp": cp + 1 - 2 * lax.rem(cp, 2)}
    ynb = {"cp": lax.rem(cp + 2, 4)}
    xnb = {"dp": 1 - dp}
    left = {"tp": jnp.maximum(z - 1, 0)}
    right = {"tp": jnp.minimum(z + 1, 3)}
    p_own = dp * 4 + cp
    p_x = (1 - dp) * 4 + cp
    p_y = dp * 4 + lax.rem(cp + 2, 4)
    p_d = (1 - dp) * 4 + lax.rem(cp + 2, 4)
    p_core = dp * 4 + cp + 1 - 2 * lax.rem(cp, 2)
    low_side = z < 2
    s1 = jnp.where(low_side, 1 - z, 5 - z)
    s2 = jnp.where(low_side, 2, 1)
    s3 = jnp.where(low_side, 3, 0)

    def remote(src, dst, ssem, rsem, dev):
        return pltpu.make_async_remote_copy(src_ref=src, dst_ref=dst, send_sem=ssem, recv_sem=rsem, device_id=dev, device_id_type=MESH)

    barrier = pltpu.get_barrier_semaphore()
    for dev in (core, ynb, xnb):
        pl.semaphore_signal(barrier, inc=1, device_id=dev, device_id_type=MESH)

    @pl.when(z > 0)
    def _():
        pl.semaphore_signal(barrier, inc=1, device_id=left, device_id_type=MESH)

    @pl.when(z < 3)
    def _():
        pl.semaphore_signal(barrier, inc=1, device_id=right, device_id_type=MESH)

    own_load = pltpu.make_async_copy(o_ref, own, own_sem)
    own_load.start()

    def w_at(j, p, start=0, n=None):
        n = slice_rows if n is None else n
        at = pl.ds(pl.multiple_of(p * slice_rows + start, half), n)
        return wlast.at[at] if j == 2 else wbuf.at[j, at]

    def load_w(src, j, part):
        return pltpu.make_async_copy(src, w_at(j, p_own, part * half, half), load_sem.at[j, part])

    def parts_of(ref):
        return ref.at[pl.ds(0, half)], ref.at[pl.ds(half, half)]

    fl, fr, far, third = parts_of(fl_ref), parts_of(fr_ref), (fara_ref, farb_ref), (third_ref,)
    sources = ((fr, far, third), (fl, fr, far), (fr, fl, far), (fl, far, third))
    for zz in range(4):
        @pl.when(z == zz)
        def _(zz=zz):
            for j in range(3):
                for part, src in enumerate(sources[zz][j]):
                    load_w(src, j, part).start()

    @pl.when(is_end)
    def _():
        pl.semaphore_wait(barrier, 4)

    @pl.when(is_mid)
    def _():
        pl.semaphore_wait(barrier, 5)

    def w_copy(j, kind):
        dev = (xnb, ynb, core, ynb, xnb, core, core, core, core)[kind]
        src = (w_at(j, p_own), w_at(j, p_own), w_at(j, p_own), w_at(j, p_x, 0, half), w_at(j, p_y, half, half),
               w_at(j, p_x), w_at(j, p_y), w_at(j, p_d, 0, half), w_at(j, p_d, half, half))[kind]
        return remote(src, src, wsend.at[j, kind], wrecv.at[j, kind], dev)

    def core_p(p):
        return p + 1 - 2 * lax.rem(p, 2)

    def w_wait(j, kind):
        dst = (w_at(j, p_x), w_at(j, p_y), w_at(j, p_core), w_at(j, p_d, 0, half), w_at(j, p_d, half, half),
               w_at(j, core_p(p_x)), w_at(j, core_p(p_y)), w_at(j, core_p(p_d), 0, half), w_at(j, core_p(p_d), half, half))[kind]
        remote(dst, dst, wsend.at[j, kind], wrecv.at[j, kind], core).wait_recv()

    def spread_own(j):
        for kind in (0, 1, 2):
            w_copy(j, kind).start()

    def spread_relay(j):
        w_wait(j, 0)
        w_copy(j, 3).start()
        w_copy(j, 5).start()
        w_wait(j, 1)
        w_copy(j, 4).start()
        w_copy(j, 6).start()

    def spread_diag(j):
        w_wait(j, 3)
        w_copy(j, 7).start()
        w_wait(j, 4)
        w_copy(j, 8).start()

    def spread_done(j):
        for kind in (2, 5, 6, 7, 8):
            w_wait(j, kind)

    def slot_of(s, dev_z):
        return s - (s > dev_z).astype(jnp.int32)

    def o_at(s, c, dev_z=None):
        return obuf.at[slot_of(s, z if dev_z is None else dev_z), pl.ds(pl.multiple_of(c * c_rows, c_rows), c_rows)]

    def o_own(c, side):
        src = o_ref.at[pl.ds(c * c_rows, c_rows)]
        return remote(src, o_at(z, c, z + (-1, 1)[side]), own_send.at[side, c], o_recv.at[z, c], (left, right)[side])

    def o_fwd(s, c, side):
        return remote(o_at(s, c), o_at(s, c, z + (-1, 1)[side]), fwd_send.at[s, c], o_recv.at[s, c], (left, right)[side])

    def o_wait(s, c):
        remote(o_at(s, c), o_at(s, c), fwd_send.at[s, c], o_recv.at[s, c], left).wait_recv()

    def o_pass(s, c):
        o_wait(s, c)

        @pl.when(s < z)
        def _():
            o_fwd(s, c, 1).start()

        @pl.when(s > z)
        def _():
            o_fwd(s, c, 0).start()

    w3_at = w_at(2, p_own, half, half)
    w3 = remote(w3_at, w3_at, w3_send, w3_recv, {"tp": jnp.where(z == 1, 0, 3)})

    def send_own(c):
        @pl.when(z > 0)
        def _():
            o_own(c, 0).start()

        @pl.when(z < 3)
        def _():
            o_own(c, 1).start()

    send_own(0)

    @pl.when(is_mid)
    def _():
        load_w(third_ref, 2, 1).wait()
        w3.start()

    for c in range(1, chunks):
        send_own(c)

    for j in range(2):
        for part in range(2):
            load_w(third_ref, j, part).wait()
        spread_own(j)

    def tile_loads(n, slot):
        at = pl.ds(pl.multiple_of(n * n_tile, n_tile), n_tile)
        return (pltpu.make_async_copy(wown_ref.at[:, at], wtile.at[slot], tile_sem.at[0, slot]),
                pltpu.make_async_copy(x_ref.at[:, at], xtile.at[slot], tile_sem.at[1, slot]))

    n_steps = width // n_tile
    for cpy in tile_loads(0, 0):
        cpy.start()
    own_load.wait()

    def own_step(n, _):
        slot = lax.rem(n, 2)

        @pl.when(n + 1 < n_steps)
        def _():
            for cpy in tile_loads(n + 1, 1 - slot):
                cpy.start()

        for cpy in tile_loads(n, slot):
            cpy.wait()
        at = pl.ds(pl.multiple_of(n * n_tile, n_tile), n_tile)
        acc[:, at] = xtile[slot].astype(F32) + jnp.dot(own[...], wtile[slot], preferred_element_type=F32)
        return 0

    lax.fori_loop(0, n_steps, own_step, 0)

    def add_shard(j, s):
        wide = 512

        def step(n, _):
            at = pl.ds(pl.multiple_of(n * wide, wide), wide)
            acc[:, at] += jnp.dot(obuf[slot_of(s, z)], wbuf[j, :, at], preferred_element_type=F32)
            return 0

        lax.fori_loop(0, width // wide, step, 0)

    spread_relay(0)
    spread_relay(1)

    @pl.when(is_end)
    def _():
        remote(w3_at, w3_at, w3_send, w3_recv, left).wait_recv()

    load_w(third_ref, 2, 0).wait()
    spread_own(2)

    @pl.when(is_mid)
    def _():
        for c in range(chunks):
            o_pass(s1, c)
            o_pass(s2, c)

    spread_diag(0)
    spread_done(0)

    @pl.when(is_end)
    def _():
        for c in range(chunks):
            o_wait(s1, c)

    add_shard(0, s1)
    spread_diag(1)
    spread_done(1)

    @pl.when(is_mid)
    def _():
        for c in range(chunks):
            o_pass(s3, c)

    spread_relay(2)

    @pl.when(is_end)
    def _():
        for c in range(chunks):
            o_wait(s2, c)

    add_shard(1, s2)
    spread_diag(2)
    spread_done(2)

    y_steps = width // y_cols

    def last_step(i, _):
        c = i // y_steps

        @pl.when(is_end & (lax.rem(i, y_steps) == 0))
        def _():
            o_wait(s3, c)

        r_at = pl.ds(pl.multiple_of(c * c_rows, c_rows), c_rows)
        n_at = pl.ds(pl.multiple_of(lax.rem(i, y_steps) * y_cols, y_cols), y_cols)
        y_ref[r_at, n_at] = (acc[r_at, n_at] + jnp.dot(obuf[slot_of(s3, z), r_at, :], wlast[:, n_at], preferred_element_type=F32)).astype(BF16)
        return 0

    rest = pl.ds((chunks - 1) * c_rows, c_rows)
    alast_ref[...] = acc[rest, :]
    lax.fori_loop(0, (chunks - 1) * y_steps, last_step, 0)

    @pl.when(is_end)
    def _():
        o_wait(s3, chunks - 1)

    olast_ref[...] = obuf[slot_of(s3, z), rest, :]

    for j in range(3):
        for kind in range(9):
            w_copy(j, kind).wait_send()
    for c in range(chunks):
        @pl.when(z > 0)
        def _(c=c):
            o_own(c, 0).wait_send()

        @pl.when(z < 3)
        def _(c=c):
            o_own(c, 1).wait_send()

    @pl.when(is_mid)
    def _():
        w3.wait_send()
        for c in range(chunks):
            for s in (s1, s2, s3):
                o_fwd(s, c, 0).wait_send()


def out_proj(o, slices, w_own, x):
    rows, kdim = o.shape
    chunks = 8
    last = rows // chunks
    width = x.shape[1]
    dma = pltpu.SemaphoreType.DMA
    return pl.pallas_call(
        out_kernel,
        in_specs=[pl.BlockSpec(memory_space=HBM)] * 8,
        out_specs=[pl.BlockSpec(memory_space=VMEM)] * 4,
        out_shape=[
            VMEM((rows - last, width), BF16),
            VMEM((kdim, width), BF16),
            VMEM((last, kdim), BF16),
            VMEM((last, width), F32),
        ],
        scratch_shapes=[
            VMEM((2, kdim, width), BF16),
            VMEM((2, kdim, 256), BF16),
            VMEM((2, rows, 256), BF16),
            VMEM((3, rows, kdim), BF16),
            VMEM((rows, kdim), BF16),
            VMEM((rows, width), F32),
            dma((3, 2)), dma((2, 2)), dma, dma((3, 9)), dma((3, 9)), dma, dma,
            dma((2, chunks)), dma((4, chunks)), dma((4, chunks)),
        ],
        compiler_params=pltpu.CompilerParams(collective_id=1, has_side_effects=True, vmem_limit_bytes=45 << 20),
        name="out_proj",
    )(o, *slices, w_own, x)


def settle_kernel(src_ref, w_ref, o_ref, acc_ref, y_ref, ytile, sem, last_sem):
    parts, tiles = sem.shape[0], last_sem.shape[0]
    rows = src_ref.shape[0] // parts
    copies = [pltpu.make_async_copy(src_ref.at[pl.ds(i * rows, rows)], y_ref.at[pl.ds(i * rows, rows)], sem.at[i]) for i in range(parts)]
    for c in copies:
        c.start()
    cols = w_ref.shape[1] // tiles
    for t in range(tiles):
        at = pl.ds(t * cols, cols)
        ytile[:, at] = (acc_ref[:, at] + jnp.dot(o_ref[...], w_ref[:, at], preferred_element_type=F32)).astype(BF16)
        copies.append(pltpu.make_async_copy(ytile.at[:, at], y_ref.at[pl.ds(src_ref.shape[0], ytile.shape[0]), at], last_sem.at[t]))
        copies[-1].start()
    for c in copies:
        c.wait()


def settle(y, w_last, o_last, acc_last):
    rows, width = y.shape
    last = o_last.shape[0]
    dma = pltpu.SemaphoreType.DMA
    return pl.pallas_call(
        settle_kernel,
        in_specs=[pl.BlockSpec(memory_space=VMEM)] * 4,
        out_specs=pl.BlockSpec(memory_space=HBM),
        out_shape=HBM((rows + last, width), y.dtype),
        scratch_shapes=[VMEM((last, width), BF16), dma((7,)), dma((4,))],
        compiler_params=pltpu.CompilerParams(vmem_limit_bytes=16 << 20),
        name="settle",
    )(in_vmem(y), in_vmem(w_last), in_vmem(o_last), in_vmem(acc_last))


def solution(mesh):
    def local_step(x_in, doc_id, pos_in_doc, norm_gain, w_q, w_k, w_v, w_o, inv_freq):
        rows = x_in.shape[0]
        q, kvg, k_new, v_new, fl, fr, fara, farb = project(x_in, norm_gain, w_k, w_v, w_q, w_o, pos_in_doc, inv_freq)
        third = lax.ppermute(fara, "tp", [(1, 0), (2, 3)])
        o, k_out, v_out = attention(q, kvg, pos_in_doc, k_new, v_new)
        y = settle(*out_proj(o, (fl, fr, fara, farb, third), w_o, x_in))
        return y, k_out, v_out

    row_spec = P(("dp", "cp"))
    in_specs = (P(("dp", "cp"), None), row_spec, row_spec, P(), P(None, "tp"), P(None, "tp"), P(None, "tp"), P("tp", None), P())
    out_specs = (P(("dp", "cp"), None), P(("dp", "cp"), "tp", None), P(("dp", "cp"), "tp", None))
    return jax.shard_map(local_step, mesh=mesh, in_specs=in_specs, out_specs=out_specs, check_vma=False)
```

```python
import functools

import jax
import jax.numpy as jnp
from jax import lax
from jax.experimental import pallas as pl
from jax.experimental.pallas import tpu as pltpu
from jax.sharding import PartitionSpec as P

MESH = pl.DeviceIdType.MESH
HBM = pltpu.HBM
VMEM = pltpu.VMEM
HEAD = 128
Q_TILE = 128
VMEM_MAX = 67043328
F32 = jnp.float32
BF16 = jnp.bfloat16


def in_vmem(arr):
    return pltpu.with_memory_space_constraint(arr, VMEM)


def rope(vec, cos_t, sin_t):
    vec = vec.astype(F32)
    return (vec * cos_t + pltpu.roll(vec, HEAD // 2, 1) * sin_t).astype(BF16)


def proj_kernel(x_ref, gain_ref, wk_ref, wv_ref, wq_ref, wo_ref, pos_ref, freq_ref,
                q_ref, kvg_ref, k_ref, v_ref, fl_ref, fr_ref, fara_ref, farb_ref,
                xbuf, hbuf, invbuf, gainbuf, posbuf, freqbuf, cosbuf, sinbuf, wkbuf, wvbuf, wqbuf, kvbuf, k3buf, v3buf, qbuf,
                x_sem, w_sem, wq_sem, kvl_sem, kv3_sem, q_sem, kv_send, kv_recv, r1_send, r1_recv, r2_send, r2_recv):
    chunks, q_tiles = 4, 4
    rows, width = hbuf.shape
    c_rows = rows // chunks
    piece = rows // 2
    cols = wkbuf.shape[1]
    q_cols = wqbuf.shape[2]
    half = fl_ref.shape[0] // 2
    n_cp = 4
    dp, z, cp = lax.axis_index("dp"), lax.axis_index("tp"), lax.axis_index("cp")
    core_cp = cp + 1 - 2 * lax.rem(cp, 2)
    y_cp = lax.rem(cp + 2, 4)
    core, ynb = {"cp": core_cp}, {"cp": y_cp}
    left = {"tp": jnp.maximum(z - 1, 0)}
    right = {"tp": jnp.minimum(z + 1, 3)}
    is_mid = (z == 1) | (z == 2)

    def remote(src, dst, ssem, rsem, dev):
        return pltpu.make_async_remote_copy(src_ref=src, dst_ref=dst, send_sem=ssem, recv_sem=rsem, device_id=dev, device_id_type=MESH)

    barrier = pltpu.get_barrier_semaphore()
    for dev in (core, ynb):
        pl.semaphore_signal(barrier, inc=1, device_id=dev, device_id_type=MESH)

    @pl.when(z > 0)
    def _():
        pl.semaphore_signal(barrier, inc=1, device_id=left, device_id_type=MESH)

    @pl.when(z < 3)
    def _():
        pl.semaphore_signal(barrier, inc=1, device_id=right, device_id_type=MESH)

    def x_load(c):
        return pltpu.make_async_copy(x_ref.at[pl.ds(c * c_rows, c_rows)], xbuf.at[c], x_sem.at[c])

    def wq_load(t):
        return pltpu.make_async_copy(wq_ref.at[:, pl.ds(t * q_cols, q_cols)], wqbuf.at[t], wq_sem.at[t])

    wk_load = pltpu.make_async_copy(wk_ref, wkbuf, w_sem.at[0])
    wv_load = pltpu.make_async_copy(wv_ref, wvbuf, w_sem.at[1])
    small = [pltpu.make_async_copy(src, dst, w_sem.at[2 + i]) for i, (src, dst) in enumerate(((gain_ref, gainbuf), (pos_ref, posbuf), (freq_ref, freqbuf)))]
    for cpy in small:
        cpy.start()
    x_load(0).start()
    wk_load.start()
    wv_load.start()
    for c in range(1, chunks):
        x_load(c).start()
    for t in range(q_tiles):
        wq_load(t).start()

    @pl.when(is_mid)
    def _():
        pl.semaphore_wait(barrier, 4)

    @pl.when(jnp.logical_not(is_mid))
    def _():
        pl.semaphore_wait(barrier, 3)

    p_own = dp * 4 + cp

    def part_of(ref, part):
        return ref.at[pl.ds(part * half, half)]

    def r1(side, part):
        src = wo_ref.at[pl.ds(pl.multiple_of((p_own * 2 + part) * half, half), half)]
        dst = part_of((fr_ref, fl_ref)[side], part)
        return remote(src, dst, r1_send.at[side, part], r1_recv.at[side, part], (left, right)[side])

    def r2(side, part):
        src = part_of((fr_ref, fl_ref)[side], part)
        return remote(src, (fara_ref, farb_ref)[part], r2_send.at[side, part], r2_recv.at[part], (left, right)[side])

    def second_hop(part):
        @pl.when(z > 0)
        def _():
            r1(1, part).wait_recv()

        @pl.when(z < 3)
        def _():
            r1(0, part).wait_recv()

        @pl.when(is_mid)
        def _():
            r2(0, part).start()
            r2(1, part).start()

    for part in range(2):
        @pl.when(z > 0)
        def _(part=part):
            r1(0, part).start()

        @pl.when(z < 3)
        def _(part=part):
            r1(1, part).start()

    def kv_at(owner, c):
        start = jnp.where(c < chunks // 2, owner, 2 * n_cp - 1 - owner) * piece + (c % (chunks // 2)) * c_rows
        return kvg_ref.at[pl.ds(pl.multiple_of(start, c_rows), c_rows)]

    def kv_local(c):
        return pltpu.make_async_copy(kvbuf.at[pl.ds(c * c_rows, c_rows)], kv_at(cp, c), kvl_sem.at[c])

    def kv_copy(kind, c):
        at = kv_at((cp, cp, y_cp)[kind], c)
        return remote(at, at, kv_send.at[kind, c], kv_recv.at[kind, c], (ynb, core, core)[kind])

    def kv_wait(kind, c):
        at = kv_at((y_cp, core_cp, lax.rem(core_cp + 2, 4))[kind], c)
        remote(at, at, kv_send.at[kind, c], kv_recv.at[kind, c], core).wait_recv()

    def kv_out(c):
        kv_local(c).wait()
        kv_copy(0, c).start()
        kv_copy(1, c).start()

    def cache_out(c):
        at = pl.ds(c * c_rows, c_rows)
        return (pltpu.make_async_copy(k3buf.at[at], k_ref.at[at], kv3_sem.at[0, c]),
                pltpu.make_async_copy(v3buf.at[at], v_ref.at[at], kv3_sem.at[1, c]))

    step = 16

    for cpy in small:
        cpy.wait()

    pos_cols = jnp.transpose(posbuf[...].astype(F32))
    for i in range(rows // HEAD):
        angle = pos_cols[:, i:i + 1] * freqbuf[...]
        cos_h, sin_h = jnp.cos(angle), jnp.sin(angle)
        cosbuf[i * HEAD:(i + 1) * HEAD, :] = jnp.concatenate([cos_h, cos_h], axis=-1)
        sinbuf[i * HEAD:(i + 1) * HEAD, :] = jnp.concatenate([-sin_h, sin_h], axis=-1)

    def turn(vec, r_at):
        return rope(vec, cosbuf[r_at, :], sinbuf[r_at, :])

    for c in range(chunks):
        x_load(c).wait()

        def square_rows(i, _, c=c):
            at = pl.ds(pl.multiple_of(i * step, step), step)
            xf = xbuf[c, at, :].astype(F32)
            mean = jnp.sum(xf * xf, axis=-1, keepdims=True) * (1.0 / width)
            invbuf[at, :] = jnp.broadcast_to(lax.rsqrt(mean + 1e-5), (step, HEAD))
            return 0

        def norm_rows(i, _, c=c):
            at = pl.ds(pl.multiple_of(i * step, step), step)
            to = pl.ds(pl.multiple_of(c * c_rows + i * step, step), step)
            inv = invbuf[at, 0:1]
            hbuf[to, :] = (xbuf[c, at, :].astype(F32) * inv * gainbuf[...]).astype(BF16)
            return 0

        lax.fori_loop(0, c_rows // step, square_rows, 0, unroll=4)
        lax.fori_loop(0, c_rows // step, norm_rows, 0, unroll=2)
        if c == 0:
            wk_load.wait()
            wv_load.wait()
        r_at = pl.ds(c * c_rows, c_rows)
        h = hbuf[r_at, :]
        k_new = jnp.dot(h, wkbuf[...], preferred_element_type=F32).astype(BF16)
        v_new = jnp.dot(h, wvbuf[...], preferred_element_type=F32).astype(BF16)
        for j in range(cols // HEAD):
            at = slice(j * HEAD, (j + 1) * HEAD)
            k_head = turn(k_new[:, at], r_at)
            kvbuf[r_at, at] = k_head
            k3buf[r_at, j, :] = k_head
            v3buf[r_at, j, :] = v_new[:, at]
        kvbuf[r_at, cols:] = v_new
        kv_local(c).start()
        for cpy in cache_out(c):
            cpy.start()
        if c > 0:
            kv_out(c - 1)

    second_hop(0)

    def q_out(t):
        return pltpu.make_async_copy(qbuf.at[t], q_ref.at[:, pl.ds(t * q_cols, q_cols)], q_sem.at[t])

    def q_tile(t):
        wq_load(t).wait()
        q_new = jnp.dot(hbuf[...], wqbuf[t], preferred_element_type=F32).astype(BF16)
        everything = pl.ds(0, rows)
        for j in range(q_cols // HEAD):
            qbuf[t, :, j * HEAD:(j + 1) * HEAD] = turn(q_new[:, j * HEAD:(j + 1) * HEAD], everything)
        q_out(t).start()

    q_tile(0)
    kv_out(chunks - 1)
    q_tile(1)
    for c in range(2):
        kv_wait(0, c)
        kv_copy(2, c).start()
    q_tile(2)
    second_hop(1)
    q_tile(3)
    for c in range(2, chunks):
        kv_wait(0, c)
        kv_copy(2, c).start()
    for c in range(chunks):
        kv_wait(1, c)
        kv_wait(2, c)
    for t in range(q_tiles):
        q_out(t).wait()
    for c in range(chunks):
        for cpy in cache_out(c):
            cpy.wait()

    for part in range(2):
        @pl.when(z > 0)
        def _(part=part):
            r1(0, part).wait_send()

        @pl.when(z < 3)
        def _(part=part):
            r1(1, part).wait_send()

        r2(0, part).wait_recv()

        @pl.when(is_mid)
        def _(part=part):
            r2(0, part).wait_send()
            r2(1, part).wait_send()

    for c in range(chunks):
        for kind in range(3):
            kv_copy(kind, c).wait_send()


def project(x, gain, w_k, w_v, w_q, w_o, pos, inv_freq):
    rows, width = x.shape
    cols = w_k.shape[1]
    q_cols = w_q.shape[1]
    w_rows = w_o.shape[0] // 8
    dma = pltpu.SemaphoreType.DMA
    hbm = pl.BlockSpec(memory_space=HBM)
    return pl.pallas_call(
        proj_kernel,
        in_specs=[hbm] * 8,
        out_specs=[hbm] * 8,
        out_shape=[HBM((rows, q_cols), BF16), HBM((4 * rows, 2 * cols), BF16)] + [HBM((rows, cols // HEAD, HEAD), BF16)] * 2
        + [HBM((w_rows, w_o.shape[1]), BF16)] * 2 + [HBM((w_rows // 2, w_o.shape[1]), BF16)] * 2,
        scratch_shapes=[
            VMEM((4, rows // 4, width), BF16),
            VMEM((rows, width), BF16),
            VMEM((rows // 4, HEAD), F32),
            VMEM((1, width), F32),
            VMEM((rows // HEAD, HEAD), jnp.int32),
            VMEM((1, HEAD // 2), F32),
            VMEM((rows, HEAD), F32),
            VMEM((rows, HEAD), F32),
            VMEM((width, cols), BF16),
            VMEM((width, cols), BF16),
            VMEM((4, width, q_cols // 4), BF16),
            VMEM((rows, 2 * cols), BF16),
            VMEM((rows, cols // HEAD, HEAD), BF16),
            VMEM((rows, cols // HEAD, HEAD), BF16),
            VMEM((4, rows, q_cols // 4), BF16),
            dma((4,)), dma((5,)), dma((4,)), dma((4,)), dma((2, 4)), dma((4,)),
            dma((3, 4)), dma((3, 4)), dma((2, 2)), dma((2, 2)), dma((2, 2)), dma((2,)),
        ],
        compiler_params=pltpu.CompilerParams(collective_id=0, has_side_effects=True, vmem_limit_bytes=VMEM_MAX),
        cost_estimate=pl.CostEstimate(flops=2 * rows * width * (2 * cols + q_cols), bytes_accessed=24 << 20, transcendentals=0),
        name="proj",
    )(x, gain.reshape(1, width), w_k, w_v, w_q, w_o, pos.reshape(rows // HEAD, HEAD), inv_freq.reshape(1, HEAD // 2))


def attn_kernel(pos_smem, q_ref, pos_ref, kv_hbm, k_ref, v_ref, o_ref, k_out_ref, v_out_ref, kv_ref, kbuf, vbuf, kv_sem, in_sem, out_sem):
    step, steps = pl.program_id(0), pl.num_programs(0)
    cp = lax.axis_index("cp")
    pieces = kv_sem.shape[0]
    piece = kv_ref.shape[0] // pieces
    per_step = q_ref.shape[0] // Q_TILE
    half_blks = piece // Q_TILE
    kv_cols = kv_ref.shape[1] // 2
    heads = kv_cols // HEAD
    group = q_ref.shape[1] // kv_cols

    def kv_load(j):
        at = pl.ds(j * piece, piece)
        return pltpu.make_async_copy(kv_hbm.at[at], kv_ref.at[at], kv_sem.at[j])

    cache = ((k_ref, kbuf, k_out_ref), (v_ref, vbuf, v_out_ref))
    loads = [pltpu.make_async_copy(src, buf, in_sem.at[i]) for i, (src, buf, _) in enumerate(cache)]
    stores = [pltpu.make_async_copy(buf, dst, out_sem.at[i]) for i, (_, buf, dst) in enumerate(cache)]

    @pl.when(step == 0)
    def _():
        for j in range(pieces):
            kv_load(j).start()
        for c in loads:
            c.start()
        for j in range(pieces):
            @pl.when(j <= cp)
            def _(j=j):
                kv_load(j).wait()

    @pl.when(step == steps // 2)
    def _():
        for j in range(pieces):
            @pl.when(j > cp)
            def _(j=j):
                kv_load(j).wait()
        for c, d in zip(loads, stores):
            c.wait()
            d.start()

    factor = HEAD ** -0.5 * 1.4426950408889634
    wide = 2 * Q_TILE
    pos_cols = jnp.transpose(pos_ref[...].astype(F32))

    def make_block(sub):
        blk = step * per_step + sub
        g0 = jnp.where(blk < half_blks, cp * piece + blk * Q_TILE, (pieces - 1 - cp) * piece + (blk - half_blks) * Q_TILE)
        low = (g0 - pos_smem[blk * Q_TILE]) // Q_TILE
        tok = g0 + lax.broadcasted_iota(jnp.int32, (Q_TILE, 1), 0)
        mine = lax.broadcasted_iota(jnp.int32, pos_cols.shape, 1) == blk
        first = tok - jnp.sum(jnp.where(mine, pos_cols, 0.0), axis=1, keepdims=True).astype(jnp.int32)
        rows_at = slice(sub * Q_TILE, (sub + 1) * Q_TILE)
        near = jnp.maximum(g0 - Q_TILE, 0)

        def limit(start, width):
            u = start + lax.broadcasted_iota(jnp.int32, (1, width), 1)
            return jnp.where((u >= first) & (u <= tok), 3e38, -1e30)

        def scores(n, start, width, lim):
            q = jnp.concatenate([q_ref[rows_at, (n * group + g) * HEAD:(n * group + g + 1) * HEAD] for g in range(group)], axis=0)
            keys = kv_ref[pl.ds(pl.multiple_of(start, Q_TILE), width), n * HEAD:(n + 1) * HEAD]
            s = lax.dot_general(q, keys, (((1,), (1,)), ((), ())), preferred_element_type=F32)
            return jnp.minimum(s, jnp.concatenate([lim] * group, axis=0))

        def values(n, start, width):
            return kv_ref[pl.ds(pl.multiple_of(start, Q_TILE), width), kv_cols + n * HEAD:kv_cols + (n + 1) * HEAD]

        def put(n, acc):
            out = acc.astype(BF16)
            for g in range(group):
                o_ref[rows_at, (n * group + g) * HEAD:(n * group + g + 1) * HEAD] = out[g * Q_TILE:(g + 1) * Q_TILE]

        return low, near, limit, scores, values, put

    def probs(s, m, inv):
        return (jnp.exp2((s - m) * factor) * inv).astype(BF16)

    blocks = [make_block(sub) for sub in range(per_step)]
    states = []
    for low, near, limit, scores, values, put in blocks:
        lim = limit(near, wide)
        for n in range(heads):
            s = scores(n, near, wide, lim)
            m = jnp.max(s, axis=-1, keepdims=True)
            e = jnp.exp2((s - m) * factor)
            total = jnp.sum(e, axis=-1, keepdims=True)
            p = (e * (1.0 / total)).astype(BF16)
            put(n, jnp.dot(p, values(n, near, wide), preferred_element_type=F32))
            states.append((m, total))

    for sub, (low, near, limit, scores, values, put) in enumerate(blocks):
        @pl.when(low < near // Q_TILE)
        def _(sub=sub, low=low, near=near, limit=limit, scores=scores, values=values, put=put):
            for n in range(heads):
                def far_scores(i, n=n):
                    return scores(n, i * Q_TILE, Q_TILE, limit(i * Q_TILE, Q_TILE))

                def far_sum(i, carry):
                    m, total = carry
                    s = far_scores(i)
                    m_new = jnp.maximum(m, jnp.max(s, axis=-1, keepdims=True))
                    part = jnp.sum(jnp.exp2((s - m_new) * factor), axis=-1, keepdims=True)
                    return m_new, total * jnp.exp2((m - m_new) * factor) + part

                m, total = lax.fori_loop(low, near // Q_TILE, far_sum, states[sub * heads + n])
                inv = 1.0 / total

                def far_pv(i, acc, n=n, m=m, inv=inv):
                    return acc + jnp.dot(probs(far_scores(i), m, inv), values(n, i * Q_TILE, Q_TILE), preferred_element_type=F32)

                p = probs(scores(n, near, wide, limit(near, wide)), m, inv)
                acc = jnp.dot(p, values(n, near, wide), preferred_element_type=F32)
                put(n, lax.fori_loop(low, near // Q_TILE, far_pv, acc))

    @pl.when(step == steps - 1)
    def _():
        for d in stores:
            d.wait()


def attention(q, kvg, pos, k, v):
    rows, q_cols = q.shape
    hbm, vmem = pl.BlockSpec(memory_space=HBM), pl.BlockSpec(memory_space=VMEM)
    dma = pltpu.SemaphoreType.DMA
    tile = 2 * Q_TILE
    block = pl.BlockSpec((tile, q_cols), lambda i, *_: (i, 0))
    return pl.pallas_call(
        attn_kernel,
        grid_spec=pltpu.PrefetchScalarGridSpec(
            num_scalar_prefetch=1,
            grid=(rows // tile,),
            in_specs=[block, vmem, hbm, hbm, hbm],
            out_specs=[block, hbm, hbm],
            scratch_shapes=[VMEM(kvg.shape, BF16), VMEM(k.shape, BF16), VMEM(v.shape, BF16), dma((8,)), dma((2,)), dma((2,))],
        ),
        out_shape=[HBM((rows, q_cols), BF16), HBM(k.shape, BF16), HBM(v.shape, BF16)],
        compiler_params=pltpu.CompilerParams(vmem_limit_bytes=VMEM_MAX),
        cost_estimate=pl.CostEstimate(flops=5 << 30, bytes_accessed=8 << 20, transcendentals=0),
        name="attn",
    )(pos, q, pos.reshape(rows // HEAD, HEAD), kvg, k, v)


def out_kernel(o_ref, fl_ref, fr_ref, fara_ref, farb_ref, third_ref, wown_ref, x_ref, y_ref, wlast, olast_ref, alast_ref,
               wbuf, wtile, xtile, obuf, own, acc,
               load_sem, tile_sem, own_sem, wsend, wrecv, w3_send, w3_recv, own_send, fwd_send, o_recv):
    rows, kdim = o_ref.shape
    width = x_ref.shape[1]
    slice_rows = fl_ref.shape[0]
    half = slice_rows // 2
    chunks = own_send.shape[1]
    c_rows = rows // chunks
    n_tile = xtile.shape[2]
    y_cols = 1024
    dp, z, cp = lax.axis_index("dp"), lax.axis_index("tp"), lax.axis_index("cp")
    is_end = (z == 0) | (z == 3)
    is_mid = (z == 1) | (z == 2)
    core = {"cp": cp + 1 - 2 * lax.rem(cp, 2)}
    ynb = {"cp": lax.rem(cp + 2, 4)}
    xnb = {"dp": 1 - dp}
    left = {"tp": jnp.maximum(z - 1, 0)}
    right = {"tp": jnp.minimum(z + 1, 3)}
    p_own = dp * 4 + cp
    p_x = (1 - dp) * 4 + cp
    p_y = dp * 4 + lax.rem(cp + 2, 4)
    p_d = (1 - dp) * 4 + lax.rem(cp + 2, 4)
    p_core = dp * 4 + cp + 1 - 2 * lax.rem(cp, 2)
    low_side = z < 2
    s1 = jnp.where(low_side, 1 - z, 5 - z)
    s2 = jnp.where(low_side, 2, 1)
    s3 = jnp.where(low_side, 3, 0)

    def remote(src, dst, ssem, rsem, dev):
        return pltpu.make_async_remote_copy(src_ref=src, dst_ref=dst, send_sem=ssem, recv_sem=rsem, device_id=dev, device_id_type=MESH)

    barrier = pltpu.get_barrier_semaphore()
    for dev in (core, ynb, xnb):
        pl.semaphore_signal(barrier, inc=1, device_id=dev, device_id_type=MESH)

    @pl.when(z > 0)
    def _():
        pl.semaphore_signal(barrier, inc=1, device_id=left, device_id_type=MESH)

    @pl.when(z < 3)
    def _():
        pl.semaphore_signal(barrier, inc=1, device_id=right, device_id_type=MESH)

    own_load = pltpu.make_async_copy(o_ref, own, own_sem)
    own_load.start()

    def w_at(j, p, start=0, n=None):
        n = slice_rows if n is None else n
        at = pl.ds(pl.multiple_of(p * slice_rows + start, half), n)
        return wlast.at[at] if j == 2 else wbuf.at[j, at]

    def load_w(src, j, part):
        return pltpu.make_async_copy(src, w_at(j, p_own, part * half, half), load_sem.at[j, part])

    def parts_of(ref):
        return ref.at[pl.ds(0, half)], ref.at[pl.ds(half, half)]

    fl, fr, far, third = parts_of(fl_ref), parts_of(fr_ref), (fara_ref, farb_ref), (third_ref,)
    sources = ((fr, far, third), (fl, fr, far), (fr, fl, far), (fl, far, third))
    for zz in range(4):
        @pl.when(z == zz)
        def _(zz=zz):
            for j in range(3):
                for part, src in enumerate(sources[zz][j]):
                    load_w(src, j, part).start()

    @pl.when(is_end)
    def _():
        pl.semaphore_wait(barrier, 4)

    @pl.when(is_mid)
    def _():
        pl.semaphore_wait(barrier, 5)

    def w_copy(j, kind):
        dev = (xnb, ynb, core, ynb, xnb, core, core, core, core)[kind]
        src = (w_at(j, p_own), w_at(j, p_own), w_at(j, p_own), w_at(j, p_x, 0, half), w_at(j, p_y, half, half),
               w_at(j, p_x), w_at(j, p_y), w_at(j, p_d, 0, half), w_at(j, p_d, half, half))[kind]
        return remote(src, src, wsend.at[j, kind], wrecv.at[j, kind], dev)

    def core_p(p):
        return p + 1 - 2 * lax.rem(p, 2)

    def w_wait(j, kind):
        dst = (w_at(j, p_x), w_at(j, p_y), w_at(j, p_core), w_at(j, p_d, 0, half), w_at(j, p_d, half, half),
               w_at(j, core_p(p_x)), w_at(j, core_p(p_y)), w_at(j, core_p(p_d), 0, half), w_at(j, core_p(p_d), half, half))[kind]
        remote(dst, dst, wsend.at[j, kind], wrecv.at[j, kind], core).wait_recv()

    def spread_own(j):
        for kind in (0, 1, 2):
            w_copy(j, kind).start()

    def spread_relay(j):
        w_wait(j, 0)
        w_copy(j, 3).start()
        w_copy(j, 5).start()
        w_wait(j, 1)
        w_copy(j, 4).start()
        w_copy(j, 6).start()

    def spread_diag(j):
        w_wait(j, 3)
        w_copy(j, 7).start()
        w_wait(j, 4)
        w_copy(j, 8).start()

    def spread_done(j):
        for kind in (2, 5, 6, 7, 8):
            w_wait(j, kind)

    def slot_of(s, dev_z):
        return s - (s > dev_z).astype(jnp.int32)

    def o_at(s, c, dev_z=None):
        return obuf.at[slot_of(s, z if dev_z is None else dev_z), pl.ds(pl.multiple_of(c * c_rows, c_rows), c_rows)]

    def o_own(c, side):
        src = o_ref.at[pl.ds(c * c_rows, c_rows)]
        return remote(src, o_at(z, c, z + (-1, 1)[side]), own_send.at[side, c], o_recv.at[z, c], (left, right)[side])

    def o_fwd(s, c, side):
        return remote(o_at(s, c), o_at(s, c, z + (-1, 1)[side]), fwd_send.at[s, c], o_recv.at[s, c], (left, right)[side])

    def o_wait(s, c):
        remote(o_at(s, c), o_at(s, c), fwd_send.at[s, c], o_recv.at[s, c], left).wait_recv()

    def o_pass(s, c):
        o_wait(s, c)

        @pl.when(s < z)
        def _():
            o_fwd(s, c, 1).start()

        @pl.when(s > z)
        def _():
            o_fwd(s, c, 0).start()

    w3_at = w_at(2, p_own, half, half)
    w3 = remote(w3_at, w3_at, w3_send, w3_recv, {"tp": jnp.where(z == 1, 0, 3)})

    def send_own(c):
        @pl.when(z > 0)
        def _():
            o_own(c, 0).start()

        @pl.when(z < 3)
        def _():
            o_own(c, 1).start()

    send_own(0)

    @pl.when(is_mid)
    def _():
        load_w(third_ref, 2, 1).wait()
        w3.start()

    for c in range(1, chunks):
        send_own(c)

    for j in range(2):
        for part in range(2):
            load_w(third_ref, j, part).wait()
        spread_own(j)

    def tile_loads(n, slot):
        at = pl.ds(pl.multiple_of(n * n_tile, n_tile), n_tile)
        return (pltpu.make_async_copy(wown_ref.at[:, at], wtile.at[slot], tile_sem.at[0, slot]),
                pltpu.make_async_copy(x_ref.at[:, at], xtile.at[slot], tile_sem.at[1, slot]))

    n_steps = width // n_tile
    for cpy in tile_loads(0, 0):
        cpy.start()
    own_load.wait()

    def own_step(n, _):
        slot = lax.rem(n, 2)

        @pl.when(n + 1 < n_steps)
        def _():
            for cpy in tile_loads(n + 1, 1 - slot):
                cpy.start()

        for cpy in tile_loads(n, slot):
            cpy.wait()
        at = pl.ds(pl.multiple_of(n * n_tile, n_tile), n_tile)
        acc[:, at] = xtile[slot].astype(F32) + jnp.dot(own[...], wtile[slot], preferred_element_type=F32)
        return 0

    lax.fori_loop(0, n_steps, own_step, 0)

    def add_shard(j, s):
        wide = 512

        def step(n, _):
            at = pl.ds(pl.multiple_of(n * wide, wide), wide)
            acc[:, at] += jnp.dot(obuf[slot_of(s, z)], wbuf[j, :, at], preferred_element_type=F32)
            return 0

        lax.fori_loop(0, width // wide, step, 0)

    spread_relay(0)
    spread_relay(1)

    @pl.when(is_end)
    def _():
        remote(w3_at, w3_at, w3_send, w3_recv, left).wait_recv()

    load_w(third_ref, 2, 0).wait()
    spread_own(2)

    @pl.when(is_mid)
    def _():
        for c in range(chunks):
            o_pass(s1, c)
            o_pass(s2, c)

    spread_diag(0)
    spread_done(0)

    @pl.when(is_end)
    def _():
        for c in range(chunks):
            o_wait(s1, c)

    add_shard(0, s1)
    spread_diag(1)
    spread_done(1)

    @pl.when(is_mid)
    def _():
        for c in range(chunks):
            o_pass(s3, c)

    spread_relay(2)

    @pl.when(is_end)
    def _():
        for c in range(chunks):
            o_wait(s2, c)

    add_shard(1, s2)
    spread_diag(2)
    spread_done(2)

    y_steps = width // y_cols

    def last_step(i, _):
        c = i // y_steps

        @pl.when(is_end & (lax.rem(i, y_steps) == 0))
        def _():
            o_wait(s3, c)

        r_at = pl.ds(pl.multiple_of(c * c_rows, c_rows), c_rows)
        n_at = pl.ds(pl.multiple_of(lax.rem(i, y_steps) * y_cols, y_cols), y_cols)
        y_ref[r_at, n_at] = (acc[r_at, n_at] + jnp.dot(obuf[slot_of(s3, z), r_at, :], wlast[:, n_at], preferred_element_type=F32)).astype(BF16)
        return 0

    rest = pl.ds((chunks - 1) * c_rows, c_rows)
    alast_ref[...] = acc[rest, :]
    lax.fori_loop(0, (chunks - 1) * y_steps, last_step, 0)

    @pl.when(is_end)
    def _():
        o_wait(s3, chunks - 1)

    olast_ref[...] = obuf[slot_of(s3, z), rest, :]

    for j in range(3):
        for kind in range(9):
            w_copy(j, kind).wait_send()
    for c in range(chunks):
        @pl.when(z > 0)
        def _(c=c):
            o_own(c, 0).wait_send()

        @pl.when(z < 3)
        def _(c=c):
            o_own(c, 1).wait_send()

    @pl.when(is_mid)
    def _():
        w3.wait_send()
        for c in range(chunks):
            for s in (s1, s2, s3):
                o_fwd(s, c, 0).wait_send()


def out_proj(o, slices, w_own, x):
    rows, kdim = o.shape
    chunks = 8
    last = rows // chunks
    width = x.shape[1]
    dma = pltpu.SemaphoreType.DMA
    return pl.pallas_call(
        out_kernel,
        in_specs=[pl.BlockSpec(memory_space=HBM)] * 8,
        out_specs=[pl.BlockSpec(memory_space=VMEM)] * 4,
        out_shape=[
            VMEM((rows - last, width), BF16),
            VMEM((kdim, width), BF16),
            VMEM((last, kdim), BF16),
            VMEM((last, width), F32),
        ],
        scratch_shapes=[
            VMEM((2, kdim, width), BF16),
            VMEM((2, kdim, 256), BF16),
            VMEM((2, rows, 256), BF16),
            VMEM((3, rows, kdim), BF16),
            VMEM((rows, kdim), BF16),
            VMEM((rows, width), F32),
            dma((3, 2)), dma((2, 2)), dma, dma((3, 9)), dma((3, 9)), dma, dma,
            dma((2, chunks)), dma((4, chunks)), dma((4, chunks)),
        ],
        compiler_params=pltpu.CompilerParams(collective_id=1, has_side_effects=True, vmem_limit_bytes=45 << 20),
        name="out_proj",
    )(o, *slices, w_own, x)


def settle_kernel(src_ref, w_ref, o_ref, acc_ref, y_ref, ytile, sem, last_sem):
    parts, tiles = sem.shape[0], last_sem.shape[0]
    rows = src_ref.shape[0] // parts
    copies = [pltpu.make_async_copy(src_ref.at[pl.ds(i * rows, rows)], y_ref.at[pl.ds(i * rows, rows)], sem.at[i]) for i in range(parts)]
    for c in copies:
        c.start()
    cols = w_ref.shape[1] // tiles
    for t in range(tiles):
        at = pl.ds(t * cols, cols)
        ytile[:, at] = (acc_ref[:, at] + jnp.dot(o_ref[...], w_ref[:, at], preferred_element_type=F32)).astype(BF16)
        copies.append(pltpu.make_async_copy(ytile.at[:, at], y_ref.at[pl.ds(src_ref.shape[0], ytile.shape[0]), at], last_sem.at[t]))
        copies[-1].start()
    for c in copies:
        c.wait()


def settle(y, w_last, o_last, acc_last):
    rows, width = y.shape
    last = o_last.shape[0]
    dma = pltpu.SemaphoreType.DMA
    return pl.pallas_call(
        settle_kernel,
        in_specs=[pl.BlockSpec(memory_space=VMEM)] * 4,
        out_specs=pl.BlockSpec(memory_space=HBM),
        out_shape=HBM((rows + last, width), y.dtype),
        scratch_shapes=[VMEM((last, width), BF16), dma((7,)), dma((4,))],
        compiler_params=pltpu.CompilerParams(vmem_limit_bytes=16 << 20),
        name="settle",
    )(in_vmem(y), in_vmem(w_last), in_vmem(o_last), in_vmem(acc_last))


def solution(mesh):
    def local_step(x_in, doc_id, pos_in_doc, norm_gain, w_q, w_k, w_v, w_o, inv_freq):
        rows = x_in.shape[0]
        q, kvg, k_new, v_new, fl, fr, fara, farb = project(x_in, norm_gain, w_k, w_v, w_q, w_o, pos_in_doc, inv_freq)
        third = lax.ppermute(fara, "tp", [(1, 0), (2, 3)])
        o, k_out, v_out = attention(q, kvg, pos_in_doc, k_new, v_new)
        y = settle(*out_proj(o, (fl, fr, fara, farb, third), w_o, x_in))
        return y, k_out, v_out

    row_spec = P(("dp", "cp"))
    in_specs = (P(("dp", "cp"), None), row_spec, row_spec, P(), P(None, "tp"), P(None, "tp"), P(None, "tp"), P("tp", None), P())
    out_specs = (P(("dp", "cp"), None), P(("dp", "cp"), "tp", None), P(("dp", "cp"), "tp", None))
    return jax.shard_map(local_step, mesh=mesh, in_specs=in_specs, out_specs=out_specs, check_vma=False)
```
